32 devices in a mesh: sub: 16 (over z, y, x), crs: 2 (over core).
Axes of the slice: x: 2, y: 2, z: 4, core: 2. Of those that a mesh axis runs over, the one named last changes fastest.
Arguments:
- multipliers: float32 [16, 128, 512], P(None, ('sub', 'crs')), may hold values from -6 to 6
- own_modes: float32 [6, 128, 512], P(None, ('sub', 'crs')), may hold values from -0.75 to 0.75
- neighbour_modes: float32 [6, 128, 512], P(None, ('sub', 'crs')), may hold values from -0.75 to 0.75
- face_index: int32 [128, 512], P(('sub', 'crs')), may hold values from 0 to 5, as said below
- neighbour_list: int32 [128, 6], replicated, may hold values from 0 to 127, as said below
- coarse_factor: float32 [768, 768], P('sub', 'crs'), may hold values from -0.21875 to 0.21875
Outputs:
- projected: float32 [16, 128, 512], P(None, ('sub', 'crs'))
The draws below stay inside these ranges and needn't reach their ends.
Inputs may be any that keep to these rules, and one draw needn't show every extreme that they name: `face_index`: the multipliers of each subdomain lie in 6 contiguous nonempty blocks, face 0 first and face 5 last. `neighbour_list`: subdomain s = (8 x + y) * 8 + z sits at (x, y, z) of a periodic grid of 2 x 8 x 8 subdomains; the 6 faces of each subdomain name its grid neighbours x plus 1, x minus 1, y plus or minus 1, z plus or minus 1 (periodic; along the first dimension both name the same subdomain), in an order that differs from subdomain to subdomain.
All inputs are finite; a program needn't handle non-finite values.
Results may differ from the reference program's by a relative error of at most 0.0001.
Values sent between devices are 32-bit elements; how exact they have to be, the bound alone decides.
A program may use at most 64 MiB of HBM per device.

```python
import jax
import jax.numpy as jnp
from jax import lax

MODES = 6
NFACE = 6
IW = 512
NRHS = 16
NSUB = 128
NC = 768
GY = 8
GX = 2
GZ = 8


def draw_face_index(key, part):
    block = IW // NFACE
    spread = block // 4
    jitter = jax.random.randint(key, (NSUB, NFACE - 1), -spread, spread + 1).astype(jnp.int32)
    starts = (lax.broadcasted_iota(jnp.int32, (NSUB, NFACE - 1), 1) + 1) * block + jitter
    places = lax.broadcasted_iota(jnp.int32, (NSUB, IW), 1)
    passed = (places[:, :, None] >= starts[:, None, :]).astype(jnp.int32)
    return jnp.sum(passed, axis=2).astype(jnp.int32)


def draw_neighbour_list(key, part):
    scores = jax.random.randint(jax.random.fold_in(key, 17), (NSUB, NFACE), 0, 1 << 20).astype(jnp.int32)
    scores = scores * 8 + lax.broadcasted_iota(jnp.int32, (NSUB, NFACE), 1)
    order = jnp.argsort(scores, axis=1, stable=True).astype(jnp.int32)
    cells = lax.iota(jnp.int32, NSUB)
    first = cells // (GY * GZ)
    second = cells // GZ % GY
    third = cells % GZ

    def place(a, b, c):
        return ((a * GY + b) * GZ + c).astype(jnp.int32)
    table = jnp.stack([place((first + 1) % GX, second, third), place((first + GX - 1) % GX, second, third), place(first, (second + 1) % GY, third), place(first, (second + GY - 1) % GY, third), place(first, second, (third + 1) % GZ), place(first, second, (third + GZ - 1) % GZ)], axis=1)
    return jnp.take_along_axis(table, order, axis=1).astype(jnp.int32)


def levels(stream_key, dims, cuts, low, top_value):
    gain = 1.0
    for dim, parts in cuts:
        draws = jax.random.uniform(jax.random.fold_in(jax.random.fold_in(stream_key, 6), dim), (parts,), jnp.float32, low / len(cuts), top_value / len(cuts))
        gain = gain * jnp.repeat(jnp.exp(draws), dims[dim] // parts).reshape((-1,) + (1,) * (len(dims) - 1 - dim))
    return gain


def normal_values(key, shape, scale, most, shards=(), kind=jnp.bfloat16):
    array = jax.random.normal(key, shape, jnp.float32) * scale
    if len(shards) > 0:
        array = levels(key, shape, shards, -0.22, 0.18) * array
    return jnp.clip(array, min=-most, max=most).astype(kind)


def setup_inputs(seed: int = 0) -> dict:
    seeds = jax.random.split(jax.random.key(seed), 7)
    return {
        "multipliers": normal_values(seeds[0], (NRHS, NSUB, IW), 1.0, 6.0, ((1, 32),), jnp.float32),
        "own_modes": normal_values(seeds[1], (MODES, NSUB, IW), (IW // 8) ** -0.5, 0.75, ((1, 32),), jnp.float32),
        "neighbour_modes": normal_values(seeds[2], (MODES, NSUB, IW), (IW // 8) ** -0.5, 0.75, ((1, 32),), jnp.float32),
        "face_index": draw_face_index(jax.random.fold_in(seeds[6], 71), 0),
        "neighbour_list": draw_neighbour_list(jax.random.fold_in(seeds[6], 71), 0),
        "coarse_factor": normal_values(seeds[5], (NC, NC), NC ** -0.5, 0.21875, ((0, 16), (1, 2)), jnp.float32),
    }


HIGHEST = lax.Precision.HIGHEST


def reference(multipliers, own_modes, neighbour_modes, face_index, neighbour_list, coarse_factor):
    masked_modes = []
    for which_face in range(NFACE):
        masked_modes.append(neighbour_modes * (face_index == which_face).astype(jnp.float32)[None])
    coarse = jnp.einsum('ksm,rsm->krs', own_modes, multipliers, precision=HIGHEST)
    face_parts = []
    for which_face in range(NFACE):
        face_parts.append(jnp.einsum('ksm,rsm->krs', masked_modes[which_face], multipliers, precision=HIGHEST))
    face_terms = jnp.stack(face_parts, axis=3)
    flattened = face_terms.reshape(MODES, NRHS, NSUB * NFACE).transpose(2, 0, 1)
    targets = neighbour_list.reshape(NSUB * NFACE)
    incoming = jax.ops.segment_sum(flattened, targets, num_segments=NSUB)
    coarse = coarse + incoming.transpose(1, 2, 0)
    right_side = coarse.transpose(2, 0, 1).reshape(NSUB * MODES, NRHS)
    halfway = jnp.einsum('cp,cr->pr', coarse_factor, right_side, precision=HIGHEST)
    amplitudes = jnp.dot(coarse_factor, halfway, precision=HIGHEST, preferred_element_type=jnp.float32)
    amplitudes = amplitudes.reshape(NSUB, MODES, NRHS).transpose(1, 2, 0)
    applied = jnp.einsum('ksm,krs->rsm', own_modes, amplitudes, precision=HIGHEST)
    for which_face in range(NFACE):
        across = amplitudes[:, :, neighbour_list[:, which_face]]
        applied = applied + jnp.einsum('ksm,krs->rsm', masked_modes[which_face], across, precision=HIGHEST)
    return multipliers - applied
```

```python
import functools

import jax
import jax.numpy as jnp
from jax import lax
from jax.experimental import pallas as pl
from jax.experimental.pallas import tpu as pltpu
from jax.sharding import PartitionSpec as P

MESH = pl.DeviceIdType.MESH
NT = (((1,), (1,)), ((), ()))
NN = (((1,), (0,)), ((), ()))
LANES = 128
EDGE = 8


def each(count, step):
    if count <= 64:
        for i in sorted(range(count), key=lambda i: min(i, count - 1 - i)):
            step(i)
    else:
        lax.fori_loop(0, count, lambda i, t: (step(i), t)[1], 0)


def both(value, axis=0):
    high = value.astype(jnp.bfloat16)
    low = (value - high.astype(jnp.float32)).astype(jnp.bfloat16)
    return jnp.concatenate([high, low], axis=axis)


def halves(value):
    rows = value.shape[0] // 2
    return value[:rows] + value[rows:]


def quarters(value):
    value = halves(value)
    cols = value.shape[1] // 2
    return value[:, :cols] + value[:, cols:]


def dot(left, right, dims):
    return lax.dot_general(left, right, dims, preferred_element_type=jnp.float32)


def twice(left, right):
    high = left.astype(jnp.bfloat16)
    low = (left - high.astype(jnp.float32)).astype(jnp.bfloat16)
    wide = jnp.concatenate(
        [jnp.concatenate([high, high], axis=1), jnp.concatenate([low, low], axis=1)], axis=0)
    return halves(dot(wide, right, NN))


def near_kernel(
    sub_size, crs_size,
    mult_h, own_h, nbr_h, face_h, nlist_h, factor_h, out_h,
    mult, own, nbr, face, nlist, factor,
    modes, pair, c_send, c_recv, fcat, fall, fown, fpair, p_send, p_recv, s_send, panel,
    in_sem, c_ssem, c_rsem, g_ssem, g_rsem, f_ssem, f_rsem, p_ssem, p_rsem, s_ssem, s_rsem,
):
    nk, subs, width = own.shape
    nrhs = mult.shape[0]
    nface = nlist.shape[0]
    part = nk * subs
    cols = factor.shape[1]
    tiles = cols // LANES
    slabs = crs_size * tiles
    row_len = sub_size // 2
    group = subs * crs_size
    devices = sub_size * crs_size
    head = crs_size - 1
    g = lax.axis_index("sub")
    c = lax.axis_index("crs")
    me = g * crs_size + c
    is_head = c == head
    is_owner = jnp.logical_and(is_head, g < slabs)
    up, down = part, part + EDGE
    off_x = part + 2 * EDGE
    off_n, off_p = off_x + part, off_x + 2 * part

    loads = [
        pltpu.make_async_copy(a, b, in_sem.at[i]) for i, (a, b) in enumerate((
            (nlist_h, nlist), (face_h, face), (nbr_h, nbr), (own_h, own),
            (mult_h, mult), (factor_h, factor)))
    ]
    for load in loads:
        load.start()
    barrier = pltpu.get_barrier_semaphore()
    first, second = g // row_len, lax.rem(g, row_len)
    across = lax.rem(first + 1, 2) * row_len + second
    after = first * row_len + lax.rem(second + 1, row_len)
    before = first * row_len + lax.rem(second + row_len - 1, row_len)
    groups = (g, across, after, before)
    near = [(groups[j], lax.rem(c + i, crs_size))
            for j in range(4) for i in range(crs_size) if j or i]

    def signal(to):
        pl.semaphore_signal(barrier, inc=1, device_id=to, device_id_type=MESH)

    for to in near:
        signal(to)

    @pl.when(is_owner)
    def _():
        for i in range(1, sub_size):
            signal((lax.rem(g + i, sub_size), head))

    modes[...] = jnp.zeros_like(modes)
    edge = down + EDGE + 3 * part
    for p in range(crs_size):
        fcat[pl.ds(p * LANES + edge, LANES - edge), :] = jnp.zeros((LANES - edge, cols), jnp.float32)
    for load in loads[:4]:
        load.wait()
    fc = face[...]
    first_sub = me * subs
    line = lax.broadcasted_iota(jnp.int32, (subs, width), 0)
    target = jnp.zeros((subs, width), jnp.int32)
    for f in range(nface):
        name = jnp.zeros((subs, width), jnp.int32)
        for s in range(subs):
            name = jnp.where(line == s, nlist[f, first_sub + s], name)
        target = jnp.where(fc == f, name, target)
    third = c * subs + line
    nxt = jnp.where(third == group - 1, 0, third + 1)
    prv = jnp.where(third == 0, group - 1, third - 1)

    def chosen(block, line):
        return jnp.where(target == block * group + line, 1.0, 0.0)

    masks = (
        chosen(g, nxt), chosen(g, prv),
        chosen(across, third), chosen(after, third), chosen(before, third),
    )
    for s in range(subs):
        at = pl.ds(s * width, width)
        own_s = own[:, s, :]
        nbr_s = nbr[:, s, :]
        rows = (
            nk * (s + 1) if s < subs - 1 else up,
            nk * (s - 1) if s > 0 else down + EDGE - nk,
            off_x + nk * s, off_n + nk * s, off_p + nk * s,
        )
        modes[pl.ds(nk * s, nk), at] = own_s
        for d in range(5):
            modes[pl.ds(rows[d], nk), at] = nbr_s * masks[d][s:s + 1, :]
    loads[4].wait()
    sums = jnp.zeros((2 * nrhs, 2 * LANES), jnp.float32)
    for s in range(subs):
        at = pl.ds(s * width, width)
        split = both(modes[:, at])
        pair[:, at] = split
        sums = sums + dot(both(mult[:, s, :]), split, NT)
    sums = quarters(sums)
    c_send[...] = sums

    @pl.when(is_head)
    def _():
        c_recv[c] = sums

    loads[5].wait()

    @pl.when(is_owner)
    def _():
        pl.semaphore_wait(barrier, len(near) + slabs - 1)

    @pl.when(jnp.logical_and(is_head, g >= slabs))
    def _():
        pl.semaphore_wait(barrier, len(near) + slabs)

    @pl.when(jnp.logical_not(is_head))
    def _():
        pl.semaphore_wait(barrier, len(near))

    def c_copy(j):
        return pltpu.make_async_remote_copy(
            src_ref=c_send, dst_ref=c_recv.at[j * crs_size + c],
            send_sem=c_ssem, recv_sem=c_rsem,
            device_id=(groups[j], head), device_id_type=MESH)

    def landed(ref, semaphore):
        pltpu.make_async_copy(ref, ref, semaphore).wait()

    for j in (1, 2, 3):
        c_copy(j).start()

    def g_copy():
        return pltpu.make_async_remote_copy(
            src_ref=factor, dst_ref=fall.at[c],
            send_sem=g_ssem, recv_sem=g_rsem,
            device_id=(g, head), device_id_type=MESH)

    @pl.when(jnp.logical_not(is_head))
    def _():
        c_copy(0).start()
        g_copy().start()

    def row(p, extra=0):
        return pl.multiple_of(p * part + extra, 8)

    def f_pieces(i):
        to = lax.rem(c + i, crs_size)
        nx = lax.rem(to + 1, crs_size)
        pv = lax.rem(to + crs_size - 1, crs_size)
        return to, (
            (row(to), 0, part, g),
            (row(nx), up, EDGE, g),
            (row(pv, part - EDGE), down, EDGE, g),
            (row(to), off_x, part, across),
            (row(to), off_p, part, after),
            (row(to), off_n, part, before),
        )

    def place(ref, p, start, size):
        return ref.at[pl.ds(pl.multiple_of(p * LANES + start, 8), size), :]

    moved = 0
    for i in range(crs_size):
        to, pieces = f_pieces(i)
        for n, (start, spot, size, where) in enumerate(pieces):
            if i or n > 2:
                moved += size
                pltpu.make_async_remote_copy(
                    src_ref=factor.at[pl.ds(start, size), :],
                    dst_ref=place(fcat, c, spot, size),
                    send_sem=f_ssem, recv_sem=f_rsem,
                    device_id=(where, to), device_id_type=MESH).start()
    _, pieces = f_pieces(0)
    for start, spot, size, _ in pieces[:3]:
        fcat[pl.ds(pl.multiple_of(c * LANES + spot, 8), size), :] = factor[pl.ds(start, size), :]

    lane = lax.broadcasted_iota(jnp.int32, (nrhs, LANES), 1)

    def rolled(value, by):
        return pltpu.roll(value, (LANES - by) % LANES, 1) if by % LANES else value

    def p_copy(j):
        return pltpu.make_async_remote_copy(
            src_ref=p_send.at[j], dst_ref=p_recv.at[g],
            send_sem=p_ssem, recv_sem=p_rsem,
            device_id=(j, head), device_id_type=MESH)

    @pl.when(is_head)
    def _():
        held = part * crs_size
        spare = jnp.zeros((LANES - held, cols), jnp.float32)
        fown[head] = both(jnp.concatenate([factor[...], spare], axis=0))
        landed(fall.at[pl.ds(0, head)], g_rsem)
        for p in range(head):
            fown[p] = both(jnp.concatenate([fall[p], spare], axis=0))
        landed(c_recv.at[pl.ds(0, 4 * crs_size - 1)], c_rsem)
        rhs = jnp.zeros((nrhs, LANES), jnp.float32)
        for p in range(crs_size):
            at = p * part
            low = c_recv[(p - 1) % crs_size]
            high = c_recv[(p + 1) % crs_size]
            mine = rolled(c_recv[p], -at)
            mine = mine + jnp.where(lane < at + EDGE, rolled(low, up - at), 0.0)
            mine = mine + jnp.where(
                lane >= at + part - EDGE, rolled(high, down - (at + part - EDGE)), 0.0)
            mine = mine + rolled(c_recv[crs_size + p], off_x - at)
            mine = mine + rolled(c_recv[2 * crs_size + p], off_n - at)
            mine = mine + rolled(c_recv[3 * crs_size + p], off_p - at)
            rhs = jnp.where((lane >= at) & (lane < at + part), mine, rhs)
        for p in range(crs_size):
            term = twice(rhs, fown[p])
            for t in range(tiles):
                p_send[p * tiles + t] = term[:, t * LANES:(t + 1) * LANES]
        for j in range(slabs):
            @pl.when(g != j)
            def _():
                p_copy(j).start()

    landed(fcat.at[pl.ds(0, moved), :], f_rsem)
    for p in range(crs_size):
        fpair[p] = both(fcat[pl.ds(p * LANES, LANES), :])

    def s_copy(t):
        to = t + jnp.where(t >= me, 1, 0)
        return pltpu.make_async_remote_copy(
            src_ref=s_send, dst_ref=panel.at[g],
            send_sem=s_ssem, recv_sem=s_rsem,
            device_id=(to // crs_size, lax.rem(to, crs_size)), device_id_type=MESH)

    @pl.when(is_owner)
    def _():
        p_recv[g] = p_send[g]
        landed(p_recv.at[pl.ds(0, sub_size - 1)], p_rsem)
        mine = p_recv[0]
        for q in range(1, sub_size):
            mine = mine + p_recv[q]
        s_send[...] = mine
        panel[g] = mine
        for t in range(devices - 1):
            s_copy(t).start()
        landed(panel.at[pl.ds(0, slabs - 1)], s_rsem)

    @pl.when(jnp.logical_not(is_owner))
    def _():
        landed(panel, s_rsem)

    amps = jnp.zeros((2 * nrhs, 2 * LANES), jnp.float32)
    for j in range(slabs):
        p, t = j // tiles, j % tiles
        amps = amps + dot(both(panel[j]), fpair[p, :, t * LANES:(t + 1) * LANES], NT)
    amps = quarters(amps)
    for s in range(subs):
        out_h[:, s, :] = twice(amps, pair[:, s * width:(s + 1) * width])

    landed(fcat.at[pl.ds(0, moved), :], f_ssem)

    @pl.when(is_head)
    def _():
        landed(c_recv.at[pl.ds(0, 3)], c_ssem)

    @pl.when(jnp.logical_not(is_head))
    def _():
        landed(c_recv.at[pl.ds(0, 4)], c_ssem)
        landed(factor, g_ssem)

    @pl.when(is_owner)
    def _():
        landed(p_send.at[pl.ds(0, slabs - 1)], p_ssem)
        for t in range(devices - 1):
            s_copy(t).wait_send()

    @pl.when(jnp.logical_and(is_head, g >= slabs))
    def _():
        landed(p_send, p_ssem)


def near_body(sub_size, crs_size, mult, own, nbr, face, nlist, factor):
    nk, subs, width = own.shape
    nrhs = mult.shape[0]
    cols = factor.shape[1]
    slabs = crs_size * cols // LANES
    f32, bf16 = jnp.float32, jnp.bfloat16
    dma = pltpu.SemaphoreType.DMA
    hbm = pl.BlockSpec(memory_space=pl.ANY)
    names = nlist.T
    applied = pl.pallas_call(
        functools.partial(near_kernel, sub_size, crs_size),
        out_shape=pltpu.VMEM(mult.shape, mult.dtype),
        in_specs=[hbm] * 6,
        out_specs=pl.BlockSpec(memory_space=pltpu.VMEM),
        scratch_shapes=[
            pltpu.VMEM(mult.shape, f32), pltpu.VMEM(own.shape, f32), pltpu.VMEM(nbr.shape, f32),
            pltpu.VMEM(face.shape, face.dtype), pltpu.SMEM(names.shape, names.dtype),
            pltpu.VMEM(factor.shape, f32),
            pltpu.VMEM((LANES, subs * width), f32),
            pltpu.VMEM((2 * LANES, subs * width), bf16),
            pltpu.VMEM((nrhs, LANES), f32),
            pltpu.VMEM((4 * crs_size, nrhs, LANES), f32),
            pltpu.VMEM((crs_size * LANES, cols), f32),
            pltpu.VMEM((crs_size,) + factor.shape, f32),
            pltpu.VMEM((crs_size, 2 * LANES, cols), bf16),
            pltpu.VMEM((crs_size, 2 * LANES, cols), bf16),
            pltpu.VMEM((slabs, nrhs, LANES), f32),
            pltpu.VMEM((sub_size, nrhs, LANES), f32),
            pltpu.VMEM((nrhs, LANES), f32),
            pltpu.VMEM((slabs, nrhs, LANES), f32),
            dma((6,)), dma, dma, dma, dma, dma, dma, dma, dma, dma, dma,
        ],
        compiler_params=pltpu.CompilerParams(collective_id=0, has_side_effects=True),
    )(mult, own, nbr, face, names, factor)
    return mult - applied


def wide_kernel(
    sub_size, crs_size,
    mult_h, own_h, nbr_h, face_h, nlist_h, factor_h, out_h,
    mult, own, nbr, face, nlist, factor,
    modes, pair, c_send, c_recv, fcat, fown, fpair, rs_send, rs_recv, ag_send, panel,
    c_ssem, c_rsem, f_ssem, f_rsem, rs_ssem, rs_rsem, ag_ssem, ag_rsem, in_sem, met,
):
    nk, subs, width = own.shape
    nrhs = mult.shape[0]
    nface = nlist.shape[0]
    part = nk * subs
    parts = sub_size // nrhs
    row_len = sub_size // 2
    group = subs * crs_size
    devices = sub_size * crs_size
    g = lax.axis_index("sub")
    c = lax.axis_index("crs")
    me = g * crs_size + c
    up, down = part, part + EDGE
    off_x = part + 2 * EDGE
    off_n, off_p = off_x + part, off_x + 2 * part

    def rank(i):
        other = lax.rem(me + i, devices)
        return (other // crs_size, lax.rem(other, crs_size))

    loads = [
        pltpu.make_async_copy(a, b, in_sem.at[i]) for i, (a, b) in enumerate((
            (nlist_h, nlist), (face_h, face), (nbr_h, nbr), (own_h, own),
            (mult_h, mult), (factor_h, factor)))
    ]
    for load in loads:
        load.start()
    barrier = pltpu.get_barrier_semaphore()
    first, second = g // row_len, lax.rem(g, row_len)
    across = lax.rem(first + 1, 2) * row_len + second
    after = first * row_len + lax.rem(second + 1, row_len)
    before = first * row_len + lax.rem(second + row_len - 1, row_len)
    groups = (g, across, after, before)

    block = 1 << (devices.bit_length() // 2)
    base = me // block * block
    inner = [base + lax.rem(me - base + i, block) for i in range(1, block)]
    outer = [lax.rem(me + i, devices) for i in range(block, devices, block)]
    near = [groups[j] * crs_size + lax.rem(c + i, crs_size)
            for j in range(4) for i in range(crs_size) if j or i]

    def signal(semaphore, other):
        pl.semaphore_signal(
            semaphore, inc=1, device_id=(other // crs_size, lax.rem(other, crs_size)),
            device_id_type=MESH)

    for other in outer + near + inner:
        signal(barrier, other)

    modes[...] = jnp.zeros_like(modes)
    fcat[:, down + EDGE + 3 * part:, :] = jnp.zeros(
        (crs_size, LANES - (down + EDGE + 3 * part), fcat.shape[2]), jnp.float32)
    for load in loads[:4]:
        load.wait()
    fc = face[...]
    first_sub = me * subs
    line = lax.broadcasted_iota(jnp.int32, (subs, width), 0)
    target = jnp.zeros((subs, width), jnp.int32)
    for f in range(nface):
        name = jnp.zeros((subs, width), jnp.int32)
        for s in range(subs):
            name = jnp.where(line == s, nlist[f, first_sub + s], name)
        target = jnp.where(fc == f, name, target)
    third = c * subs + line
    nxt = jnp.where(third == group - 1, 0, third + 1)
    prv = jnp.where(third == 0, group - 1, third - 1)

    def chosen(block, line):
        return jnp.where(target == block * group + line, 1.0, 0.0)

    masks = (
        chosen(g, nxt), chosen(g, prv),
        chosen(across, third), chosen(after, third), chosen(before, third),
    )
    for s in range(subs):
        cols = pl.ds(s * width, width)
        own_s = own[:, s, :]
        nbr_s = nbr[:, s, :]
        rows = (
            nk * (s + 1) if s < subs - 1 else up,
            nk * (s - 1) if s > 0 else down + EDGE - nk,
            off_x + nk * s, off_n + nk * s, off_p + nk * s,
        )
        modes[pl.ds(nk * s, nk), cols] = own_s
        for d in range(5):
            value = nbr_s * masks[d][s:s + 1, :]
            spot = pl.ds(rows[d], nk)
            modes[spot, cols] = value
    loads[4].wait()
    sums = jnp.zeros((2 * nrhs, 2 * LANES), jnp.float32)
    for s in range(subs):
        cols = pl.ds(s * width, width)
        split = both(modes[:, cols])
        pair[:, cols] = split
        sums = sums + dot(both(mult[:, s, :]), split, NT)
    sums = quarters(sums)
    c_send[...] = sums
    c_recv[0, c] = sums

    pl.semaphore_wait(barrier, len(outer) + len(near) + len(inner))

    def c_copy(j, i):
        to = lax.rem(c + i, crs_size)
        return pltpu.make_async_remote_copy(
            src_ref=c_send, dst_ref=c_recv.at[j, c],
            send_sem=c_ssem.at[j, i], recv_sem=c_rsem.at[j, i],
            device_id=(groups[j], to), device_id_type=MESH)

    def c_wait(j, i):
        src = lax.rem(c + crs_size - i, crs_size)
        pltpu.make_async_remote_copy(
            src_ref=c_send, dst_ref=c_recv.at[j, src],
            send_sem=c_ssem.at[j, i], recv_sem=c_rsem.at[j, i],
            device_id=(groups[j], src), device_id_type=MESH).wait_recv()

    for j in (1, 2, 3, 0):
        for i in range(crs_size):
            if j or i:
                c_copy(j, i).start()

    def row(p, extra=0):
        return pl.multiple_of(p * part + extra, 8)

    def f_pieces(i):
        to = lax.rem(c + i, crs_size)
        nx = lax.rem(to + 1, crs_size)
        pv = lax.rem(to + crs_size - 1, crs_size)
        return to, (
            (row(to), 0, part, g),
            (row(nx), up, EDGE, g),
            (row(pv, part - EDGE), down, EDGE, g),
            (row(to), off_x, part, across),
            (row(to), off_p, part, after),
            (row(to), off_n, part, before),
        )

    def f_copy(i, n):
        to, pieces = f_pieces(i)
        start, place, size, where = pieces[n]
        return pltpu.make_async_remote_copy(
            src_ref=factor.at[pl.ds(start, size), :],
            dst_ref=fcat.at[c, pl.ds(place, size), :],
            send_sem=f_ssem.at[i, n], recv_sem=f_rsem.at[i, n],
            device_id=(where, to), device_id_type=MESH)

    def f_wait(i, n):
        to, pieces = f_pieces(i)
        start, place, size, where = pieces[n]
        src = lax.rem(c + crs_size - i, crs_size)
        pltpu.make_async_remote_copy(
            src_ref=factor.at[pl.ds(start, size), :],
            dst_ref=fcat.at[src, pl.ds(place, size), :],
            send_sem=f_ssem.at[i, n], recv_sem=f_rsem.at[i, n],
            device_id=(where, to), device_id_type=MESH).wait_recv()

    for other in outer:
        signal(met, other)

    loads[5].wait()
    span = LANES // part
    blocks = fown.shape[0]
    for b in range(blocks):
        held = factor[b * span * part:min((b + 1) * span, crs_size) * part, :]
        if held.shape[0] < LANES:
            held = jnp.concatenate(
                [held, jnp.zeros((LANES - held.shape[0], held.shape[1]), jnp.float32)], axis=0)
        fown[b] = both(held)

    for j in (0, 1, 2, 3):
        for i in range(crs_size):
            if j or i:
                c_wait(j, i)

    lane = lax.broadcasted_iota(jnp.int32, (nrhs, LANES), 1)

    def rolled(value, by):
        return pltpu.roll(value, (LANES - by) % LANES, 1) if by % LANES else value

    total = jnp.zeros((nrhs, factor.shape[1]), jnp.float32)
    for b in range(blocks):
        group_rhs = jnp.zeros((nrhs, LANES), jnp.float32)
        for p in range(b * span, min((b + 1) * span, crs_size)):
            at = (p - b * span) * part
            low = c_recv[0, (p - 1) % crs_size]
            high = c_recv[0, (p + 1) % crs_size]
            rhs = rolled(c_recv[0, p], -at)
            rhs = rhs + jnp.where(lane < at + EDGE, rolled(low, up - at), 0.0)
            rhs = rhs + jnp.where(
                lane >= at + part - EDGE, rolled(high, down - (at + part - EDGE)), 0.0)
            rhs = rhs + rolled(c_recv[1, p], off_x - at)
            rhs = rhs + rolled(c_recv[2, p], off_n - at)
            rhs = rhs + rolled(c_recv[3, p], off_p - at)
            group_rhs = jnp.where((lane >= at) & (lane < at + part), rhs, group_rhs)
        total = total + twice(group_rhs, fown[b])

    chunk = factor.shape[1] // parts
    for q in range(parts):
        for r in range(nrhs):
            rs_send[q * nrhs + r] = total[r:r + 1, q * chunk:(q + 1) * chunk]

    def rs_copy(i):
        to = lax.rem(g + i, sub_size)
        return pltpu.make_async_remote_copy(
            src_ref=rs_send.at[to], dst_ref=rs_recv.at[g],
            send_sem=rs_ssem.at[i], recv_sem=rs_rsem.at[i],
            device_id=(to, c), device_id_type=MESH)

    def rs_wait(i):
        src = lax.rem(g + sub_size - i, sub_size)
        pltpu.make_async_remote_copy(
            src_ref=rs_send.at[src], dst_ref=rs_recv.at[src],
            send_sem=rs_ssem.at[i], recv_sem=rs_rsem.at[i],
            device_id=(src, c), device_id_type=MESH).wait_recv()

    pl.semaphore_wait(met, len(outer))
    each(sub_size - 1, lambda i: rs_copy(i + 1).start())
    moves = [(i, n) for i in range(crs_size) for n in range(6) if i or n > 2]
    for i, n in moves:
        f_copy(i, n).start()
    _, pieces = f_pieces(0)
    for start, place, size, _ in pieces[:3]:
        fcat[c, pl.ds(place, size), :] = factor[pl.ds(start, size), :]

    rs_recv[g] = rs_send[g]
    each(sub_size - 1, lambda i: rs_wait(i + 1))
    mine = rs_recv[0]
    for q in range(1, sub_size):
        mine = mine + rs_recv[q]
    ag_send[...] = mine

    def ag_copy(i):
        return pltpu.make_async_remote_copy(
            src_ref=ag_send, dst_ref=panel.at[c, g],
            send_sem=ag_ssem.at[i], recv_sem=ag_rsem.at[i],
            device_id=rank(i), device_id_type=MESH)

    def ag_wait(i):
        fg, fcr = rank(devices - i)
        pltpu.make_async_remote_copy(
            src_ref=ag_send, dst_ref=panel.at[fcr, fg],
            send_sem=ag_ssem.at[i], recv_sem=ag_rsem.at[i],
            device_id=(fg, fcr), device_id_type=MESH).wait_recv()

    each(devices - 1, lambda i: ag_copy(i + 1).start())
    panel[c, g] = mine
    for i, n in moves:
        f_wait(i, n)
    for p in range(crs_size):
        fpair[p] = both(fcat[p])
    each(devices - 1, lambda i: ag_wait(i + 1))

    amps = jnp.zeros((2 * nrhs, 2 * LANES), jnp.float32)
    for p in range(crs_size):
        for q in range(parts):
            rows = panel[p, q * nrhs:(q + 1) * nrhs].reshape(nrhs, chunk)
            amps = amps + dot(both(rows), fpair[p, :, q * chunk:(q + 1) * chunk], NT)
    amps = quarters(amps)
    for s in range(subs):
        out_h[:, s, :] = twice(amps, pair[:, s * width:(s + 1) * width])

    for j in range(4):
        for i in range(crs_size):
            if j or i:
                c_copy(j, i).wait_send()
    for i, n in moves:
        f_copy(i, n).wait_send()
    each(sub_size - 1, lambda i: rs_copy(i + 1).wait_send())
    each(devices - 1, lambda i: ag_copy(i + 1).wait_send())


def wide_body(sub_size, crs_size, mult, own, nbr, face, nlist, factor):
    nk, subs, width = own.shape
    nrhs = mult.shape[0]
    part = nk * subs
    blocks = -(-crs_size // (LANES // part))
    cols = factor.shape[1]
    chunk = cols * nrhs // sub_size
    f32 = jnp.float32
    dma = pltpu.SemaphoreType.DMA
    bf16 = jnp.bfloat16
    hbm = pl.BlockSpec(memory_space=pl.ANY)
    names = nlist.T
    applied = pl.pallas_call(
        functools.partial(wide_kernel, sub_size, crs_size),
        out_shape=pltpu.VMEM(mult.shape, mult.dtype),
        in_specs=[hbm] * 6,
        out_specs=pl.BlockSpec(memory_space=pltpu.VMEM),
        scratch_shapes=[
            pltpu.VMEM(mult.shape, f32), pltpu.VMEM(own.shape, f32), pltpu.VMEM(nbr.shape, f32),
            pltpu.VMEM(face.shape, face.dtype), pltpu.SMEM(names.shape, names.dtype),
            pltpu.VMEM(factor.shape, f32),
            pltpu.VMEM((LANES, subs * width), f32),
            pltpu.VMEM((2 * LANES, subs * width), bf16),
            pltpu.VMEM((nrhs, LANES), f32),
            pltpu.VMEM((4, crs_size, nrhs, LANES), f32),
            pltpu.VMEM((crs_size, LANES, cols), f32),
            pltpu.VMEM((blocks, 2 * LANES, cols), bf16),
            pltpu.VMEM((crs_size, 2 * LANES, cols), bf16),
            pltpu.VMEM((sub_size, 1, chunk), f32),
            pltpu.VMEM((sub_size, 1, chunk), f32),
            pltpu.VMEM((1, chunk), f32),
            pltpu.VMEM((crs_size, sub_size, 1, chunk), f32),
            dma((4, crs_size)), dma((4, crs_size)),
            dma((crs_size, 6)), dma((crs_size, 6)),
            dma((sub_size,)), dma((sub_size,)),
            dma((sub_size * crs_size,)), dma((sub_size * crs_size,)), dma((6,)),
            pltpu.SemaphoreType.REGULAR,
        ],
        compiler_params=pltpu.CompilerParams(collective_id=0, has_side_effects=True),
    )(mult, own, nbr, face, names, factor)
    return mult - applied


def body(sub_size, crs_size, mult, own, nbr, face, nlist, factor):
    part = own.shape[0] * own.shape[1]
    slabs = crs_size * factor.shape[1] // LANES
    fits = part * crs_size <= LANES and slabs <= sub_size and factor.shape[1] % LANES == 0
    form = near_body if fits else wide_body
    return form(sub_size, crs_size, mult, own, nbr, face, nlist, factor)


def solution(mesh):
    placed = (
        P(None, ("sub", "crs"), None),
        P(None, ("sub", "crs"), None),
        P(None, ("sub", "crs"), None),
        P(("sub", "crs"), None),
        P(),
        P("sub", "crs"),
    )
    return jax.shard_map(
        functools.partial(body, mesh.shape["sub"], mesh.shape["crs"]),
        mesh=mesh, in_specs=placed, out_specs=P(None, ("sub", "crs"), None), check_vma=False
    )
```

```python
import functools

import jax
import jax.numpy as jnp
from jax import lax
from jax.experimental import pallas as pl
from jax.experimental.pallas import tpu as pltpu
from jax.sharding import PartitionSpec as P

MESH = pl.DeviceIdType.MESH
NT = (((1,), (1,)), ((), ()))
NN = (((1,), (0,)), ((), ()))
LANES = 128
EDGE = 8


def each(count, step):
    if count <= 64:
        for i in sorted(range(count), key=lambda i: min(i, count - 1 - i)):
            step(i)
    else:
        lax.fori_loop(0, count, lambda i, t: (step(i), t)[1], 0)


def both(value, axis=0):
    high = value.astype(jnp.bfloat16)
    low = (value - high.astype(jnp.float32)).astype(jnp.bfloat16)
    return jnp.concatenate([high, low], axis=axis)


def halves(value):
    rows = value.shape[0] // 2
    return value[:rows] + value[rows:]


def quarters(value):
    value = halves(value)
    cols = value.shape[1] // 2
    return value[:, :cols] + value[:, cols:]


def dot(left, right, dims):
    return lax.dot_general(left, right, dims, preferred_element_type=jnp.float32)


def twice(left, right):
    high = left.astype(jnp.bfloat16)
    low = (left - high.astype(jnp.float32)).astype(jnp.bfloat16)
    wide = jnp.concatenate(
        [jnp.concatenate([high, high], axis=1), jnp.concatenate([low, low], axis=1)], axis=0)
    return halves(dot(wide, right, NN))


def homes_of(sub_size, slabs):
    return [sub_size // 2 - slabs // 2 + j for j in range(slabs)]


def parted(value):
    high = value.astype(jnp.bfloat16).astype(jnp.float32)
    return high, value - high


def near_kernel(
    sub_size, crs_size,
    mult_h, own_h, nbr_h, face_h, nlist_h, factor_h, out_h,
    mult, own, nbr, face, nlist, factor,
    modes, pair, s_send, s_recv, slab, high, low, a_send, a_recv,
    in_sem, f_ssem, f_rsem, s_ssem, s_rsem, a_ssem, a_rsem,
):
    nk, subs, width = own.shape
    nrhs = mult.shape[0]
    nface = nlist.shape[0]
    part = nk * subs
    held = part * crs_size
    tiles = factor.shape[1] // LANES
    slabs = crs_size * tiles
    row_len = sub_size // 2
    group = subs * crs_size
    devices = sub_size * crs_size
    head = crs_size - 1
    homes = homes_of(sub_size, slabs)
    g = lax.axis_index("sub")
    c = lax.axis_index("crs")
    me = g * crs_size + c
    owns = jnp.full((), False)
    mine = jnp.zeros((), jnp.int32)
    for j, home in enumerate(homes):
        owns = jnp.logical_or(owns, g == home)
        mine = jnp.where(g == home, j, mine)
    is_owner = jnp.logical_and(c == head, owns)
    is_plain = jnp.logical_not(is_owner)
    keeps = jnp.logical_and(is_owner, mine >= head * tiles)
    up, down = part, part + EDGE
    off_x = part + 2 * EDGE
    off_n, off_p = off_x + part, off_x + 2 * part
    edge = off_p + part

    def around(g):
        first, second = g // row_len, g % row_len
        return (
            (first + 1) % 2 * row_len + second,
            first * row_len + (second + 1) % row_len,
            first * row_len + (second + row_len - 1) % row_len,
        )

    def landed(ref, semaphore):
        pltpu.make_async_copy(ref, ref, semaphore).wait()

    barrier = pltpu.get_barrier_semaphore()

    @pl.when(is_owner)
    def _():
        for i in range(1, devices):
            to = lax.rem(me + i, devices)
            pl.semaphore_signal(
                barrier, inc=1, device_id=(to // crs_size, lax.rem(to, crs_size)), device_id_type=MESH)

    loads = [
        pltpu.make_async_copy(a, b, in_sem.at[i]) for i, (a, b) in enumerate((
            (factor_h, factor), (nlist_h, nlist), (face_h, face), (nbr_h, nbr), (own_h, own),
            (mult_h, mult)))
    ]
    for load in loads:
        load.start()
    modes[...] = jnp.zeros_like(modes)
    loads[0].wait()

    @pl.when(is_owner)
    def _():
        pl.semaphore_wait(barrier, slabs - 1)

    @pl.when(is_plain)
    def _():
        pl.semaphore_wait(barrier, slabs)

    def f_copy(t, home):
        return pltpu.make_async_remote_copy(
            src_ref=factor.at[:, t * LANES:(t + 1) * LANES],
            dst_ref=slab.at[pl.ds(pl.multiple_of(g * held, 8), held), :],
            send_sem=f_ssem, recv_sem=f_rsem,
            device_id=(home, head), device_id_type=MESH)

    for t in range(tiles):
        home = jnp.zeros((), jnp.int32)
        for p in range(crs_size):
            home = jnp.where(c == p, homes[p * tiles + t], home)
        self_kept = jnp.logical_and(c == head, g == home)

        @pl.when(jnp.logical_not(self_kept))
        def _():
            f_copy(t, home).start()

        @pl.when(self_kept)
        def _():
            slab[pl.ds(pl.multiple_of(g * held, 8), held), :] = factor[:, t * LANES:(t + 1) * LANES]

    for load in loads[1:5]:
        load.wait()
    across, after, before = around(g)
    fc = face[...]
    first_sub = me * subs
    line = lax.broadcasted_iota(jnp.int32, (subs, width), 0)
    target = jnp.zeros((subs, width), jnp.int32)
    for f in range(nface):
        name = jnp.zeros((subs, width), jnp.int32)
        for s in range(subs):
            name = jnp.where(line == s, nlist[f, first_sub + s], name)
        target = jnp.where(fc == f, name, target)
    third = c * subs + line
    nxt = jnp.where(third == group - 1, 0, third + 1)
    prv = jnp.where(third == 0, group - 1, third - 1)

    def chosen(block, line):
        return jnp.where(target == block * group + line, 1.0, 0.0)

    masks = (
        chosen(g, nxt), chosen(g, prv),
        chosen(across, third), chosen(after, third), chosen(before, third),
    )
    for s in range(subs):
        at = pl.ds(s * width, width)
        own_s = own[:, s, :]
        nbr_s = nbr[:, s, :]
        rows = (
            nk * (s + 1) if s < subs - 1 else up,
            nk * (s - 1) if s > 0 else down + EDGE - nk,
            off_x + nk * s, off_n + nk * s, off_p + nk * s,
        )
        modes[pl.ds(nk * s, nk), at] = own_s
        for d in range(5):
            modes[pl.ds(rows[d], nk), at] = nbr_s * masks[d][s:s + 1, :]
    loads[5].wait()
    sums = jnp.zeros((2 * nrhs, 2 * LANES), jnp.float32)
    for s in range(subs):
        at = pl.ds(s * width, width)
        split = both(modes[:, at])
        pair[:, at] = split
        sums = sums + dot(both(mult[:, s, :]), split, NT)
    sums = quarters(sums)
    s_send[...] = sums

    def s_copy(j):
        return pltpu.make_async_remote_copy(
            src_ref=s_send, dst_ref=s_recv.at[me],
            send_sem=s_ssem, recv_sem=s_rsem,
            device_id=(homes[j], head), device_id_type=MESH)

    for j in range(slabs):
        @pl.when(jnp.logical_not(jnp.logical_and(is_owner, mine == j)))
        def _():
            s_copy(j).start()

    spare = jnp.zeros((LANES - edge, LANES), jnp.float32)

    def rows_of(ref, d):
        b, p = d // crs_size, d % crs_size

        def take(block, p, start=0, size=part):
            at = block * held + p * part + start
            return ref[at:at + size, :]

        x, n, q = around(b)
        return jnp.concatenate([
            take(b, p), take(b, (p + 1) % crs_size, 0, EDGE),
            take(b, (p - 1) % crs_size, part - EDGE, EDGE),
            take(x, p), take(n, p), take(q, p), spare], axis=0)

    def tile_of(k):
        return jnp.concatenate([
            jnp.concatenate([rows_of(high, d), rows_of(low, d)], axis=1)
            for d in (2 * k, 2 * k + 1)], axis=0)

    def a_copy(d):
        return pltpu.make_async_remote_copy(
            src_ref=a_send.at[d], dst_ref=a_recv.at[mine],
            send_sem=a_ssem, recv_sem=a_rsem,
            device_id=(d // crs_size, d % crs_size), device_id_type=MESH)

    @pl.when(is_owner)
    def _():
        s_recv[me] = sums

        @pl.when(keeps)
        def _():
            landed(slab.at[pl.ds(0, (sub_size - 1) * held), :], f_rsem)

        @pl.when(jnp.logical_not(keeps))
        def _():
            landed(slab, f_rsem)

        high[...], low[...] = parted(slab[...])
        landed(s_recv.at[pl.ds(0, devices - 1)], s_rsem)
        total = jnp.zeros((2 * nrhs, 2 * LANES), jnp.float32)
        for k in range(devices // 2):
            both_sums = jnp.concatenate([s_recv[2 * k], s_recv[2 * k + 1]], axis=1)
            total = total + dot(jnp.concatenate(parted(both_sums), axis=0), tile_of(k), NN)
        panel = quarters(total)
        ph, pw = parted(panel)
        wide = jnp.concatenate(
            [jnp.concatenate([ph, ph], axis=1), jnp.concatenate([pw, pw], axis=1)], axis=0)
        for k in range(devices // 2):
            term = halves(dot(wide, tile_of(k), NT))
            for i in range(2):
                d = 2 * k + i
                a_send[d] = term[:, i * LANES:(i + 1) * LANES]

                @pl.when(me != d)
                def _():
                    a_copy(d).start()
        a_recv[mine] = a_send[me]
        landed(a_recv.at[pl.ds(0, slabs - 1)], a_rsem)

    @pl.when(is_plain)
    def _():
        landed(a_recv, a_rsem)

    amps = a_recv[0]
    for j in range(1, slabs):
        amps = amps + a_recv[j]
    for s in range(subs):
        out_h[:, s, :] = twice(amps, pair[:, s * width:(s + 1) * width])

    @pl.when(keeps)
    def _():
        landed(factor.at[:, 0:(tiles - 1) * LANES], f_ssem)

    @pl.when(jnp.logical_not(keeps))
    def _():
        landed(factor, f_ssem)

    @pl.when(is_owner)
    def _():
        landed(s_recv.at[pl.ds(0, slabs - 1)], s_ssem)
        landed(a_send.at[pl.ds(0, devices - 1)], a_ssem)

    @pl.when(is_plain)
    def _():
        landed(s_recv.at[pl.ds(0, slabs)], s_ssem)


def near_body(sub_size, crs_size, mult, own, nbr, face, nlist, factor):
    nk, subs, width = own.shape
    nrhs = mult.shape[0]
    cols = factor.shape[1]
    devices = sub_size * crs_size
    slabs = crs_size * cols // LANES
    order = sub_size * factor.shape[0]
    f32, bf16 = jnp.float32, jnp.bfloat16
    dma = pltpu.SemaphoreType.DMA
    hbm = pl.BlockSpec(memory_space=pl.ANY)
    names = nlist.T
    applied = pl.pallas_call(
        functools.partial(near_kernel, sub_size, crs_size),
        out_shape=pltpu.VMEM(mult.shape, mult.dtype),
        in_specs=[hbm] * 6,
        out_specs=pl.BlockSpec(memory_space=pltpu.VMEM),
        scratch_shapes=[
            pltpu.VMEM(mult.shape, f32), pltpu.VMEM(own.shape, f32), pltpu.VMEM(nbr.shape, f32),
            pltpu.VMEM(face.shape, face.dtype), pltpu.SMEM(names.shape, names.dtype),
            pltpu.VMEM(factor.shape, f32),
            pltpu.VMEM((LANES, subs * width), f32),
            pltpu.VMEM((2 * LANES, subs * width), bf16),
            pltpu.VMEM((nrhs, LANES), f32),
            pltpu.VMEM((devices, nrhs, LANES), f32),
            pltpu.VMEM((order, LANES), f32),
            pltpu.VMEM((order, LANES), f32),
            pltpu.VMEM((order, LANES), f32),
            pltpu.VMEM((devices, nrhs, LANES), f32),
            pltpu.VMEM((slabs, nrhs, LANES), f32),
            dma((6,)), dma, dma, dma, dma, dma, dma,
        ],
        compiler_params=pltpu.CompilerParams(collective_id=0, has_side_effects=True),
    )(mult, own, nbr, face, names, factor)
    return mult - applied


def wide_kernel(
    sub_size, crs_size,
    mult_h, own_h, nbr_h, face_h, nlist_h, factor_h, out_h,
    mult, own, nbr, face, nlist, factor,
    modes, pair, c_send, c_recv, fcat, fown, fpair, rs_send, rs_recv, ag_send, panel,
    c_ssem, c_rsem, f_ssem, f_rsem, rs_ssem, rs_rsem, ag_ssem, ag_rsem, in_sem, met,
):
    nk, subs, width = own.shape
    nrhs = mult.shape[0]
    nface = nlist.shape[0]
    part = nk * subs
    parts = sub_size // nrhs
    row_len = sub_size // 2
    group = subs * crs_size
    devices = sub_size * crs_size
    g = lax.axis_index("sub")
    c = lax.axis_index("crs")
    me = g * crs_size + c
    up, down = part, part + EDGE
    off_x = part + 2 * EDGE
    off_n, off_p = off_x + part, off_x + 2 * part

    def rank(i):
        other = lax.rem(me + i, devices)
        return (other // crs_size, lax.rem(other, crs_size))

    loads = [
        pltpu.make_async_copy(a, b, in_sem.at[i]) for i, (a, b) in enumerate((
            (nlist_h, nlist), (face_h, face), (nbr_h, nbr), (own_h, own),
            (mult_h, mult), (factor_h, factor)))
    ]
    for load in loads:
        load.start()
    barrier = pltpu.get_barrier_semaphore()
    first, second = g // row_len, lax.rem(g, row_len)
    across = lax.rem(first + 1, 2) * row_len + second
    after = first * row_len + lax.rem(second + 1, row_len)
    before = first * row_len + lax.rem(second + row_len - 1, row_len)
    groups = (g, across, after, before)

    block = 1 << (devices.bit_length() // 2)
    base = me // block * block
    inner = [base + lax.rem(me - base + i, block) for i in range(1, block)]
    outer = [lax.rem(me + i, devices) for i in range(block, devices, block)]
    near = [groups[j] * crs_size + lax.rem(c + i, crs_size)
            for j in range(4) for i in range(crs_size) if j or i]

    def signal(semaphore, other):
        pl.semaphore_signal(
            semaphore, inc=1, device_id=(other // crs_size, lax.rem(other, crs_size)),
            device_id_type=MESH)

    for other in outer + near + inner:
        signal(barrier, other)

    modes[...] = jnp.zeros_like(modes)
    fcat[:, down + EDGE + 3 * part:, :] = jnp.zeros(
        (crs_size, LANES - (down + EDGE + 3 * part), fcat.shape[2]), jnp.float32)
    for load in loads[:4]:
        load.wait()
    fc = face[...]
    first_sub = me * subs
    line = lax.broadcasted_iota(jnp.int32, (subs, width), 0)
    target = jnp.zeros((subs, width), jnp.int32)
    for f in range(nface):
        name = jnp.zeros((subs, width), jnp.int32)
        for s in range(subs):
            name = jnp.where(line == s, nlist[f, first_sub + s], name)
        target = jnp.where(fc == f, name, target)
    third = c * subs + line
    nxt = jnp.where(third == group - 1, 0, third + 1)
    prv = jnp.where(third == 0, group - 1, third - 1)

    def chosen(block, line):
        return jnp.where(target == block * group + line, 1.0, 0.0)

    masks = (
        chosen(g, nxt), chosen(g, prv),
        chosen(across, third), chosen(after, third), chosen(before, third),
    )
    for s in range(subs):
        cols = pl.ds(s * width, width)
        own_s = own[:, s, :]
        nbr_s = nbr[:, s, :]
        rows = (
            nk * (s + 1) if s < subs - 1 else up,
            nk * (s - 1) if s > 0 else down + EDGE - nk,
            off_x + nk * s, off_n + nk * s, off_p + nk * s,
        )
        modes[pl.ds(nk * s, nk), cols] = own_s
        for d in range(5):
            value = nbr_s * masks[d][s:s + 1, :]
            spot = pl.ds(rows[d], nk)
            modes[spot, cols] = value
    loads[4].wait()
    sums = jnp.zeros((2 * nrhs, 2 * LANES), jnp.float32)
    for s in range(subs):
        cols = pl.ds(s * width, width)
        split = both(modes[:, cols])
        pair[:, cols] = split
        sums = sums + dot(both(mult[:, s, :]), split, NT)
    sums = quarters(sums)
    c_send[...] = sums
    c_recv[0, c] = sums

    pl.semaphore_wait(barrier, len(outer) + len(near) + len(inner))

    def c_copy(j, i):
        to = lax.rem(c + i, crs_size)
        return pltpu.make_async_remote_copy(
            src_ref=c_send, dst_ref=c_recv.at[j, c],
            send_sem=c_ssem.at[j, i], recv_sem=c_rsem.at[j, i],
            device_id=(groups[j], to), device_id_type=MESH)

    def c_wait(j, i):
        src = lax.rem(c + crs_size - i, crs_size)
        pltpu.make_async_remote_copy(
            src_ref=c_send, dst_ref=c_recv.at[j, src],
            send_sem=c_ssem.at[j, i], recv_sem=c_rsem.at[j, i],
            device_id=(groups[j], src), device_id_type=MESH).wait_recv()

    for j in (1, 2, 3, 0):
        for i in range(crs_size):
            if j or i:
                c_copy(j, i).start()

    def row(p, extra=0):
        return pl.multiple_of(p * part + extra, 8)

    def f_pieces(i):
        to = lax.rem(c + i, crs_size)
        nx = lax.rem(to + 1, crs_size)
        pv = lax.rem(to + crs_size - 1, crs_size)
        return to, (
            (row(to), 0, part, g),
            (row(nx), up, EDGE, g),
            (row(pv, part - EDGE), down, EDGE, g),
            (row(to), off_x, part, across),
            (row(to), off_p, part, after),
            (row(to), off_n, part, before),
        )

    def f_copy(i, n):
        to, pieces = f_pieces(i)
        start, place, size, where = pieces[n]
        return pltpu.make_async_remote_copy(
            src_ref=factor.at[pl.ds(start, size), :],
            dst_ref=fcat.at[c, pl.ds(place, size), :],
            send_sem=f_ssem.at[i, n], recv_sem=f_rsem.at[i, n],
            device_id=(where, to), device_id_type=MESH)

    def f_wait(i, n):
        to, pieces = f_pieces(i)
        start, place, size, where = pieces[n]
        src = lax.rem(c + crs_size - i, crs_size)
        pltpu.make_async_remote_copy(
            src_ref=factor.at[pl.ds(start, size), :],
            dst_ref=fcat.at[src, pl.ds(place, size), :],
            send_sem=f_ssem.at[i, n], recv_sem=f_rsem.at[i, n],
            device_id=(where, to), device_id_type=MESH).wait_recv()

    for other in outer:
        signal(met, other)

    loads[5].wait()
    span = LANES // part
    blocks = fown.shape[0]
    for b in range(blocks):
        held = factor[b * span * part:min((b + 1) * span, crs_size) * part, :]
        if held.shape[0] < LANES:
            held = jnp.concatenate(
                [held, jnp.zeros((LANES - held.shape[0], held.shape[1]), jnp.float32)], axis=0)
        fown[b] = both(held)

    for j in (0, 1, 2, 3):
        for i in range(crs_size):
            if j or i:
                c_wait(j, i)

    lane = lax.broadcasted_iota(jnp.int32, (nrhs, LANES), 1)

    def rolled(value, by):
        return pltpu.roll(value, (LANES - by) % LANES, 1) if by % LANES else value

    total = jnp.zeros((nrhs, factor.shape[1]), jnp.float32)
    for b in range(blocks):
        group_rhs = jnp.zeros((nrhs, LANES), jnp.float32)
        for p in range(b * span, min((b + 1) * span, crs_size)):
            at = (p - b * span) * part
            low = c_recv[0, (p - 1) % crs_size]
            high = c_recv[0, (p + 1) % crs_size]
            rhs = rolled(c_recv[0, p], -at)
            rhs = rhs + jnp.where(lane < at + EDGE, rolled(low, up - at), 0.0)
            rhs = rhs + jnp.where(
                lane >= at + part - EDGE, rolled(high, down - (at + part - EDGE)), 0.0)
            rhs = rhs + rolled(c_recv[1, p], off_x - at)
            rhs = rhs + rolled(c_recv[2, p], off_n - at)
            rhs = rhs + rolled(c_recv[3, p], off_p - at)
            group_rhs = jnp.where((lane >= at) & (lane < at + part), rhs, group_rhs)
        total = total + twice(group_rhs, fown[b])

    chunk = factor.shape[1] // parts
    for q in range(parts):
        for r in range(nrhs):
            rs_send[q * nrhs + r] = total[r:r + 1, q * chunk:(q + 1) * chunk]

    def rs_copy(i):
        to = lax.rem(g + i, sub_size)
        return pltpu.make_async_remote_copy(
            src_ref=rs_send.at[to], dst_ref=rs_recv.at[g],
            send_sem=rs_ssem.at[i], recv_sem=rs_rsem.at[i],
            device_id=(to, c), device_id_type=MESH)

    def rs_wait(i):
        src = lax.rem(g + sub_size - i, sub_size)
        pltpu.make_async_remote_copy(
            src_ref=rs_send.at[src], dst_ref=rs_recv.at[src],
            send_sem=rs_ssem.at[i], recv_sem=rs_rsem.at[i],
            device_id=(src, c), device_id_type=MESH).wait_recv()

    pl.semaphore_wait(met, len(outer))
    each(sub_size - 1, lambda i: rs_copy(i + 1).start())
    moves = [(i, n) for i in range(crs_size) for n in range(6) if i or n > 2]
    for i, n in moves:
        f_copy(i, n).start()
    _, pieces = f_pieces(0)
    for start, place, size, _ in pieces[:3]:
        fcat[c, pl.ds(place, size), :] = factor[pl.ds(start, size), :]

    rs_recv[g] = rs_send[g]
    each(sub_size - 1, lambda i: rs_wait(i + 1))
    mine = rs_recv[0]
    for q in range(1, sub_size):
        mine = mine + rs_recv[q]
    ag_send[...] = mine

    def ag_copy(i):
        return pltpu.make_async_remote_copy(
            src_ref=ag_send, dst_ref=panel.at[c, g],
            send_sem=ag_ssem.at[i], recv_sem=ag_rsem.at[i],
            device_id=rank(i), device_id_type=MESH)

    def ag_wait(i):
        fg, fcr = rank(devices - i)
        pltpu.make_async_remote_copy(
            src_ref=ag_send, dst_ref=panel.at[fcr, fg],
            send_sem=ag_ssem.at[i], recv_sem=ag_rsem.at[i],
            device_id=(fg, fcr), device_id_type=MESH).wait_recv()

    each(devices - 1, lambda i: ag_copy(i + 1).start())
    panel[c, g] = mine
    for i, n in moves:
        f_wait(i, n)
    for p in range(crs_size):
        fpair[p] = both(fcat[p])
    each(devices - 1, lambda i: ag_wait(i + 1))

    amps = jnp.zeros((2 * nrhs, 2 * LANES), jnp.float32)
    for p in range(crs_size):
        for q in range(parts):
            rows = panel[p, q * nrhs:(q + 1) * nrhs].reshape(nrhs, chunk)
            amps = amps + dot(both(rows), fpair[p, :, q * chunk:(q + 1) * chunk], NT)
    amps = quarters(amps)
    for s in range(subs):
        out_h[:, s, :] = twice(amps, pair[:, s * width:(s + 1) * width])

    for j in range(4):
        for i in range(crs_size):
            if j or i:
                c_copy(j, i).wait_send()
    for i, n in moves:
        f_copy(i, n).wait_send()
    each(sub_size - 1, lambda i: rs_copy(i + 1).wait_send())
    each(devices - 1, lambda i: ag_copy(i + 1).wait_send())


def wide_body(sub_size, crs_size, mult, own, nbr, face, nlist, factor):
    nk, subs, width = own.shape
    nrhs = mult.shape[0]
    part = nk * subs
    blocks = -(-crs_size // (LANES // part))
    cols = factor.shape[1]
    chunk = cols * nrhs // sub_size
    f32 = jnp.float32
    dma = pltpu.SemaphoreType.DMA
    bf16 = jnp.bfloat16
    hbm = pl.BlockSpec(memory_space=pl.ANY)
    names = nlist.T
    applied = pl.pallas_call(
        functools.partial(wide_kernel, sub_size, crs_size),
        out_shape=pltpu.VMEM(mult.shape, mult.dtype),
        in_specs=[hbm] * 6,
        out_specs=pl.BlockSpec(memory_space=pltpu.VMEM),
        scratch_shapes=[
            pltpu.VMEM(mult.shape, f32), pltpu.VMEM(own.shape, f32), pltpu.VMEM(nbr.shape, f32),
            pltpu.VMEM(face.shape, face.dtype), pltpu.SMEM(names.shape, names.dtype),
            pltpu.VMEM(factor.shape, f32),
            pltpu.VMEM((LANES, subs * width), f32),
            pltpu.VMEM((2 * LANES, subs * width), bf16),
            pltpu.VMEM((nrhs, LANES), f32),
            pltpu.VMEM((4, crs_size, nrhs, LANES), f32),
            pltpu.VMEM((crs_size, LANES, cols), f32),
            pltpu.VMEM((blocks, 2 * LANES, cols), bf16),
            pltpu.VMEM((crs_size, 2 * LANES, cols), bf16),
            pltpu.VMEM((sub_size, 1, chunk), f32),
            pltpu.VMEM((sub_size, 1, chunk), f32),
            pltpu.VMEM((1, chunk), f32),
            pltpu.VMEM((crs_size, sub_size, 1, chunk), f32),
            dma((4, crs_size)), dma((4, crs_size)),
            dma((crs_size, 6)), dma((crs_size, 6)),
            dma((sub_size,)), dma((sub_size,)),
            dma((sub_size * crs_size,)), dma((sub_size * crs_size,)), dma((6,)),
            pltpu.SemaphoreType.REGULAR,
        ],
        compiler_params=pltpu.CompilerParams(collective_id=0, has_side_effects=True),
    )(mult, own, nbr, face, names, factor)
    return mult - applied


def body(sub_size, crs_size, mult, own, nbr, face, nlist, factor):
    slabs = crs_size * factor.shape[1] // LANES
    fits = slabs <= sub_size // 2 and factor.shape[1] % LANES == 0 and sub_size * crs_size <= LANES // 2
    form = near_body if fits else wide_body
    return form(sub_size, crs_size, mult, own, nbr, face, nlist, factor)


def solution(mesh):
    placed = (
        P(None, ("sub", "crs"), None),
        P(None, ("sub", "crs"), None),
        P(None, ("sub", "crs"), None),
        P(("sub", "crs"), None),
        P(),
        P("sub", "crs"),
    )
    return jax.shard_map(
        functools.partial(body, mesh.shape["sub"], mesh.shape["crs"]),
        mesh=mesh, in_specs=placed, out_specs=P(None, ("sub", "crs"), None), check_vma=False
    )
```

```python
import functools

import jax
import jax.numpy as jnp
from jax import lax
from jax.experimental import pallas as pl
from jax.experimental.pallas import tpu as pltpu
from jax.sharding import PartitionSpec as P

MESH = pl.DeviceIdType.MESH
NT = (((1,), (1,)), ((), ()))
NN = (((1,), (0,)), ((), ()))
LANES = 128
EDGE = 8


def each(count, step):
    if count <= 64:
        for i in sorted(range(count), key=lambda i: min(i, count - 1 - i)):
            step(i)
    else:
        lax.fori_loop(0, count, lambda i, t: (step(i), t)[1], 0)


def both(value, axis=0):
    high = value.astype(jnp.bfloat16)
    low = (value - high.astype(jnp.float32)).astype(jnp.bfloat16)
    return jnp.concatenate([high, low], axis=axis)


def halves(value):
    rows = value.shape[0] // 2
    return value[:rows] + value[rows:]


def quarters(value):
    value = halves(value)
    cols = value.shape[1] // 2
    return value[:, :cols] + value[:, cols:]


def dot(left, right, dims):
    return lax.dot_general(left, right, dims, preferred_element_type=jnp.float32)


def twice(left, right):
    high = left.astype(jnp.bfloat16)
    low = (left - high.astype(jnp.float32)).astype(jnp.bfloat16)
    wide = jnp.concatenate(
        [jnp.concatenate([high, high], axis=1), jnp.concatenate([low, low], axis=1)], axis=0)
    return halves(dot(wide, right, NN))


def homes_of(sub_size, slabs):
    q = sub_size // 4
    return (1, 2 * q, q + 1, q, q + 2, 2 * q + 2)[:slabs]


def parted(value):
    high = value.astype(jnp.bfloat16).astype(jnp.float32)
    return high, value - high


def near_kernel(
    sub_size, crs_size,
    mult_h, own_h, nbr_h, face_h, nlist_h, factor_h, out_h,
    mult, own, nbr, face, nlist, factor,
    modes, pair, s_send, s_recv, slab, high, low, a_send, a_recv,
    in_sem, f_ssem, f_rsem, s_ssem, s_rsem, a_ssem, a_rsem,
):
    nk, subs, width = own.shape
    nrhs = mult.shape[0]
    nface = nlist.shape[0]
    part = nk * subs
    held = part * crs_size
    tiles = factor.shape[1] // LANES
    slabs = crs_size * tiles
    row_len = sub_size // 2
    group = subs * crs_size
    devices = sub_size * crs_size
    head = crs_size - 1
    homes = homes_of(sub_size, slabs)
    g = lax.axis_index("sub")
    c = lax.axis_index("crs")
    me = g * crs_size + c
    owns = jnp.full((), False)
    mine = jnp.zeros((), jnp.int32)
    for j, home in enumerate(homes):
        owns = jnp.logical_or(owns, g == home)
        mine = jnp.where(g == home, j, mine)
    is_owner = jnp.logical_and(c == head, owns)
    is_plain = jnp.logical_not(is_owner)
    keeps = jnp.logical_and(is_owner, mine >= head * tiles)
    up, down = part, part + EDGE
    off_x = part + 2 * EDGE
    off_n, off_p = off_x + part, off_x + 2 * part
    edge = off_p + part

    def around(g):
        first, second = g // row_len, g % row_len
        return (
            (first + 1) % 2 * row_len + second,
            first * row_len + (second + 1) % row_len,
            first * row_len + (second + row_len - 1) % row_len,
        )

    def landed(ref, semaphore):
        pltpu.make_async_copy(ref, ref, semaphore).wait()

    barrier = pltpu.get_barrier_semaphore()

    @pl.when(is_owner)
    def _():
        for i in range(devices - 1):
            to = i + jnp.where(i >= me, 1, 0)
            pl.semaphore_signal(
                barrier, inc=1, device_id=(to // crs_size, lax.rem(to, crs_size)), device_id_type=MESH)

    loads = [
        pltpu.make_async_copy(a, b, in_sem.at[i]) for i, (a, b) in enumerate((
            (factor_h, factor), (nlist_h, nlist), (face_h, face), (nbr_h, nbr), (own_h, own),
            (mult_h, mult)))
    ]
    for load in loads:
        load.start()
    modes[...] = jnp.zeros_like(modes)
    loads[0].wait()

    @pl.when(is_owner)
    def _():
        pl.semaphore_wait(barrier, slabs - 1)

    @pl.when(is_plain)
    def _():
        pl.semaphore_wait(barrier, slabs)

    def home_of(j):
        home = jnp.zeros((), jnp.int32)
        for i in range(slabs):
            home = jnp.where(j == i, homes[i], home)
        return home

    def tile_in(t):
        return factor.at[:, pl.ds(pl.multiple_of(t * LANES, LANES), LANES)]

    def f_copy(t, home):
        return pltpu.make_async_remote_copy(
            src_ref=tile_in(t),
            dst_ref=slab.at[pl.ds(pl.multiple_of(g * held, 8), held), :],
            send_sem=f_ssem, recv_sem=f_rsem,
            device_id=(home, head), device_id_type=MESH)

    for t in range(tiles):
        t = lax.rem(t + g, tiles)
        home = home_of(c * tiles + t)
        self_kept = jnp.logical_and(c == head, g == home)

        @pl.when(jnp.logical_not(self_kept))
        def _():
            f_copy(t, home).start()

        @pl.when(self_kept)
        def _():
            slab[pl.ds(pl.multiple_of(g * held, 8), held), :] = tile_in(t)[...]

    for load in loads[1:5]:
        load.wait()
    across, after, before = around(g)
    fc = face[...]
    first_sub = me * subs
    line = lax.broadcasted_iota(jnp.int32, (subs, width), 0)
    target = jnp.zeros((subs, width), jnp.int32)
    for f in range(nface):
        name = jnp.zeros((subs, width), jnp.int32)
        for s in range(subs):
            name = jnp.where(line == s, nlist[f, first_sub + s], name)
        target = jnp.where(fc == f, name, target)
    third = c * subs + line
    nxt = jnp.where(third == group - 1, 0, third + 1)
    prv = jnp.where(third == 0, group - 1, third - 1)

    def chosen(block, line):
        return jnp.where(target == block * group + line, 1.0, 0.0)

    masks = (
        chosen(g, nxt), chosen(g, prv),
        chosen(across, third), chosen(after, third), chosen(before, third),
    )
    for s in range(subs):
        at = pl.ds(s * width, width)
        own_s = own[:, s, :]
        nbr_s = nbr[:, s, :]
        rows = (
            nk * (s + 1) if s < subs - 1 else up,
            nk * (s - 1) if s > 0 else down + EDGE - nk,
            off_x + nk * s, off_n + nk * s, off_p + nk * s,
        )
        modes[pl.ds(nk * s, nk), at] = own_s
        for d in range(5):
            modes[pl.ds(rows[d], nk), at] = nbr_s * masks[d][s:s + 1, :]
    loads[5].wait()
    sums = jnp.zeros((2 * nrhs, 2 * LANES), jnp.float32)
    for s in range(subs):
        at = pl.ds(s * width, width)
        split = both(modes[:, at])
        pair[:, at] = split
        sums = sums + dot(both(mult[:, s, :]), split, NT)
    sums = quarters(sums)
    s_send[...] = sums

    def s_copy(j):
        return pltpu.make_async_remote_copy(
            src_ref=s_send, dst_ref=s_recv.at[me],
            send_sem=s_ssem, recv_sem=s_rsem,
            device_id=(home_of(j), head), device_id_type=MESH)

    for j in range(slabs - 1):
        s_copy(j + jnp.where(jnp.logical_and(is_owner, j >= mine), 1, 0)).start()

    @pl.when(is_plain)
    def _():
        s_copy(slabs - 1).start()

    spare = jnp.zeros((LANES - edge, LANES), jnp.float32)

    def rows_of(ref, d):
        b, p = d // crs_size, d % crs_size

        def take(block, p, start=0, size=part):
            at = block * held + p * part + start
            return ref[at:at + size, :]

        x, n, q = around(b)
        return jnp.concatenate([
            take(b, p), take(b, (p + 1) % crs_size, 0, EDGE),
            take(b, (p - 1) % crs_size, part - EDGE, EDGE),
            take(x, p), take(n, p), take(q, p), spare], axis=0)

    def tile_of(k):
        return jnp.concatenate([
            jnp.concatenate([rows_of(high, d), rows_of(low, d)], axis=1)
            for d in (2 * k, 2 * k + 1)], axis=0)

    def a_copy(d):
        return pltpu.make_async_remote_copy(
            src_ref=a_send.at[d], dst_ref=a_recv.at[mine],
            send_sem=a_ssem, recv_sem=a_rsem,
            device_id=(lax.div(d, crs_size), lax.rem(d, crs_size)), device_id_type=MESH)

    def a_group(start, stop):
        inside = jnp.logical_and(me >= start, me < stop)
        for d in range(start, stop - 1):
            a_copy(d + jnp.where(jnp.logical_and(inside, d >= me), 1, 0)).start()

        @pl.when(jnp.logical_not(inside))
        def _():
            a_copy(jnp.int32(stop - 1)).start()

    @pl.when(is_owner)
    def _():
        s_recv[me] = sums

        @pl.when(keeps)
        def _():
            landed(slab.at[pl.ds(0, (sub_size - 1) * held), :], f_rsem)

        @pl.when(jnp.logical_not(keeps))
        def _():
            landed(slab, f_rsem)

        high[...], low[...] = parted(slab[...])
        landed(s_recv.at[pl.ds(0, devices - 1)], s_rsem)
        total = jnp.zeros((2 * nrhs, 2 * LANES), jnp.float32)
        for k in range(devices // 2):
            both_sums = jnp.concatenate([s_recv[2 * k], s_recv[2 * k + 1]], axis=1)
            total = total + dot(jnp.concatenate(parted(both_sums), axis=0), tile_of(k), NN)
        panel = quarters(total)
        ph, pw = parted(panel)
        wide = jnp.concatenate(
            [jnp.concatenate([ph, ph], axis=1), jnp.concatenate([pw, pw], axis=1)], axis=0)
        def form(k):
            term = halves(dot(wide, tile_of(k), NT))
            for i in range(2):
                a_send[2 * k + i] = term[:, i * LANES:(i + 1) * LANES]

        quarter = devices // 4
        for start, stop in ((0, 2), (3 * quarter, devices), (2 * quarter, 3 * quarter), (2, quarter), (quarter, 2 * quarter)):
            for k in range(start // 2, stop // 2):
                form(k)
            a_group(start, stop)
        a_recv[mine] = a_send[me]
        landed(a_recv.at[pl.ds(0, slabs - 1)], a_rsem)

    @pl.when(is_plain)
    def _():
        landed(a_recv, a_rsem)

    amps = a_recv[0]
    for j in range(1, slabs):
        amps = amps + a_recv[j]
    for s in range(subs):
        out_h[:, s, :] = twice(amps, pair[:, s * width:(s + 1) * width])

    @pl.when(keeps)
    def _():
        landed(factor.at[:, 0:(tiles - 1) * LANES], f_ssem)

    @pl.when(jnp.logical_not(keeps))
    def _():
        landed(factor, f_ssem)

    @pl.when(is_owner)
    def _():
        landed(s_recv.at[pl.ds(0, slabs - 1)], s_ssem)
        landed(a_send.at[pl.ds(0, devices - 1)], a_ssem)

    @pl.when(is_plain)
    def _():
        landed(s_recv.at[pl.ds(0, slabs)], s_ssem)


def near_body(sub_size, crs_size, mult, own, nbr, face, nlist, factor):
    nk, subs, width = own.shape
    nrhs = mult.shape[0]
    cols = factor.shape[1]
    devices = sub_size * crs_size
    slabs = crs_size * cols // LANES
    order = sub_size * factor.shape[0]
    f32, bf16 = jnp.float32, jnp.bfloat16
    dma = pltpu.SemaphoreType.DMA
    hbm = pl.BlockSpec(memory_space=pl.ANY)
    names = nlist.T
    applied = pl.pallas_call(
        functools.partial(near_kernel, sub_size, crs_size),
        out_shape=pltpu.VMEM(mult.shape, mult.dtype),
        in_specs=[hbm] * 6,
        out_specs=pl.BlockSpec(memory_space=pltpu.VMEM),
        scratch_shapes=[
            pltpu.VMEM(mult.shape, f32), pltpu.VMEM(own.shape, f32), pltpu.VMEM(nbr.shape, f32),
            pltpu.VMEM(face.shape, face.dtype), pltpu.SMEM(names.shape, names.dtype),
            pltpu.VMEM(factor.shape, f32),
            pltpu.VMEM((LANES, subs * width), f32),
            pltpu.VMEM((2 * LANES, subs * width), bf16),
            pltpu.VMEM((nrhs, LANES), f32),
            pltpu.VMEM((devices, nrhs, LANES), f32),
            pltpu.VMEM((order, LANES), f32),
            pltpu.VMEM((order, LANES), f32),
            pltpu.VMEM((order, LANES), f32),
            pltpu.VMEM((devices, nrhs, LANES), f32),
            pltpu.VMEM((slabs, nrhs, LANES), f32),
            dma((6,)), dma, dma, dma, dma, dma, dma,
        ],
        compiler_params=pltpu.CompilerParams(collective_id=0, has_side_effects=True),
    )(mult, own, nbr, face, names, factor)
    return mult - applied


def wide_kernel(
    sub_size, crs_size,
    mult_h, own_h, nbr_h, face_h, nlist_h, factor_h, out_h,
    mult, own, nbr, face, nlist, factor,
    modes, pair, c_send, c_recv, fcat, fown, fpair, rs_send, rs_recv, ag_send, panel,
    c_ssem, c_rsem, f_ssem, f_rsem, rs_ssem, rs_rsem, ag_ssem, ag_rsem, in_sem, met,
):
    nk, subs, width = own.shape
    nrhs = mult.shape[0]
    nface = nlist.shape[0]
    part = nk * subs
    parts = sub_size // nrhs
    row_len = sub_size // 2
    group = subs * crs_size
    devices = sub_size * crs_size
    g = lax.axis_index("sub")
    c = lax.axis_index("crs")
    me = g * crs_size + c
    up, down = part, part + EDGE
    off_x = part + 2 * EDGE
    off_n, off_p = off_x + part, off_x + 2 * part

    def rank(i):
        other = lax.rem(me + i, devices)
        return (other // crs_size, lax.rem(other, crs_size))

    loads = [
        pltpu.make_async_copy(a, b, in_sem.at[i]) for i, (a, b) in enumerate((
            (nlist_h, nlist), (face_h, face), (nbr_h, nbr), (own_h, own),
            (mult_h, mult), (factor_h, factor)))
    ]
    for load in loads:
        load.start()
    barrier = pltpu.get_barrier_semaphore()
    first, second = g // row_len, lax.rem(g, row_len)
    across = lax.rem(first + 1, 2) * row_len + second
    after = first * row_len + lax.rem(second + 1, row_len)
    before = first * row_len + lax.rem(second + row_len - 1, row_len)
    groups = (g, across, after, before)

    block = 1 << (devices.bit_length() // 2)
    base = me // block * block
    inner = [base + lax.rem(me - base + i, block) for i in range(1, block)]
    outer = [lax.rem(me + i, devices) for i in range(block, devices, block)]
    near = [groups[j] * crs_size + lax.rem(c + i, crs_size)
            for j in range(4) for i in range(crs_size) if j or i]

    def signal(semaphore, other):
        pl.semaphore_signal(
            semaphore, inc=1, device_id=(other // crs_size, lax.rem(other, crs_size)),
            device_id_type=MESH)

    for other in outer + near + inner:
        signal(barrier, other)

    modes[...] = jnp.zeros_like(modes)
    fcat[:, down + EDGE + 3 * part:, :] = jnp.zeros(
        (crs_size, LANES - (down + EDGE + 3 * part), fcat.shape[2]), jnp.float32)
    for load in loads[:4]:
        load.wait()
    fc = face[...]
    first_sub = me * subs
    line = lax.broadcasted_iota(jnp.int32, (subs, width), 0)
    target = jnp.zeros((subs, width), jnp.int32)
    for f in range(nface):
        name = jnp.zeros((subs, width), jnp.int32)
        for s in range(subs):
            name = jnp.where(line == s, nlist[f, first_sub + s], name)
        target = jnp.where(fc == f, name, target)
    third = c * subs + line
    nxt = jnp.where(third == group - 1, 0, third + 1)
    prv = jnp.where(third == 0, group - 1, third - 1)

    def chosen(block, line):
        return jnp.where(target == block * group + line, 1.0, 0.0)

    masks = (
        chosen(g, nxt), chosen(g, prv),
        chosen(across, third), chosen(after, third), chosen(before, third),
    )
    for s in range(subs):
        cols = pl.ds(s * width, width)
        own_s = own[:, s, :]
        nbr_s = nbr[:, s, :]
        rows = (
            nk * (s + 1) if s < subs - 1 else up,
            nk * (s - 1) if s > 0 else down + EDGE - nk,
            off_x + nk * s, off_n + nk * s, off_p + nk * s,
        )
        modes[pl.ds(nk * s, nk), cols] = own_s
        for d in range(5):
            value = nbr_s * masks[d][s:s + 1, :]
            spot = pl.ds(rows[d], nk)
            modes[spot, cols] = value
    loads[4].wait()
    sums = jnp.zeros((2 * nrhs, 2 * LANES), jnp.float32)
    for s in range(subs):
        cols = pl.ds(s * width, width)
        split = both(modes[:, cols])
        pair[:, cols] = split
        sums = sums + dot(both(mult[:, s, :]), split, NT)
    sums = quarters(sums)
    c_send[...] = sums
    c_recv[0, c] = sums

    pl.semaphore_wait(barrier, len(outer) + len(near) + len(inner))

    def c_copy(j, i):
        to = lax.rem(c + i, crs_size)
        return pltpu.make_async_remote_copy(
            src_ref=c_send, dst_ref=c_recv.at[j, c],
            send_sem=c_ssem.at[j, i], recv_sem=c_rsem.at[j, i],
            device_id=(groups[j], to), device_id_type=MESH)

    def c_wait(j, i):
        src = lax.rem(c + crs_size - i, crs_size)
        pltpu.make_async_remote_copy(
            src_ref=c_send, dst_ref=c_recv.at[j, src],
            send_sem=c_ssem.at[j, i], recv_sem=c_rsem.at[j, i],
            device_id=(groups[j], src), device_id_type=MESH).wait_recv()

    for j in (1, 2, 3, 0):
        for i in range(crs_size):
            if j or i:
                c_copy(j, i).start()

    def row(p, extra=0):
        return pl.multiple_of(p * part + extra, 8)

    def f_pieces(i):
        to = lax.rem(c + i, crs_size)
        nx = lax.rem(to + 1, crs_size)
        pv = lax.rem(to + crs_size - 1, crs_size)
        return to, (
            (row(to), 0, part, g),
            (row(nx), up, EDGE, g),
            (row(pv, part - EDGE), down, EDGE, g),
            (row(to), off_x, part, across),
            (row(to), off_p, part, after),
            (row(to), off_n, part, before),
        )

    def f_copy(i, n):
        to, pieces = f_pieces(i)
        start, place, size, where = pieces[n]
        return pltpu.make_async_remote_copy(
            src_ref=factor.at[pl.ds(start, size), :],
            dst_ref=fcat.at[c, pl.ds(place, size), :],
            send_sem=f_ssem.at[i, n], recv_sem=f_rsem.at[i, n],
            device_id=(where, to), device_id_type=MESH)

    def f_wait(i, n):
        to, pieces = f_pieces(i)
        start, place, size, where = pieces[n]
        src = lax.rem(c + crs_size - i, crs_size)
        pltpu.make_async_remote_copy(
            src_ref=factor.at[pl.ds(start, size), :],
            dst_ref=fcat.at[src, pl.ds(place, size), :],
            send_sem=f_ssem.at[i, n], recv_sem=f_rsem.at[i, n],
            device_id=(where, to), device_id_type=MESH).wait_recv()

    for other in outer:
        signal(met, other)

    loads[5].wait()
    span = LANES // part
    blocks = fown.shape[0]
    for b in range(blocks):
        held = factor[b * span * part:min((b + 1) * span, crs_size) * part, :]
        if held.shape[0] < LANES:
            held = jnp.concatenate(
                [held, jnp.zeros((LANES - held.shape[0], held.shape[1]), jnp.float32)], axis=0)
        fown[b] = both(held)

    for j in (0, 1, 2, 3):
        for i in range(crs_size):
            if j or i:
                c_wait(j, i)

    lane = lax.broadcasted_iota(jnp.int32, (nrhs, LANES), 1)

    def rolled(value, by):
        return pltpu.roll(value, (LANES - by) % LANES, 1) if by % LANES else value

    total = jnp.zeros((nrhs, factor.shape[1]), jnp.float32)
    for b in range(blocks):
        group_rhs = jnp.zeros((nrhs, LANES), jnp.float32)
        for p in range(b * span, min((b + 1) * span, crs_size)):
            at = (p - b * span) * part
            low = c_recv[0, (p - 1) % crs_size]
            high = c_recv[0, (p + 1) % crs_size]
            rhs = rolled(c_recv[0, p], -at)
            rhs = rhs + jnp.where(lane < at + EDGE, rolled(low, up - at), 0.0)
            rhs = rhs + jnp.where(
                lane >= at + part - EDGE, rolled(high, down - (at + part - EDGE)), 0.0)
            rhs = rhs + rolled(c_recv[1, p], off_x - at)
            rhs = rhs + rolled(c_recv[2, p], off_n - at)
            rhs = rhs + rolled(c_recv[3, p], off_p - at)
            group_rhs = jnp.where((lane >= at) & (lane < at + part), rhs, group_rhs)
        total = total + twice(group_rhs, fown[b])

    chunk = factor.shape[1] // parts
    for q in range(parts):
        for r in range(nrhs):
            rs_send[q * nrhs + r] = total[r:r + 1, q * chunk:(q + 1) * chunk]

    def rs_copy(i):
        to = lax.rem(g + i, sub_size)
        return pltpu.make_async_remote_copy(
            src_ref=rs_send.at[to], dst_ref=rs_recv.at[g],
            send_sem=rs_ssem.at[i], recv_sem=rs_rsem.at[i],
            device_id=(to, c), device_id_type=MESH)

    def rs_wait(i):
        src = lax.rem(g + sub_size - i, sub_size)
        pltpu.make_async_remote_copy(
            src_ref=rs_send.at[src], dst_ref=rs_recv.at[src],
            send_sem=rs_ssem.at[i], recv_sem=rs_rsem.at[i],
            device_id=(src, c), device_id_type=MESH).wait_recv()

    pl.semaphore_wait(met, len(outer))
    each(sub_size - 1, lambda i: rs_copy(i + 1).start())
    moves = [(i, n) for i in range(crs_size) for n in range(6) if i or n > 2]
    for i, n in moves:
        f_copy(i, n).start()
    _, pieces = f_pieces(0)
    for start, place, size, _ in pieces[:3]:
        fcat[c, pl.ds(place, size), :] = factor[pl.ds(start, size), :]

    rs_recv[g] = rs_send[g]
    each(sub_size - 1, lambda i: rs_wait(i + 1))
    mine = rs_recv[0]
    for q in range(1, sub_size):
        mine = mine + rs_recv[q]
    ag_send[...] = mine

    def ag_copy(i):
        return pltpu.make_async_remote_copy(
            src_ref=ag_send, dst_ref=panel.at[c, g],
            send_sem=ag_ssem.at[i], recv_sem=ag_rsem.at[i],
            device_id=rank(i), device_id_type=MESH)

    def ag_wait(i):
        fg, fcr = rank(devices - i)
        pltpu.make_async_remote_copy(
            src_ref=ag_send, dst_ref=panel.at[fcr, fg],
            send_sem=ag_ssem.at[i], recv_sem=ag_rsem.at[i],
            device_id=(fg, fcr), device_id_type=MESH).wait_recv()

    each(devices - 1, lambda i: ag_copy(i + 1).start())
    panel[c, g] = mine
    for i, n in moves:
        f_wait(i, n)
    for p in range(crs_size):
        fpair[p] = both(fcat[p])
    each(devices - 1, lambda i: ag_wait(i + 1))

    amps = jnp.zeros((2 * nrhs, 2 * LANES), jnp.float32)
    for p in range(crs_size):
        for q in range(parts):
            rows = panel[p, q * nrhs:(q + 1) * nrhs].reshape(nrhs, chunk)
            amps = amps + dot(both(rows), fpair[p, :, q * chunk:(q + 1) * chunk], NT)
    amps = quarters(amps)
    for s in range(subs):
        out_h[:, s, :] = twice(amps, pair[:, s * width:(s + 1) * width])

    for j in range(4):
        for i in range(crs_size):
            if j or i:
                c_copy(j, i).wait_send()
    for i, n in moves:
        f_copy(i, n).wait_send()
    each(sub_size - 1, lambda i: rs_copy(i + 1).wait_send())
    each(devices - 1, lambda i: ag_copy(i + 1).wait_send())


def wide_body(sub_size, crs_size, mult, own, nbr, face, nlist, factor):
    nk, subs, width = own.shape
    nrhs = mult.shape[0]
    part = nk * subs
    blocks = -(-crs_size // (LANES // part))
    cols = factor.shape[1]
    chunk = cols * nrhs // sub_size
    f32 = jnp.float32
    dma = pltpu.SemaphoreType.DMA
    bf16 = jnp.bfloat16
    hbm = pl.BlockSpec(memory_space=pl.ANY)
    names = nlist.T
    applied = pl.pallas_call(
        functools.partial(wide_kernel, sub_size, crs_size),
        out_shape=pltpu.VMEM(mult.shape, mult.dtype),
        in_specs=[hbm] * 6,
        out_specs=pl.BlockSpec(memory_space=pltpu.VMEM),
        scratch_shapes=[
            pltpu.VMEM(mult.shape, f32), pltpu.VMEM(own.shape, f32), pltpu.VMEM(nbr.shape, f32),
            pltpu.VMEM(face.shape, face.dtype), pltpu.SMEM(names.shape, names.dtype),
            pltpu.VMEM(factor.shape, f32),
            pltpu.VMEM((LANES, subs * width), f32),
            pltpu.VMEM((2 * LANES, subs * width), bf16),
            pltpu.VMEM((nrhs, LANES), f32),
            pltpu.VMEM((4, crs_size, nrhs, LANES), f32),
            pltpu.VMEM((crs_size, LANES, cols), f32),
            pltpu.VMEM((blocks, 2 * LANES, cols), bf16),
            pltpu.VMEM((crs_size, 2 * LANES, cols), bf16),
            pltpu.VMEM((sub_size, 1, chunk), f32),
            pltpu.VMEM((sub_size, 1, chunk), f32),
            pltpu.VMEM((1, chunk), f32),
            pltpu.VMEM((crs_size, sub_size, 1, chunk), f32),
            dma((4, crs_size)), dma((4, crs_size)),
            dma((crs_size, 6)), dma((crs_size, 6)),
            dma((sub_size,)), dma((sub_size,)),
            dma((sub_size * crs_size,)), dma((sub_size * crs_size,)), dma((6,)),
            pltpu.SemaphoreType.REGULAR,
        ],
        compiler_params=pltpu.CompilerParams(collective_id=0, has_side_effects=True),
    )(mult, own, nbr, face, names, factor)
    return mult - applied


def body(sub_size, crs_size, mult, own, nbr, face, nlist, factor):
    slabs = crs_size * factor.shape[1] // LANES
    fits = slabs <= 6 and factor.shape[1] % LANES == 0 and 12 <= sub_size <= LANES // 4
    form = near_body if fits else wide_body
    return form(sub_size, crs_size, mult, own, nbr, face, nlist, factor)


def solution(mesh):
    placed = (
        P(None, ("sub", "crs"), None),
        P(None, ("sub", "crs"), None),
        P(None, ("sub", "crs"), None),
        P(("sub", "crs"), None),
        P(),
        P("sub", "crs"),
    )
    return jax.shard_map(
        functools.partial(body, mesh.shape["sub"], mesh.shape["crs"]),
        mesh=mesh, in_specs=placed, out_specs=P(None, ("sub", "crs"), None), check_vma=False
    )
```

```python
import functools

import jax
import jax.numpy as jnp
from jax import lax
from jax.experimental import pallas as pl
from jax.experimental.pallas import tpu as pltpu
from jax.sharding import PartitionSpec as P

MESH = pl.DeviceIdType.MESH
NT = (((1,), (1,)), ((), ()))
NN = (((1,), (0,)), ((), ()))
LANES = 128
EDGE = 8


def each(count, step):
    if count <= 64:
        for i in sorted(range(count), key=lambda i: min(i, count - 1 - i)):
            step(i)
    else:
        lax.fori_loop(0, count, lambda i, t: (step(i), t)[1], 0)


def both(value, axis=0):
    high = value.astype(jnp.bfloat16)
    low = (value - high.astype(jnp.float32)).astype(jnp.bfloat16)
    return jnp.concatenate([high, low], axis=axis)


def halves(value):
    rows = value.shape[0] // 2
    return value[:rows] + value[rows:]


def quarters(value):
    value = halves(value)
    cols = value.shape[1] // 2
    return value[:, :cols] + value[:, cols:]


def dot(left, right, dims):
    return lax.dot_general(left, right, dims, preferred_element_type=jnp.float32)


def twice(left, right):
    high = left.astype(jnp.bfloat16)
    low = (left - high.astype(jnp.float32)).astype(jnp.bfloat16)
    wide = jnp.concatenate(
        [jnp.concatenate([high, high], axis=1), jnp.concatenate([low, low], axis=1)], axis=0)
    return halves(dot(wide, right, NN))


def homes_of(sub_size, slabs):
    q = sub_size // 4
    return (q, 2 * q + 2, q + 2, 2 * q + 1, q + 1, 2 * q)[:slabs]


WAVES = 4
N2, N3 = 2, 2


def parted(value):
    high = value.astype(jnp.bfloat16).astype(jnp.float32)
    return high, value - high


def near_kernel(
    sub_size, crs_size,
    mult_h, own_h, nbr_h, face_h, nlist_h, factor_h, out_h,
    mult, own, nbr, face, nlist, factor,
    modes, pair, s_send, s_recv, e_rows, slab, high, low, a_send, a_recv,
    in_sem, f_ssem, f_rsem, s_ssem, s_rsem, a_ssem, a_rsem,
):
    nk, subs, width = own.shape
    nrhs = mult.shape[0]
    nface = nlist.shape[0]
    part = nk * subs
    held = part * crs_size
    tiles = factor.shape[1] // LANES
    slabs = crs_size * tiles
    row_len = sub_size // 2
    group = subs * crs_size
    devices = sub_size * crs_size
    head = crs_size - 1
    wave = sub_size // WAVES
    homes = homes_of(sub_size, slabs)
    g = lax.axis_index("sub")
    c = lax.axis_index("crs")
    me = g * crs_size + c
    owns = jnp.full((), False)
    mine = jnp.zeros((), jnp.int32)
    for j, home in enumerate(homes):
        owns = jnp.logical_or(owns, g == home)
        mine = jnp.where(g == home, j, mine)
    is_owner = jnp.logical_and(c == head, owns)
    is_plain = jnp.logical_not(is_owner)
    keeps = jnp.logical_and(is_owner, mine >= head * tiles)
    far = 2 * held
    edge = far + part

    def around(g):
        first, second = g // row_len, g % row_len
        return (
            (first + 1) % 2 * row_len + second,
            first * row_len + (second + 1) % row_len,
            first * row_len + (second + row_len - 1) % row_len,
        )

    def landed(ref, semaphore):
        pltpu.make_async_copy(ref, ref, semaphore).wait()

    barrier = pltpu.get_barrier_semaphore()

    @pl.when(is_owner)
    def _():
        for i in range(devices - 1):
            to = i + jnp.where(i >= me, 1, 0)
            pl.semaphore_signal(
                barrier, inc=1, device_id=(to // crs_size, lax.rem(to, crs_size)), device_id_type=MESH)

    loads = [
        pltpu.make_async_copy(a, b, in_sem.at[i]) for i, (a, b) in enumerate((
            (factor_h, factor), (nlist_h, nlist), (face_h, face), (nbr_h, nbr), (own_h, own),
            (mult_h, mult)))
    ]
    for load in loads:
        load.start()
    modes[edge:, :] = jnp.zeros((LANES - edge, modes.shape[1]), jnp.float32)

    @pl.when(is_owner)
    def _():
        for i in range(sub_size // 2):
            slab[i * LANES + far:(i + 1) * LANES, :] = jnp.zeros((LANES - far, LANES), jnp.float32)

    loads[0].wait()
    late = g >= sub_size // 2
    last = g >= sub_size - wave

    def meet():
        @pl.when(is_owner)
        def _():
            pl.semaphore_wait(barrier, slabs - 1)

        @pl.when(is_plain)
        def _():
            pl.semaphore_wait(barrier, slabs)

    def home_of(j):
        home = jnp.zeros((), jnp.int32)
        for i in range(slabs):
            home = jnp.where(j == i, homes[i], home)
        return home

    def tile_in(t):
        return factor.at[:, pl.ds(pl.multiple_of(t * LANES, LANES), LANES)]

    def f_copy(t, home):
        return pltpu.make_async_remote_copy(
            src_ref=tile_in(t),
            dst_ref=slab.at[pl.ds(pl.multiple_of(g // 2 * LANES + lax.rem(g, 2) * held, 8), held), :],
            send_sem=f_ssem, recv_sem=f_rsem,
            device_id=(home, head), device_id_type=MESH)

    def f_start(t):
        t = lax.rem(t + g, tiles)
        home = home_of(c * tiles + t)
        self_kept = jnp.logical_and(c == head, g == home)

        @pl.when(jnp.logical_not(self_kept))
        def _():
            f_copy(t, home).start()

        @pl.when(self_kept)
        def _():
            slab[pl.ds(pl.multiple_of(g // 2 * LANES + lax.rem(g, 2) * held, 8), held), :] = tile_in(t)[...]

    @pl.when(late)
    def _():
        meet()
        for t in range(N2):
            f_start(t)

    @pl.when(last)
    def _():
        for t in range(N2, N3):
            f_start(t)

    for load in loads[1:5]:
        load.wait()
    across, after, before = around(g)
    fc = face[...]
    first_sub = me * subs
    line = lax.broadcasted_iota(jnp.int32, (subs, width), 0)
    target = jnp.zeros((subs, width), jnp.int32)
    for f in range(nface):
        name = jnp.zeros((subs, width), jnp.int32)
        for s in range(subs):
            name = jnp.where(line == s, nlist[f, first_sub + s], name)
        target = jnp.where(fc == f, name, target)
    third = c * subs + line
    nxt = jnp.where(third == group - 1, 0, third + 1)
    prv = jnp.where(third == 0, group - 1, third - 1)

    def chosen(block, line):
        return jnp.where(target == block * group + line, 1.0, 0.0)

    masks = (
        chosen(g, nxt), chosen(g, prv),
        chosen(across, third), chosen(after, third), chosen(before, third),
    )
    here, there = lax.rem(g, 2) * held, lax.rem(g + 1, 2) * held
    mine_at, other_at = c * part, (1 - c) * part

    def block(*pieces):
        rows, at = [], 0
        for start, value in pieces:
            if start > at:
                rows.append(jnp.zeros((start - at, width), jnp.float32))
            rows.append(value)
            at = start + nk
        if at < part:
            rows.append(jnp.zeros((part - at, width), jnp.float32))
        return jnp.concatenate(rows, axis=0)

    for s in range(subs):
        own_s = own[:, s, :]
        nbr_s = nbr[:, s, :]
        to = [nbr_s * masks[d][s:s + 1, :] for d in range(5)]
        first_at, last_at = s == 0, s == subs - 1
        inner = [(nk * s, own_s)]
        if not last_at:
            inner.append((nk * (s + 1), to[0]))
        if not first_at:
            inner.insert(0, (nk * (s - 1), to[1]))
        outer = []
        if last_at:
            outer.append((0, to[0]))
        if first_at:
            outer.append((part - nk, to[1]))
        for base, value in (
            (here + mine_at, block(*inner)),
            (here + other_at, block(*outer)),
            (there + mine_at, block((nk * s, to[3]))),
            (there + other_at, block((nk * s, to[4]))),
            (far, block((nk * s, to[2]))),
        ):
            start = base if isinstance(base, int) else pl.multiple_of(base, 8)
            modes[pl.ds(start, part), pl.ds(s * width, width)] = value
    loads[5].wait()
    sums = jnp.zeros((2 * nrhs, 2 * LANES), jnp.float32)
    for s in range(subs):
        at = pl.ds(s * width, width)
        split = both(modes[:, at])
        pair[:, at] = split
        sums = sums + dot(both(mult[:, s, :]), split, NT)
    sums = quarters(sums)
    s_send[...] = sums
    pl.when(jnp.logical_not(late))(meet)

    def s_copy(j):
        return pltpu.make_async_remote_copy(
            src_ref=s_send, dst_ref=s_recv.at[me],
            send_sem=s_ssem, recv_sem=s_rsem.at[g // wave],
            device_id=(home_of(j), head), device_id_type=MESH)

    for j in range(slabs - 1):
        s_copy(j + jnp.where(jnp.logical_and(is_owner, j >= mine), 1, 0)).start()

    @pl.when(is_plain)
    def _():
        s_copy(slabs - 1).start()

    @pl.when(jnp.logical_not(late))
    def _():
        for t in range(N2):
            f_start(t)

    @pl.when(jnp.logical_not(last))
    def _():
        for t in range(N2, N3):
            f_start(t)

    for t in range(N3, tiles):
        f_start(t)

    def a_copy(d):
        return pltpu.make_async_remote_copy(
            src_ref=a_send.at[d], dst_ref=a_recv.at[mine],
            send_sem=a_ssem, recv_sem=a_rsem,
            device_id=(lax.div(d, crs_size), lax.rem(d, crs_size)), device_id_type=MESH)

    def a_group(start, stop):
        inside = jnp.logical_and(me >= start, me < stop)
        for d in range(start, stop - 1):
            a_copy(d + jnp.where(jnp.logical_and(inside, d >= me), 1, 0)).start()

        @pl.when(jnp.logical_not(inside))
        def _():
            a_copy(jnp.int32(stop - 1)).start()

    @pl.when(is_owner)
    def _():
        s_recv[me] = sums

        lane = lax.broadcasted_iota(jnp.int32, (nrhs, LANES), 1)
        rhs = [jnp.zeros((nrhs, LANES), jnp.float32)] * (sub_size // 2)

        def rows_of(d):
            b, p = d // crs_size, d % crs_size
            x, n, q = around(b)

            def take(block, start, size):
                at = block // 2 * LANES + block % 2 * held + start
                return jnp.concatenate([high[at:at + size, :], low[at:at + size, :]], axis=1)

            others = [take(n, p * part, part), take(q, p * part, part)]
            halves_of = [take(b, 0, held), jnp.concatenate(others if p == 0 else others[::-1], axis=0)]
            spare = jnp.zeros((LANES - edge, 2 * LANES), jnp.float32)
            return jnp.concatenate(
                (halves_of if b % 2 == 0 else halves_of[::-1]) + [take(x, p * part, part), spare], axis=0)

        def only(value, at, size):
            return jnp.where((lane >= at) & (lane < at + size), value, 0.0)

        def turned(value, by):
            return pltpu.roll(value, by % LANES, 1)

        order = (*range(WAVES - 2), WAVES - 1, WAVES - 2)
        for w in order:
            inside = g // wave == w
            count = wave * crs_size

            @pl.when(inside)
            def _():
                landed(s_recv.at[pl.ds(0, count - 1)], s_rsem.at[w])

            @pl.when(jnp.logical_not(inside))
            def _():
                landed(s_recv.at[pl.ds(0, count)], s_rsem.at[w])

            for b in range(w * wave, (w + 1) * wave):
                x, n, q = around(b)
                this, that = b % 2 * held, (b + 1) % 2 * held
                pair_sum = s_recv[b * crs_size] + s_recv[b * crs_size + 1]
                rhs[b // 2] = rhs[b // 2] + only(pair_sum, this, held)
                for p in range(crs_size):
                    value = s_recv[b * crs_size + p]
                    at, off = p * part, (1 - p) * part
                    rhs[n // 2] = rhs[n // 2] + only(value, that + at, part)
                    rhs[q // 2] = rhs[q // 2] + only(turned(value, at - off), that + at, part)
                    rhs[x // 2] = rhs[x // 2] + only(turned(value, this + at - far), this + at, part)
            if w == order[-2]:
                @pl.when(keeps)
                def _():
                    landed(slab.at[pl.ds(0, (sub_size - 1) * held), :], f_rsem)

                @pl.when(jnp.logical_not(keeps))
                def _():
                    landed(slab.at[pl.ds(0, sub_size * held), :], f_rsem)

                high[...], low[...] = parted(slab[...])
        for i, value in enumerate(rhs):
            at = pl.ds(i * LANES, LANES)
            e_rows[0:nrhs, at], e_rows[nrhs:2 * nrhs, at] = parted(value)
        split = jnp.concatenate([high[...], low[...]], axis=1)
        panel = quarters(dot(e_rows[...], split, NN))
        ph, pw = parted(panel)
        wide = jnp.concatenate(
            [jnp.concatenate([ph, ph], axis=1), jnp.concatenate([pw, pw], axis=1)], axis=0)
        first_rows = jnp.concatenate([rows_of(d) for d in range(crs_size)], axis=0)
        term = halves(dot(wide, first_rows, NT))
        for d in range(crs_size):
            a_send[d] = term[:, d * LANES:(d + 1) * LANES]
            a_copy(jnp.int32(d)).start()
        amps = halves(dot(wide, split, NT))
        tiled = [amps[:, i * LANES:(i + 1) * LANES] for i in range(sub_size // 2)]

        def form(d):
            b, p = d // crs_size, d % crs_size
            x, n, q = around(b)
            this, that = b % 2 * held, (b + 1) % 2 * held
            at, off = p * part, (1 - p) * part
            value = turned(tiled[x // 2], far - this - at)
            value = jnp.where((lane >= this) & (lane < this + held), tiled[b // 2], value)
            value = jnp.where((lane >= that + at) & (lane < that + at + part), tiled[n // 2], value)
            a_send[d] = jnp.where(
                (lane >= that + off) & (lane < that + off + part), turned(tiled[q // 2], off - at), value)

        quarter = devices // 4
        for start, stop in ((3 * quarter, devices), (2 * quarter, 3 * quarter), (2, quarter), (quarter, 2 * quarter)):
            for d in range(start, stop):
                form(d)
            a_group(start, stop)
        a_recv[mine] = a_send[me]
        landed(a_recv.at[pl.ds(0, slabs - 1)], a_rsem)

    @pl.when(is_plain)
    def _():
        landed(a_recv, a_rsem)

    amps = a_recv[0]
    for j in range(1, slabs):
        amps = amps + a_recv[j]
    for s in range(subs):
        out_h[:, s, :] = twice(amps, pair[:, s * width:(s + 1) * width])

    @pl.when(keeps)
    def _():
        landed(factor.at[:, 0:(tiles - 1) * LANES], f_ssem)

    @pl.when(jnp.logical_not(keeps))
    def _():
        landed(factor, f_ssem)

    @pl.when(is_owner)
    def _():
        landed(s_recv.at[pl.ds(0, slabs - 1)], s_ssem)
        landed(a_send.at[pl.ds(0, devices - 1)], a_ssem)

    @pl.when(is_plain)
    def _():
        landed(s_recv.at[pl.ds(0, slabs)], s_ssem)


def near_body(sub_size, crs_size, mult, own, nbr, face, nlist, factor):
    nk, subs, width = own.shape
    nrhs = mult.shape[0]
    cols = factor.shape[1]
    devices = sub_size * crs_size
    slabs = crs_size * cols // LANES
    order = sub_size * (LANES // 2)
    f32, bf16 = jnp.float32, jnp.bfloat16
    dma = pltpu.SemaphoreType.DMA
    hbm = pl.BlockSpec(memory_space=pl.ANY)
    names = nlist.T
    applied = pl.pallas_call(
        functools.partial(near_kernel, sub_size, crs_size),
        out_shape=pltpu.VMEM(mult.shape, mult.dtype),
        in_specs=[hbm] * 6,
        out_specs=pl.BlockSpec(memory_space=pltpu.VMEM),
        scratch_shapes=[
            pltpu.VMEM(mult.shape, f32), pltpu.VMEM(own.shape, f32), pltpu.VMEM(nbr.shape, f32),
            pltpu.VMEM(face.shape, face.dtype), pltpu.SMEM(names.shape, names.dtype),
            pltpu.VMEM(factor.shape, f32),
            pltpu.VMEM((LANES, subs * width), f32),
            pltpu.VMEM((2 * LANES, subs * width), bf16),
            pltpu.VMEM((nrhs, LANES), f32),
            pltpu.VMEM((devices, nrhs, LANES), f32),
            pltpu.VMEM((2 * nrhs, order), f32),
            pltpu.VMEM((order, LANES), f32),
            pltpu.VMEM((order, LANES), f32),
            pltpu.VMEM((order, LANES), f32),
            pltpu.VMEM((devices, nrhs, LANES), f32),
            pltpu.VMEM((slabs, nrhs, LANES), f32),
            dma((6,)), dma, dma, dma, dma((WAVES,)), dma, dma,
        ],
        compiler_params=pltpu.CompilerParams(collective_id=0, has_side_effects=True),
    )(mult, own, nbr, face, names, factor)
    return mult - applied


def wide_kernel(
    sub_size, crs_size,
    mult_h, own_h, nbr_h, face_h, nlist_h, factor_h, out_h,
    mult, own, nbr, face, nlist, factor,
    modes, pair, c_send, c_recv, fcat, fown, fpair, rs_send, rs_recv, ag_send, panel,
    c_ssem, c_rsem, f_ssem, f_rsem, rs_ssem, rs_rsem, ag_ssem, ag_rsem, in_sem, met,
):
    nk, subs, width = own.shape
    nrhs = mult.shape[0]
    nface = nlist.shape[0]
    part = nk * subs
    parts = sub_size // nrhs
    row_len = sub_size // 2
    group = subs * crs_size
    devices = sub_size * crs_size
    g = lax.axis_index("sub")
    c = lax.axis_index("crs")
    me = g * crs_size + c
    up, down = part, part + EDGE
    off_x = part + 2 * EDGE
    off_n, off_p = off_x + part, off_x + 2 * part

    def rank(i):
        other = lax.rem(me + i, devices)
        return (other // crs_size, lax.rem(other, crs_size))

    loads = [
        pltpu.make_async_copy(a, b, in_sem.at[i]) for i, (a, b) in enumerate((
            (nlist_h, nlist), (face_h, face), (nbr_h, nbr), (own_h, own),
            (mult_h, mult), (factor_h, factor)))
    ]
    for load in loads:
        load.start()
    barrier = pltpu.get_barrier_semaphore()
    first, second = g // row_len, lax.rem(g, row_len)
    across = lax.rem(first + 1, 2) * row_len + second
    after = first * row_len + lax.rem(second + 1, row_len)
    before = first * row_len + lax.rem(second + row_len - 1, row_len)
    groups = (g, across, after, before)

    block = 1 << (devices.bit_length() // 2)
    base = me // block * block
    inner = [base + lax.rem(me - base + i, block) for i in range(1, block)]
    outer = [lax.rem(me + i, devices) for i in range(block, devices, block)]
    near = [groups[j] * crs_size + lax.rem(c + i, crs_size)
            for j in range(4) for i in range(crs_size) if j or i]

    def signal(semaphore, other):
        pl.semaphore_signal(
            semaphore, inc=1, device_id=(other // crs_size, lax.rem(other, crs_size)),
            device_id_type=MESH)

    for other in outer + near + inner:
        signal(barrier, other)

    modes[...] = jnp.zeros_like(modes)
    fcat[:, down + EDGE + 3 * part:, :] = jnp.zeros(
        (crs_size, LANES - (down + EDGE + 3 * part), fcat.shape[2]), jnp.float32)
    for load in loads[:4]:
        load.wait()
    fc = face[...]
    first_sub = me * subs
    line = lax.broadcasted_iota(jnp.int32, (subs, width), 0)
    target = jnp.zeros((subs, width), jnp.int32)
    for f in range(nface):
        name = jnp.zeros((subs, width), jnp.int32)
        for s in range(subs):
            name = jnp.where(line == s, nlist[f, first_sub + s], name)
        target = jnp.where(fc == f, name, target)
    third = c * subs + line
    nxt = jnp.where(third == group - 1, 0, third + 1)
    prv = jnp.where(third == 0, group - 1, third - 1)

    def chosen(block, line):
        return jnp.where(target == block * group + line, 1.0, 0.0)

    masks = (
        chosen(g, nxt), chosen(g, prv),
        chosen(across, third), chosen(after, third), chosen(before, third),
    )
    for s in range(subs):
        cols = pl.ds(s * width, width)
        own_s = own[:, s, :]
        nbr_s = nbr[:, s, :]
        rows = (
            nk * (s + 1) if s < subs - 1 else up,
            nk * (s - 1) if s > 0 else down + EDGE - nk,
            off_x + nk * s, off_n + nk * s, off_p + nk * s,
        )
        modes[pl.ds(nk * s, nk), cols] = own_s
        for d in range(5):
            value = nbr_s * masks[d][s:s + 1, :]
            spot = pl.ds(rows[d], nk)
            modes[spot, cols] = value
    loads[4].wait()
    sums = jnp.zeros((2 * nrhs, 2 * LANES), jnp.float32)
    for s in range(subs):
        cols = pl.ds(s * width, width)
        split = both(modes[:, cols])
        pair[:, cols] = split
        sums = sums + dot(both(mult[:, s, :]), split, NT)
    sums = quarters(sums)
    c_send[...] = sums
    c_recv[0, c] = sums

    pl.semaphore_wait(barrier, len(outer) + len(near) + len(inner))

    def c_copy(j, i):
        to = lax.rem(c + i, crs_size)
        return pltpu.make_async_remote_copy(
            src_ref=c_send, dst_ref=c_recv.at[j, c],
            send_sem=c_ssem.at[j, i], recv_sem=c_rsem.at[j, i],
            device_id=(groups[j], to), device_id_type=MESH)

    def c_wait(j, i):
        src = lax.rem(c + crs_size - i, crs_size)
        pltpu.make_async_remote_copy(
            src_ref=c_send, dst_ref=c_recv.at[j, src],
            send_sem=c_ssem.at[j, i], recv_sem=c_rsem.at[j, i],
            device_id=(groups[j], src), device_id_type=MESH).wait_recv()

    for j in (1, 2, 3, 0):
        for i in range(crs_size):
            if j or i:
                c_copy(j, i).start()

    def row(p, extra=0):
        return pl.multiple_of(p * part + extra, 8)

    def f_pieces(i):
        to = lax.rem(c + i, crs_size)
        nx = lax.rem(to + 1, crs_size)
        pv = lax.rem(to + crs_size - 1, crs_size)
        return to, (
            (row(to), 0, part, g),
            (row(nx), up, EDGE, g),
            (row(pv, part - EDGE), down, EDGE, g),
            (row(to), off_x, part, across),
            (row(to), off_p, part, after),
            (row(to), off_n, part, before),
        )

    def f_copy(i, n):
        to, pieces = f_pieces(i)
        start, place, size, where = pieces[n]
        return pltpu.make_async_remote_copy(
            src_ref=factor.at[pl.ds(start, size), :],
            dst_ref=fcat.at[c, pl.ds(place, size), :],
            send_sem=f_ssem.at[i, n], recv_sem=f_rsem.at[i, n],
            device_id=(where, to), device_id_type=MESH)

    def f_wait(i, n):
        to, pieces = f_pieces(i)
        start, place, size, where = pieces[n]
        src = lax.rem(c + crs_size - i, crs_size)
        pltpu.make_async_remote_copy(
            src_ref=factor.at[pl.ds(start, size), :],
            dst_ref=fcat.at[src, pl.ds(place, size), :],
            send_sem=f_ssem.at[i, n], recv_sem=f_rsem.at[i, n],
            device_id=(where, to), device_id_type=MESH).wait_recv()

    for other in outer:
        signal(met, other)

    loads[5].wait()
    span = LANES // part
    blocks = fown.shape[0]
    for b in range(blocks):
        held = factor[b * span * part:min((b + 1) * span, crs_size) * part, :]
        if held.shape[0] < LANES:
            held = jnp.concatenate(
                [held, jnp.zeros((LANES - held.shape[0], held.shape[1]), jnp.float32)], axis=0)
        fown[b] = both(held)

    for j in (0, 1, 2, 3):
        for i in range(crs_size):
            if j or i:
                c_wait(j, i)

    lane = lax.broadcasted_iota(jnp.int32, (nrhs, LANES), 1)

    def rolled(value, by):
        return pltpu.roll(value, (LANES - by) % LANES, 1) if by % LANES else value

    total = jnp.zeros((nrhs, factor.shape[1]), jnp.float32)
    for b in range(blocks):
        group_rhs = jnp.zeros((nrhs, LANES), jnp.float32)
        for p in range(b * span, min((b + 1) * span, crs_size)):
            at = (p - b * span) * part
            low = c_recv[0, (p - 1) % crs_size]
            high = c_recv[0, (p + 1) % crs_size]
            rhs = rolled(c_recv[0, p], -at)
            rhs = rhs + jnp.where(lane < at + EDGE, rolled(low, up - at), 0.0)
            rhs = rhs + jnp.where(
                lane >= at + part - EDGE, rolled(high, down - (at + part - EDGE)), 0.0)
            rhs = rhs + rolled(c_recv[1, p], off_x - at)
            rhs = rhs + rolled(c_recv[2, p], off_n - at)
            rhs = rhs + rolled(c_recv[3, p], off_p - at)
            group_rhs = jnp.where((lane >= at) & (lane < at + part), rhs, group_rhs)
        total = total + twice(group_rhs, fown[b])

    chunk = factor.shape[1] // parts
    for q in range(parts):
        for r in range(nrhs):
            rs_send[q * nrhs + r] = total[r:r + 1, q * chunk:(q + 1) * chunk]

    def rs_copy(i):
        to = lax.rem(g + i, sub_size)
        return pltpu.make_async_remote_copy(
            src_ref=rs_send.at[to], dst_ref=rs_recv.at[g],
            send_sem=rs_ssem.at[i], recv_sem=rs_rsem.at[i],
            device_id=(to, c), device_id_type=MESH)

    def rs_wait(i):
        src = lax.rem(g + sub_size - i, sub_size)
        pltpu.make_async_remote_copy(
            src_ref=rs_send.at[src], dst_ref=rs_recv.at[src],
            send_sem=rs_ssem.at[i], recv_sem=rs_rsem.at[i],
            device_id=(src, c), device_id_type=MESH).wait_recv()

    pl.semaphore_wait(met, len(outer))
    each(sub_size - 1, lambda i: rs_copy(i + 1).start())
    moves = [(i, n) for i in range(crs_size) for n in range(6) if i or n > 2]
    for i, n in moves:
        f_copy(i, n).start()
    _, pieces = f_pieces(0)
    for start, place, size, _ in pieces[:3]:
        fcat[c, pl.ds(place, size), :] = factor[pl.ds(start, size), :]

    rs_recv[g] = rs_send[g]
    each(sub_size - 1, lambda i: rs_wait(i + 1))
    mine = rs_recv[0]
    for q in range(1, sub_size):
        mine = mine + rs_recv[q]
    ag_send[...] = mine

    def ag_copy(i):
        return pltpu.make_async_remote_copy(
            src_ref=ag_send, dst_ref=panel.at[c, g],
            send_sem=ag_ssem.at[i], recv_sem=ag_rsem.at[i],
            device_id=rank(i), device_id_type=MESH)

    def ag_wait(i):
        fg, fcr = rank(devices - i)
        pltpu.make_async_remote_copy(
            src_ref=ag_send, dst_ref=panel.at[fcr, fg],
            send_sem=ag_ssem.at[i], recv_sem=ag_rsem.at[i],
            device_id=(fg, fcr), device_id_type=MESH).wait_recv()

    each(devices - 1, lambda i: ag_copy(i + 1).start())
    panel[c, g] = mine
    for i, n in moves:
        f_wait(i, n)
    for p in range(crs_size):
        fpair[p] = both(fcat[p])
    each(devices - 1, lambda i: ag_wait(i + 1))

    amps = jnp.zeros((2 * nrhs, 2 * LANES), jnp.float32)
    for p in range(crs_size):
        for q in range(parts):
            rows = panel[p, q * nrhs:(q + 1) * nrhs].reshape(nrhs, chunk)
            amps = amps + dot(both(rows), fpair[p, :, q * chunk:(q + 1) * chunk], NT)
    amps = quarters(amps)
    for s in range(subs):
        out_h[:, s, :] = twice(amps, pair[:, s * width:(s + 1) * width])

    for j in range(4):
        for i in range(crs_size):
            if j or i:
                c_copy(j, i).wait_send()
    for i, n in moves:
        f_copy(i, n).wait_send()
    each(sub_size - 1, lambda i: rs_copy(i + 1).wait_send())
    each(devices - 1, lambda i: ag_copy(i + 1).wait_send())


def wide_body(sub_size, crs_size, mult, own, nbr, face, nlist, factor):
    nk, subs, width = own.shape
    nrhs = mult.shape[0]
    part = nk * subs
    blocks = -(-crs_size // (LANES // part))
    cols = factor.shape[1]
    chunk = cols * nrhs // sub_size
    f32 = jnp.float32
    dma = pltpu.SemaphoreType.DMA
    bf16 = jnp.bfloat16
    hbm = pl.BlockSpec(memory_space=pl.ANY)
    names = nlist.T
    applied = pl.pallas_call(
        functools.partial(wide_kernel, sub_size, crs_size),
        out_shape=pltpu.VMEM(mult.shape, mult.dtype),
        in_specs=[hbm] * 6,
        out_specs=pl.BlockSpec(memory_space=pltpu.VMEM),
        scratch_shapes=[
            pltpu.VMEM(mult.shape, f32), pltpu.VMEM(own.shape, f32), pltpu.VMEM(nbr.shape, f32),
            pltpu.VMEM(face.shape, face.dtype), pltpu.SMEM(names.shape, names.dtype),
            pltpu.VMEM(factor.shape, f32),
            pltpu.VMEM((LANES, subs * width), f32),
            pltpu.VMEM((2 * LANES, subs * width), bf16),
            pltpu.VMEM((nrhs, LANES), f32),
            pltpu.VMEM((4, crs_size, nrhs, LANES), f32),
            pltpu.VMEM((crs_size, LANES, cols), f32),
            pltpu.VMEM((blocks, 2 * LANES, cols), bf16),
            pltpu.VMEM((crs_size, 2 * LANES, cols), bf16),
            pltpu.VMEM((sub_size, 1, chunk), f32),
            pltpu.VMEM((sub_size, 1, chunk), f32),
            pltpu.VMEM((1, chunk), f32),
            pltpu.VMEM((crs_size, sub_size, 1, chunk), f32),
            dma((4, crs_size)), dma((4, crs_size)),
            dma((crs_size, 6)), dma((crs_size, 6)),
            dma((sub_size,)), dma((sub_size,)),
            dma((sub_size * crs_size,)), dma((sub_size * crs_size,)), dma((6,)),
            pltpu.SemaphoreType.REGULAR,
        ],
        compiler_params=pltpu.CompilerParams(collective_id=0, has_side_effects=True),
    )(mult, own, nbr, face, names, factor)
    return mult - applied


def body(sub_size, crs_size, mult, own, nbr, face, nlist, factor):
    slabs = crs_size * factor.shape[1] // LANES
    held = own.shape[0] * own.shape[1] * crs_size
    fits = (slabs <= 6 and crs_size == 2 and factor.shape[1] % LANES == 0 and held * 5 <= LANES * 2
            and 12 <= sub_size <= LANES // 4)
    form = near_body if fits else wide_body
    return form(sub_size, crs_size, mult, own, nbr, face, nlist, factor)


def solution(mesh):
    placed = (
        P(None, ("sub", "crs"), None),
        P(None, ("sub", "crs"), None),
        P(None, ("sub", "crs"), None),
        P(("sub", "crs"), None),
        P(),
        P("sub", "crs"),
    )
    return jax.shard_map(
        functools.partial(body, mesh.shape["sub"], mesh.shape["crs"]),
        mesh=mesh, in_specs=placed, out_specs=P(None, ("sub", "crs"), None), check_vma=False
    )
```

```python
import functools

import jax
import jax.numpy as jnp
from jax import lax
from jax.experimental import pallas as pl
from jax.experimental.pallas import tpu as pltpu
from jax.sharding import PartitionSpec as P

MESH = pl.DeviceIdType.MESH
NT = (((1,), (1,)), ((), ()))
NN = (((1,), (0,)), ((), ()))
LANES = 128
EDGE = 8


def each(count, step):
    if count <= 64:
        for i in sorted(range(count), key=lambda i: min(i, count - 1 - i)):
            step(i)
    else:
        lax.fori_loop(0, count, lambda i, t: (step(i), t)[1], 0)


def both(value, axis=0):
    high = value.astype(jnp.bfloat16)
    low = (value - high.astype(jnp.float32)).astype(jnp.bfloat16)
    return jnp.concatenate([high, low], axis=axis)


def halves(value):
    rows = value.shape[0] // 2
    return value[:rows] + value[rows:]


def quarters(value):
    value = halves(value)
    cols = value.shape[1] // 2
    return value[:, :cols] + value[:, cols:]


def dot(left, right, dims):
    return lax.dot_general(left, right, dims, preferred_element_type=jnp.float32)


def twice(left, right):
    high = left.astype(jnp.bfloat16)
    low = (left - high.astype(jnp.float32)).astype(jnp.bfloat16)
    wide = jnp.concatenate(
        [jnp.concatenate([high, high], axis=1), jnp.concatenate([low, low], axis=1)], axis=0)
    return halves(dot(wide, right, NN))


def homes_of(sub_size, slabs):
    q = sub_size // 4
    return (q, 2 * q + 2, q + 2, 2 * q + 1, q + 1, 2 * q)[:slabs]


N2, N3 = 2, 2


def parted(value):
    high = value.astype(jnp.bfloat16).astype(jnp.float32)
    return high, value - high


def near_kernel(
    sub_size, crs_size,
    mult_h, own_h, nbr_h, face_h, nlist_h, factor_h, out_h,
    mult, own, nbr, face, nlist, factor,
    modes, pair, s_send, s_recv, e_rows, slab, high, low, a_send, a_recv,
    in_sem, f_ssem, f_rsem, s_ssem, s_rsem, a_ssem, a_rsem,
):
    nk, subs, width = own.shape
    nrhs = mult.shape[0]
    nface = nlist.shape[0]
    part = nk * subs
    held = part * crs_size
    tiles = factor.shape[1] // LANES
    slabs = crs_size * tiles
    row_len = sub_size // 2
    group = subs * crs_size
    devices = sub_size * crs_size
    head = crs_size - 1
    homes = homes_of(sub_size, slabs)
    g = lax.axis_index("sub")
    c = lax.axis_index("crs")
    me = g * crs_size + c
    owns = jnp.full((), False)
    mine = jnp.zeros((), jnp.int32)
    for j, home in enumerate(homes):
        owns = jnp.logical_or(owns, g == home)
        mine = jnp.where(g == home, j, mine)
    is_owner = jnp.logical_and(c == head, owns)
    is_plain = jnp.logical_not(is_owner)
    keeps = jnp.logical_and(is_owner, mine >= head * tiles)
    far = 2 * held
    edge = far + part

    def around(g):
        first, second = g // row_len, g % row_len
        return (
            (first + 1) % 2 * row_len + second,
            first * row_len + (second + 1) % row_len,
            first * row_len + (second + row_len - 1) % row_len,
        )

    def landed(ref, semaphore):
        pltpu.make_async_copy(ref, ref, semaphore).wait()

    barrier = pltpu.get_barrier_semaphore()

    @pl.when(is_owner)
    def _():
        for i in range(devices - 1):
            to = i + jnp.where(i >= me, 1, 0)
            pl.semaphore_signal(
                barrier, inc=1, device_id=(to // crs_size, lax.rem(to, crs_size)), device_id_type=MESH)

    loads = [
        pltpu.make_async_copy(a, b, in_sem.at[i]) for i, a, b in (
            (0, factor_h, factor), (1, nlist_h, nlist), (2, face_h, face), (2, nbr_h, nbr),
            (2, own_h, own), (3, mult_h, mult))
    ]
    for load in loads:
        load.start()
    modes[edge:, :] = jnp.zeros((LANES - edge, modes.shape[1]), jnp.float32)

    @pl.when(is_owner)
    def _():
        for i in range(sub_size // 2):
            slab[i * LANES + far:(i + 1) * LANES, :] = jnp.zeros((LANES - far, LANES), jnp.float32)

    loads[0].wait()
    late = g >= sub_size // 2
    last = g >= sub_size - sub_size // 4

    def meet():
        @pl.when(is_owner)
        def _():
            pl.semaphore_wait(barrier, slabs - 1)

        @pl.when(is_plain)
        def _():
            pl.semaphore_wait(barrier, slabs)

    def home_of(j):
        home = jnp.zeros((), jnp.int32)
        for i in range(slabs):
            home = jnp.where(j == i, homes[i], home)
        return home

    def tile_in(t):
        return factor.at[:, pl.ds(pl.multiple_of(t * LANES, LANES), LANES)]

    def f_copy(t, home):
        return pltpu.make_async_remote_copy(
            src_ref=tile_in(t),
            dst_ref=slab.at[pl.ds(pl.multiple_of(g // 2 * LANES + lax.rem(g, 2) * held, 8), held), :],
            send_sem=f_ssem, recv_sem=f_rsem,
            device_id=(home, head), device_id_type=MESH)

    def f_start(t):
        t = lax.rem(t + g, tiles)
        home = home_of(c * tiles + t)
        self_kept = jnp.logical_and(c == head, g == home)

        @pl.when(jnp.logical_not(self_kept))
        def _():
            f_copy(t, home).start()

        @pl.when(self_kept)
        def _():
            slab[pl.ds(pl.multiple_of(g // 2 * LANES + lax.rem(g, 2) * held, 8), held), :] = tile_in(t)[...]

    @pl.when(late)
    def _():
        meet()
        for t in range(N2):
            f_start(t)

    @pl.when(last)
    def _():
        for t in range(N2, N3):
            f_start(t)

    loads[1].wait()
    landed(mult.at[pl.ds(0, 2 * nk + 1)], in_sem.at[2])
    across, after, before = around(g)
    fc = face[...]
    first_sub = me * subs
    line = lax.broadcasted_iota(jnp.int32, (subs, width), 0)
    target = jnp.zeros((subs, width), jnp.int32)
    for f in range(nface):
        name = jnp.zeros((subs, width), jnp.int32)
        for s in range(subs):
            name = jnp.where(line == s, nlist[f, first_sub + s], name)
        target = jnp.where(fc == f, name, target)
    third = c * subs + line
    nxt = jnp.where(third == group - 1, 0, third + 1)
    prv = jnp.where(third == 0, group - 1, third - 1)

    def chosen(block, line):
        return jnp.where(target == block * group + line, 1.0, 0.0)

    masks = (
        chosen(g, nxt), chosen(g, prv),
        chosen(across, third), chosen(after, third), chosen(before, third),
    )
    here, there = lax.rem(g, 2) * held, lax.rem(g + 1, 2) * held
    mine_at, other_at = c * part, (1 - c) * part

    def block(*pieces):
        rows, at = [], 0
        for start, value in pieces:
            if start > at:
                rows.append(jnp.zeros((start - at, width), jnp.float32))
            rows.append(value)
            at = start + nk
        if at < part:
            rows.append(jnp.zeros((part - at, width), jnp.float32))
        return jnp.concatenate(rows, axis=0)

    for s in range(subs):
        own_s = own[:, s, :]
        nbr_s = nbr[:, s, :]
        to = [nbr_s * masks[d][s:s + 1, :] for d in range(5)]
        first_at, last_at = s == 0, s == subs - 1
        inner = [(nk * s, own_s)]
        if not last_at:
            inner.append((nk * (s + 1), to[0]))
        if not first_at:
            inner.insert(0, (nk * (s - 1), to[1]))
        outer = []
        if last_at:
            outer.append((0, to[0]))
        if first_at:
            outer.append((part - nk, to[1]))
        for base, value in (
            (here + mine_at, block(*inner)),
            (here + other_at, block(*outer)),
            (there + mine_at, block((nk * s, to[3]))),
            (there + other_at, block((nk * s, to[4]))),
            (far, block((nk * s, to[2]))),
        ):
            start = base if isinstance(base, int) else pl.multiple_of(base, 8)
            modes[pl.ds(start, part), pl.ds(s * width, width)] = value
    loads[5].wait()
    sums = jnp.zeros((2 * nrhs, 2 * LANES), jnp.float32)
    for s in range(subs):
        at = pl.ds(s * width, width)
        split = both(modes[:, at])
        pair[:, at] = split
        sums = sums + dot(both(mult[:, s, :]), split, NT)
    sums = quarters(sums)
    s_send[...] = sums
    pl.when(jnp.logical_not(late))(meet)

    def s_copy(j):
        return pltpu.make_async_remote_copy(
            src_ref=s_send, dst_ref=s_recv.at[me],
            send_sem=s_ssem, recv_sem=s_rsem,
            device_id=(home_of(j), head), device_id_type=MESH)

    turn = jnp.where(is_owner, mine + 1, lax.rem(g, 2) * crs_size)
    for i in range(slabs - 1):
        s_copy(lax.rem(turn + i, slabs)).start()

    @pl.when(is_plain)
    def _():
        s_copy(lax.rem(turn + slabs - 1, slabs)).start()

    @pl.when(jnp.logical_not(late))
    def _():
        for t in range(N2):
            f_start(t)

    @pl.when(jnp.logical_not(last))
    def _():
        for t in range(N2, N3):
            f_start(t)

    for t in range(N3, tiles):
        f_start(t)

    def a_copy(d):
        return pltpu.make_async_remote_copy(
            src_ref=a_send.at[d], dst_ref=a_recv.at[mine],
            send_sem=a_ssem, recv_sem=a_rsem,
            device_id=(lax.div(d, crs_size), lax.rem(d, crs_size)), device_id_type=MESH)

    def a_group(start, stop):
        inside = jnp.logical_and(me >= start, me < stop)
        for d in range(start, stop - 1):
            a_copy(d + jnp.where(jnp.logical_and(inside, d >= me), 1, 0)).start()

        @pl.when(jnp.logical_not(inside))
        def _():
            a_copy(jnp.int32(stop - 1)).start()

    @pl.when(is_owner)
    def _():
        s_recv[me] = sums

        lane = lax.broadcasted_iota(jnp.int32, (nrhs, LANES), 1)
        rhs = [jnp.zeros((nrhs, LANES), jnp.float32)] * (sub_size // 2)

        def rows_of(d):
            b, p = d // crs_size, d % crs_size
            x, n, q = around(b)

            def take(block, start, size):
                at = block // 2 * LANES + block % 2 * held + start
                return jnp.concatenate([high[at:at + size, :], low[at:at + size, :]], axis=1)

            others = [take(n, p * part, part), take(q, p * part, part)]
            halves_of = [take(b, 0, held), jnp.concatenate(others if p == 0 else others[::-1], axis=0)]
            spare = jnp.zeros((LANES - edge, 2 * LANES), jnp.float32)
            return jnp.concatenate(
                (halves_of if b % 2 == 0 else halves_of[::-1]) + [take(x, p * part, part), spare], axis=0)

        def only(value, at, size):
            return jnp.where((lane >= at) & (lane < at + size), value, 0.0)

        def turned(value, by):
            return pltpu.roll(value, by % LANES, 1)

        @pl.when(keeps)
        def _():
            landed(slab.at[pl.ds(0, (sub_size - 1) * held), :], f_rsem)

        @pl.when(jnp.logical_not(keeps))
        def _():
            landed(slab.at[pl.ds(0, sub_size * held), :], f_rsem)

        high[...], low[...] = parted(slab[...])
        landed(s_recv.at[pl.ds(0, devices - 1)], s_rsem)
        for b in range(sub_size):
            x, n, q = around(b)
            this, that = b % 2 * held, (b + 1) % 2 * held
            pair_sum = s_recv[b * crs_size] + s_recv[b * crs_size + 1]
            rhs[b // 2] = rhs[b // 2] + only(pair_sum, this, held)
            for p in range(crs_size):
                value = s_recv[b * crs_size + p]
                at, off = p * part, (1 - p) * part
                rhs[n // 2] = rhs[n // 2] + only(value, that + at, part)
                rhs[q // 2] = rhs[q // 2] + only(turned(value, at - off), that + at, part)
                rhs[x // 2] = rhs[x // 2] + only(turned(value, this + at - far), this + at, part)
        for i, value in enumerate(rhs):
            at = pl.ds(i * LANES, LANES)
            e_rows[0:nrhs, at], e_rows[nrhs:2 * nrhs, at] = parted(value)
        split = jnp.concatenate([high[...], low[...]], axis=1)
        panel = quarters(dot(e_rows[...], split, NN))
        ph, pw = parted(panel)
        wide = jnp.concatenate(
            [jnp.concatenate([ph, ph], axis=1), jnp.concatenate([pw, pw], axis=1)], axis=0)
        first_rows = jnp.concatenate([rows_of(d) for d in range(crs_size)], axis=0)
        term = halves(dot(wide, first_rows, NT))
        for d in range(crs_size):
            a_send[d] = term[:, d * LANES:(d + 1) * LANES]
            a_copy(jnp.int32(d)).start()
        amps = halves(dot(wide, split, NT))
        tiled = [amps[:, i * LANES:(i + 1) * LANES] for i in range(sub_size // 2)]

        def form(d):
            b, p = d // crs_size, d % crs_size
            x, n, q = around(b)
            this, that = b % 2 * held, (b + 1) % 2 * held
            at, off = p * part, (1 - p) * part
            value = turned(tiled[x // 2], far - this - at)
            value = jnp.where((lane >= this) & (lane < this + held), tiled[b // 2], value)
            value = jnp.where((lane >= that + at) & (lane < that + at + part), tiled[n // 2], value)
            a_send[d] = jnp.where(
                (lane >= that + off) & (lane < that + off + part), turned(tiled[q // 2], off - at), value)

        quarter = devices // 4
        for start, stop in ((3 * quarter, devices), (2 * quarter, 3 * quarter), (2, quarter), (quarter, 2 * quarter)):
            for d in range(start, stop):
                form(d)
            a_group(start, stop)
        a_recv[mine] = a_send[me]
        landed(a_recv.at[pl.ds(0, slabs - 1)], a_rsem)

    @pl.when(is_plain)
    def _():
        landed(a_recv, a_rsem)

    amps = a_recv[0]
    for j in range(1, slabs):
        amps = amps + a_recv[j]
    for s in range(subs):
        out_h[:, s, :] = mult[:, s, :] - twice(amps, pair[:, s * width:(s + 1) * width])

    @pl.when(keeps)
    def _():
        landed(factor.at[:, 0:(tiles - 1) * LANES], f_ssem)

    @pl.when(jnp.logical_not(keeps))
    def _():
        landed(factor, f_ssem)

    @pl.when(is_owner)
    def _():
        landed(s_recv.at[pl.ds(0, slabs - 1)], s_ssem)
        landed(a_send.at[pl.ds(0, devices - 1)], a_ssem)

    @pl.when(is_plain)
    def _():
        landed(s_recv.at[pl.ds(0, slabs)], s_ssem)


def near_body(sub_size, crs_size, mult, own, nbr, face, nlist, factor):
    nk, subs, width = own.shape
    nrhs = mult.shape[0]
    cols = factor.shape[1]
    devices = sub_size * crs_size
    slabs = crs_size * cols // LANES
    order = sub_size * (LANES // 2)
    f32, bf16 = jnp.float32, jnp.bfloat16
    dma = pltpu.SemaphoreType.DMA
    hbm = pl.BlockSpec(memory_space=pl.ANY)
    names = nlist.T
    projected = pl.pallas_call(
        functools.partial(near_kernel, sub_size, crs_size),
        out_shape=pltpu.VMEM(mult.shape, mult.dtype),
        in_specs=[hbm] * 6,
        out_specs=pl.BlockSpec(memory_space=pltpu.VMEM),
        scratch_shapes=[
            pltpu.VMEM(mult.shape, f32), pltpu.VMEM(own.shape, f32), pltpu.VMEM(nbr.shape, f32),
            pltpu.VMEM(face.shape, face.dtype), pltpu.SMEM(names.shape, names.dtype),
            pltpu.VMEM(factor.shape, f32),
            pltpu.VMEM((LANES, subs * width), f32),
            pltpu.VMEM((2 * LANES, subs * width), bf16),
            pltpu.VMEM((nrhs, LANES), f32),
            pltpu.VMEM((devices, nrhs, LANES), f32),
            pltpu.VMEM((2 * nrhs, order), f32),
            pltpu.VMEM((order, LANES), f32),
            pltpu.VMEM((order, LANES), f32),
            pltpu.VMEM((order, LANES), f32),
            pltpu.VMEM((devices, nrhs, LANES), f32),
            pltpu.VMEM((slabs, nrhs, LANES), f32),
            dma((4,)), dma, dma, dma, dma, dma, dma,
        ],
        compiler_params=pltpu.CompilerParams(collective_id=0, has_side_effects=True),
    )(mult, own, nbr, face, names, factor)
    return projected


def wide_kernel(
    sub_size, crs_size,
    mult_h, own_h, nbr_h, face_h, nlist_h, factor_h, out_h,
    mult, own, nbr, face, nlist, factor,
    modes, pair, c_send, c_recv, fcat, fown, fpair, rs_send, rs_recv, ag_send, panel,
    c_ssem, c_rsem, f_ssem, f_rsem, rs_ssem, rs_rsem, ag_ssem, ag_rsem, in_sem, met,
):
    nk, subs, width = own.shape
    nrhs = mult.shape[0]
    nface = nlist.shape[0]
    part = nk * subs
    parts = sub_size // nrhs
    row_len = sub_size // 2
    group = subs * crs_size
    devices = sub_size * crs_size
    g = lax.axis_index("sub")
    c = lax.axis_index("crs")
    me = g * crs_size + c
    up, down = part, part + EDGE
    off_x = part + 2 * EDGE
    off_n, off_p = off_x + part, off_x + 2 * part

    def rank(i):
        other = lax.rem(me + i, devices)
        return (other // crs_size, lax.rem(other, crs_size))

    loads = [
        pltpu.make_async_copy(a, b, in_sem.at[i]) for i, (a, b) in enumerate((
            (nlist_h, nlist), (face_h, face), (nbr_h, nbr), (own_h, own),
            (mult_h, mult), (factor_h, factor)))
    ]
    for load in loads:
        load.start()
    barrier = pltpu.get_barrier_semaphore()
    first, second = g // row_len, lax.rem(g, row_len)
    across = lax.rem(first + 1, 2) * row_len + second
    after = first * row_len + lax.rem(second + 1, row_len)
    before = first * row_len + lax.rem(second + row_len - 1, row_len)
    groups = (g, across, after, before)

    block = 1 << (devices.bit_length() // 2)
    base = me // block * block
    inner = [base + lax.rem(me - base + i, block) for i in range(1, block)]
    outer = [lax.rem(me + i, devices) for i in range(block, devices, block)]
    near = [groups[j] * crs_size + lax.rem(c + i, crs_size)
            for j in range(4) for i in range(crs_size) if j or i]

    def signal(semaphore, other):
        pl.semaphore_signal(
            semaphore, inc=1, device_id=(other // crs_size, lax.rem(other, crs_size)),
            device_id_type=MESH)

    for other in outer + near + inner:
        signal(barrier, other)

    modes[...] = jnp.zeros_like(modes)
    fcat[:, down + EDGE + 3 * part:, :] = jnp.zeros(
        (crs_size, LANES - (down + EDGE + 3 * part), fcat.shape[2]), jnp.float32)
    for load in loads[:4]:
        load.wait()
    fc = face[...]
    first_sub = me * subs
    line = lax.broadcasted_iota(jnp.int32, (subs, width), 0)
    target = jnp.zeros((subs, width), jnp.int32)
    for f in range(nface):
        name = jnp.zeros((subs, width), jnp.int32)
        for s in range(subs):
            name = jnp.where(line == s, nlist[f, first_sub + s], name)
        target = jnp.where(fc == f, name, target)
    third = c * subs + line
    nxt = jnp.where(third == group - 1, 0, third + 1)
    prv = jnp.where(third == 0, group - 1, third - 1)

    def chosen(block, line):
        return jnp.where(target == block * group + line, 1.0, 0.0)

    masks = (
        chosen(g, nxt), chosen(g, prv),
        chosen(across, third), chosen(after, third), chosen(before, third),
    )
    for s in range(subs):
        cols = pl.ds(s * width, width)
        own_s = own[:, s, :]
        nbr_s = nbr[:, s, :]
        rows = (
            nk * (s + 1) if s < subs - 1 else up,
            nk * (s - 1) if s > 0 else down + EDGE - nk,
            off_x + nk * s, off_n + nk * s, off_p + nk * s,
        )
        modes[pl.ds(nk * s, nk), cols] = own_s
        for d in range(5):
            value = nbr_s * masks[d][s:s + 1, :]
            spot = pl.ds(rows[d], nk)
            modes[spot, cols] = value
    loads[4].wait()
    sums = jnp.zeros((2 * nrhs, 2 * LANES), jnp.float32)
    for s in range(subs):
        cols = pl.ds(s * width, width)
        split = both(modes[:, cols])
        pair[:, cols] = split
        sums = sums + dot(both(mult[:, s, :]), split, NT)
    sums = quarters(sums)
    c_send[...] = sums
    c_recv[0, c] = sums

    pl.semaphore_wait(barrier, len(outer) + len(near) + len(inner))

    def c_copy(j, i):
        to = lax.rem(c + i, crs_size)
        return pltpu.make_async_remote_copy(
            src_ref=c_send, dst_ref=c_recv.at[j, c],
            send_sem=c_ssem.at[j, i], recv_sem=c_rsem.at[j, i],
            device_id=(groups[j], to), device_id_type=MESH)

    def c_wait(j, i):
        src = lax.rem(c + crs_size - i, crs_size)
        pltpu.make_async_remote_copy(
            src_ref=c_send, dst_ref=c_recv.at[j, src],
            send_sem=c_ssem.at[j, i], recv_sem=c_rsem.at[j, i],
            device_id=(groups[j], src), device_id_type=MESH).wait_recv()

    for j in (1, 2, 3, 0):
        for i in range(crs_size):
            if j or i:
                c_copy(j, i).start()

    def row(p, extra=0):
        return pl.multiple_of(p * part + extra, 8)

    def f_pieces(i):
        to = lax.rem(c + i, crs_size)
        nx = lax.rem(to + 1, crs_size)
        pv = lax.rem(to + crs_size - 1, crs_size)
        return to, (
            (row(to), 0, part, g),
            (row(nx), up, EDGE, g),
            (row(pv, part - EDGE), down, EDGE, g),
            (row(to), off_x, part, across),
            (row(to), off_p, part, after),
            (row(to), off_n, part, before),
        )

    def f_copy(i, n):
        to, pieces = f_pieces(i)
        start, place, size, where = pieces[n]
        return pltpu.make_async_remote_copy(
            src_ref=factor.at[pl.ds(start, size), :],
            dst_ref=fcat.at[c, pl.ds(place, size), :],
            send_sem=f_ssem.at[i, n], recv_sem=f_rsem.at[i, n],
            device_id=(where, to), device_id_type=MESH)

    def f_wait(i, n):
        to, pieces = f_pieces(i)
        start, place, size, where = pieces[n]
        src = lax.rem(c + crs_size - i, crs_size)
        pltpu.make_async_remote_copy(
            src_ref=factor.at[pl.ds(start, size), :],
            dst_ref=fcat.at[src, pl.ds(place, size), :],
            send_sem=f_ssem.at[i, n], recv_sem=f_rsem.at[i, n],
            device_id=(where, to), device_id_type=MESH).wait_recv()

    for other in outer:
        signal(met, other)

    loads[5].wait()
    span = LANES // part
    blocks = fown.shape[0]
    for b in range(blocks):
        held = factor[b * span * part:min((b + 1) * span, crs_size) * part, :]
        if held.shape[0] < LANES:
            held = jnp.concatenate(
                [held, jnp.zeros((LANES - held.shape[0], held.shape[1]), jnp.float32)], axis=0)
        fown[b] = both(held)

    for j in (0, 1, 2, 3):
        for i in range(crs_size):
            if j or i:
                c_wait(j, i)

    lane = lax.broadcasted_iota(jnp.int32, (nrhs, LANES), 1)

    def rolled(value, by):
        return pltpu.roll(value, (LANES - by) % LANES, 1) if by % LANES else value

    total = jnp.zeros((nrhs, factor.shape[1]), jnp.float32)
    for b in range(blocks):
        group_rhs = jnp.zeros((nrhs, LANES), jnp.float32)
        for p in range(b * span, min((b + 1) * span, crs_size)):
            at = (p - b * span) * part
            low = c_recv[0, (p - 1) % crs_size]
            high = c_recv[0, (p + 1) % crs_size]
            rhs = rolled(c_recv[0, p], -at)
            rhs = rhs + jnp.where(lane < at + EDGE, rolled(low, up - at), 0.0)
            rhs = rhs + jnp.where(
                lane >= at + part - EDGE, rolled(high, down - (at + part - EDGE)), 0.0)
            rhs = rhs + rolled(c_recv[1, p], off_x - at)
            rhs = rhs + rolled(c_recv[2, p], off_n - at)
            rhs = rhs + rolled(c_recv[3, p], off_p - at)
            group_rhs = jnp.where((lane >= at) & (lane < at + part), rhs, group_rhs)
        total = total + twice(group_rhs, fown[b])

    chunk = factor.shape[1] // parts
    for q in range(parts):
        for r in range(nrhs):
            rs_send[q * nrhs + r] = total[r:r + 1, q * chunk:(q + 1) * chunk]

    def rs_copy(i):
        to = lax.rem(g + i, sub_size)
        return pltpu.make_async_remote_copy(
            src_ref=rs_send.at[to], dst_ref=rs_recv.at[g],
            send_sem=rs_ssem.at[i], recv_sem=rs_rsem.at[i],
            device_id=(to, c), device_id_type=MESH)

    def rs_wait(i):
        src = lax.rem(g + sub_size - i, sub_size)
        pltpu.make_async_remote_copy(
            src_ref=rs_send.at[src], dst_ref=rs_recv.at[src],
            send_sem=rs_ssem.at[i], recv_sem=rs_rsem.at[i],
            device_id=(src, c), device_id_type=MESH).wait_recv()

    pl.semaphore_wait(met, len(outer))
    each(sub_size - 1, lambda i: rs_copy(i + 1).start())
    moves = [(i, n) for i in range(crs_size) for n in range(6) if i or n > 2]
    for i, n in moves:
        f_copy(i, n).start()
    _, pieces = f_pieces(0)
    for start, place, size, _ in pieces[:3]:
        fcat[c, pl.ds(place, size), :] = factor[pl.ds(start, size), :]

    rs_recv[g] = rs_send[g]
    each(sub_size - 1, lambda i: rs_wait(i + 1))
    mine = rs_recv[0]
    for q in range(1, sub_size):
        mine = mine + rs_recv[q]
    ag_send[...] = mine

    def ag_copy(i):
        return pltpu.make_async_remote_copy(
            src_ref=ag_send, dst_ref=panel.at[c, g],
            send_sem=ag_ssem.at[i], recv_sem=ag_rsem.at[i],
            device_id=rank(i), device_id_type=MESH)

    def ag_wait(i):
        fg, fcr = rank(devices - i)
        pltpu.make_async_remote_copy(
            src_ref=ag_send, dst_ref=panel.at[fcr, fg],
            send_sem=ag_ssem.at[i], recv_sem=ag_rsem.at[i],
            device_id=(fg, fcr), device_id_type=MESH).wait_recv()

    each(devices - 1, lambda i: ag_copy(i + 1).start())
    panel[c, g] = mine
    for i, n in moves:
        f_wait(i, n)
    for p in range(crs_size):
        fpair[p] = both(fcat[p])
    each(devices - 1, lambda i: ag_wait(i + 1))

    amps = jnp.zeros((2 * nrhs, 2 * LANES), jnp.float32)
    for p in range(crs_size):
        for q in range(parts):
            rows = panel[p, q * nrhs:(q + 1) * nrhs].reshape(nrhs, chunk)
            amps = amps + dot(both(rows), fpair[p, :, q * chunk:(q + 1) * chunk], NT)
    amps = quarters(amps)
    for s in range(subs):
        out_h[:, s, :] = twice(amps, pair[:, s * width:(s + 1) * width])

    for j in range(4):
        for i in range(crs_size):
            if j or i:
                c_copy(j, i).wait_send()
    for i, n in moves:
        f_copy(i, n).wait_send()
    each(sub_size - 1, lambda i: rs_copy(i + 1).wait_send())
    each(devices - 1, lambda i: ag_copy(i + 1).wait_send())


def wide_body(sub_size, crs_size, mult, own, nbr, face, nlist, factor):
    nk, subs, width = own.shape
    nrhs = mult.shape[0]
    part = nk * subs
    blocks = -(-crs_size // (LANES // part))
    cols = factor.shape[1]
    chunk = cols * nrhs // sub_size
    f32 = jnp.float32
    dma = pltpu.SemaphoreType.DMA
    bf16 = jnp.bfloat16
    hbm = pl.BlockSpec(memory_space=pl.ANY)
    names = nlist.T
    applied = pl.pallas_call(
        functools.partial(wide_kernel, sub_size, crs_size),
        out_shape=pltpu.VMEM(mult.shape, mult.dtype),
        in_specs=[hbm] * 6,
        out_specs=pl.BlockSpec(memory_space=pltpu.VMEM),
        scratch_shapes=[
            pltpu.VMEM(mult.shape, f32), pltpu.VMEM(own.shape, f32), pltpu.VMEM(nbr.shape, f32),
            pltpu.VMEM(face.shape, face.dtype), pltpu.SMEM(names.shape, names.dtype),
            pltpu.VMEM(factor.shape, f32),
            pltpu.VMEM((LANES, subs * width), f32),
            pltpu.VMEM((2 * LANES, subs * width), bf16),
            pltpu.VMEM((nrhs, LANES), f32),
            pltpu.VMEM((4, crs_size, nrhs, LANES), f32),
            pltpu.VMEM((crs_size, LANES, cols), f32),
            pltpu.VMEM((blocks, 2 * LANES, cols), bf16),
            pltpu.VMEM((crs_size, 2 * LANES, cols), bf16),
            pltpu.VMEM((sub_size, 1, chunk), f32),
            pltpu.VMEM((sub_size, 1, chunk), f32),
            pltpu.VMEM((1, chunk), f32),
            pltpu.VMEM((crs_size, sub_size, 1, chunk), f32),
            dma((4, crs_size)), dma((4, crs_size)),
            dma((crs_size, 6)), dma((crs_size, 6)),
            dma((sub_size,)), dma((sub_size,)),
            dma((sub_size * crs_size,)), dma((sub_size * crs_size,)), dma((6,)),
            pltpu.SemaphoreType.REGULAR,
        ],
        compiler_params=pltpu.CompilerParams(collective_id=0, has_side_effects=True),
    )(mult, own, nbr, face, names, factor)
    return mult - applied


def body(sub_size, crs_size, mult, own, nbr, face, nlist, factor):
    slabs = crs_size * factor.shape[1] // LANES
    held = own.shape[0] * own.shape[1] * crs_size
    fits = (slabs <= 6 and crs_size == 2 and factor.shape[1] % LANES == 0 and held * 5 <= LANES * 2
            and 12 <= sub_size <= LANES // 4 and mult.shape[0] > 2 * own.shape[0])
    form = near_body if fits else wide_body
    return form(sub_size, crs_size, mult, own, nbr, face, nlist, factor)


def solution(mesh):
    placed = (
        P(None, ("sub", "crs"), None),
        P(None, ("sub", "crs"), None),
        P(None, ("sub", "crs"), None),
        P(("sub", "crs"), None),
        P(),
        P("sub", "crs"),
    )
    return jax.shard_map(
        functools.partial(body, mesh.shape["sub"], mesh.shape["crs"]),
        mesh=mesh, in_specs=placed, out_specs=P(None, ("sub", "crs"), None), check_vma=False
    )
```

```python
import functools

import jax
import jax.numpy as jnp
from jax import lax
from jax.experimental import pallas as pl
from jax.experimental.pallas import tpu as pltpu
from jax.sharding import PartitionSpec as P

MESH = pl.DeviceIdType.MESH
NT = (((1,), (1,)), ((), ()))
NN = (((1,), (0,)), ((), ()))
LANES = 128
EDGE = 8


def each(count, step):
    if count <= 64:
        for i in sorted(range(count), key=lambda i: min(i, count - 1 - i)):
            step(i)
    else:
        lax.fori_loop(0, count, lambda i, t: (step(i), t)[1], 0)


def both(value, axis=0):
    high = value.astype(jnp.bfloat16)
    low = (value - high.astype(jnp.float32)).astype(jnp.bfloat16)
    return jnp.concatenate([high, low], axis=axis)


def halves(value):
    rows = value.shape[0] // 2
    return value[:rows] + value[rows:]


def quarters(value):
    value = halves(value)
    cols = value.shape[1] // 2
    return value[:, :cols] + value[:, cols:]


def dot(left, right, dims):
    return lax.dot_general(left, right, dims, preferred_element_type=jnp.float32)


def twice(left, right):
    high = left.astype(jnp.bfloat16)
    low = (left - high.astype(jnp.float32)).astype(jnp.bfloat16)
    wide = jnp.concatenate(
        [jnp.concatenate([high, high], axis=1), jnp.concatenate([low, low], axis=1)], axis=0)
    return halves(dot(wide, right, NN))


def homes_of(sub_size, slabs):
    q = sub_size // 4
    return (q, 2 * q + 2, q + 2, 2 * q + 1, q + 1, 2 * q)[:slabs]


N2, N3 = 2, 2


def parted(value):
    high = value.astype(jnp.bfloat16).astype(jnp.float32)
    return high, value - high


def near_kernel(
    sub_size, crs_size,
    mult_h, own_h, nbr_h, face_h, nlist_h, factor_h, out_h,
    mult, own, nbr, face, nlist, factor,
    modes, pair, s_send, s_recv, slab, high, low, a_send, a_recv,
    in_sem, f_ssem, f_rsem, s_ssem, s_rsem, a_ssem, a_rsem,
):
    nk, subs, width = own.shape
    nrhs = mult.shape[0]
    nface = nlist.shape[0]
    part = nk * subs
    held = part * crs_size
    tiles = factor.shape[1] // LANES
    slabs = crs_size * tiles
    row_len = sub_size // 2
    group = subs * crs_size
    devices = sub_size * crs_size
    head = crs_size - 1
    homes = homes_of(sub_size, slabs)
    g = lax.axis_index("sub")
    c = lax.axis_index("crs")
    me = g * crs_size + c
    owns = jnp.full((), False)
    mine = jnp.zeros((), jnp.int32)
    for j, home in enumerate(homes):
        owns = jnp.logical_or(owns, g == home)
        mine = jnp.where(g == home, j, mine)
    is_owner = jnp.logical_and(c == head, owns)
    is_plain = jnp.logical_not(is_owner)
    keeps = jnp.logical_and(is_owner, mine >= head * tiles)
    far = 2 * held
    edge = far + part

    def around(g):
        first, second = g // row_len, g % row_len
        return (
            (first + 1) % 2 * row_len + second,
            first * row_len + (second + 1) % row_len,
            first * row_len + (second + row_len - 1) % row_len,
        )

    def landed(ref, semaphore):
        pltpu.make_async_copy(ref, ref, semaphore).wait()

    barrier = pltpu.get_barrier_semaphore()

    @pl.when(is_owner)
    def _():
        for i in range(devices - 1):
            to = i + jnp.where(i >= me, 1, 0)
            pl.semaphore_signal(
                barrier, inc=1, device_id=(to // crs_size, lax.rem(to, crs_size)), device_id_type=MESH)

    loads = [
        pltpu.make_async_copy(a, b, in_sem.at[i]) for i, a, b in (
            (0, factor_h, factor), (1, nlist_h, nlist), (2, face_h, face), (2, nbr_h, nbr),
            (2, own_h, own), (3, mult_h, mult))
    ]
    for load in loads:
        load.start()
    modes[edge:, :] = jnp.zeros((LANES - edge, modes.shape[1]), jnp.float32)

    @pl.when(is_owner)
    def _():
        for i in range(sub_size // 2):
            slab[i * LANES + far:(i + 1) * LANES, :] = jnp.zeros((LANES - far, LANES), jnp.float32)

    loads[0].wait()
    late = g >= sub_size // 2
    last = g >= sub_size - sub_size // 4

    def meet():
        @pl.when(is_owner)
        def _():
            pl.semaphore_wait(barrier, slabs - 1)

        @pl.when(is_plain)
        def _():
            pl.semaphore_wait(barrier, slabs)

    def home_of(j):
        home = jnp.zeros((), jnp.int32)
        for i in range(slabs):
            home = jnp.where(j == i, homes[i], home)
        return home

    def tile_in(t):
        return factor.at[:, pl.ds(pl.multiple_of(t * LANES, LANES), LANES)]

    def f_copy(t, home):
        return pltpu.make_async_remote_copy(
            src_ref=tile_in(t),
            dst_ref=slab.at[pl.ds(pl.multiple_of(g // 2 * LANES + lax.rem(g, 2) * held, 8), held), :],
            send_sem=f_ssem, recv_sem=f_rsem,
            device_id=(home, head), device_id_type=MESH)

    def f_start(t):
        t = lax.rem(t + g, tiles)
        home = home_of(c * tiles + t)
        self_kept = jnp.logical_and(c == head, g == home)

        @pl.when(jnp.logical_not(self_kept))
        def _():
            f_copy(t, home).start()

        @pl.when(self_kept)
        def _():
            slab[pl.ds(pl.multiple_of(g // 2 * LANES + lax.rem(g, 2) * held, 8), held), :] = tile_in(t)[...]

    @pl.when(late)
    def _():
        meet()
        for t in range(N2):
            f_start(t)

    @pl.when(last)
    def _():
        for t in range(N2, N3):
            f_start(t)

    loads[1].wait()
    landed(mult.at[pl.ds(0, 2 * nk + 1)], in_sem.at[2])
    across, after, before = around(g)
    fc = face[...]
    first_sub = me * subs
    line = lax.broadcasted_iota(jnp.int32, (subs, width), 0)
    target = jnp.zeros((subs, width), jnp.int32)
    for f in range(nface):
        name = jnp.zeros((subs, width), jnp.int32)
        for s in range(subs):
            name = jnp.where(line == s, nlist[f, first_sub + s], name)
        target = jnp.where(fc == f, name, target)
    third = c * subs + line
    nxt = jnp.where(third == group - 1, 0, third + 1)
    prv = jnp.where(third == 0, group - 1, third - 1)

    def chosen(block, line):
        return jnp.where(target == block * group + line, 1.0, 0.0)

    masks = (
        chosen(g, nxt), chosen(g, prv),
        chosen(across, third), chosen(after, third), chosen(before, third),
    )
    here, there = lax.rem(g, 2) * held, lax.rem(g + 1, 2) * held
    mine_at, other_at = c * part, (1 - c) * part

    def block(*pieces):
        rows, at = [], 0
        for start, value in pieces:
            if start > at:
                rows.append(jnp.zeros((start - at, width), jnp.float32))
            rows.append(value)
            at = start + nk
        if at < part:
            rows.append(jnp.zeros((part - at, width), jnp.float32))
        return jnp.concatenate(rows, axis=0)

    for s in range(subs):
        own_s = own[:, s, :]
        nbr_s = nbr[:, s, :]
        to = [nbr_s * masks[d][s:s + 1, :] for d in range(5)]
        first_at, last_at = s == 0, s == subs - 1
        inner = [(nk * s, own_s)]
        if not last_at:
            inner.append((nk * (s + 1), to[0]))
        if not first_at:
            inner.insert(0, (nk * (s - 1), to[1]))
        outer = []
        if last_at:
            outer.append((0, to[0]))
        if first_at:
            outer.append((part - nk, to[1]))
        for base, value in (
            (here + mine_at, block(*inner)),
            (here + other_at, block(*outer)),
            (there + mine_at, block((nk * s, to[3]))),
            (there + other_at, block((nk * s, to[4]))),
            (far, block((nk * s, to[2]))),
        ):
            start = base if isinstance(base, int) else pl.multiple_of(base, 8)
            modes[pl.ds(start, part), pl.ds(s * width, width)] = value
    loads[5].wait()
    sums = jnp.zeros((2 * nrhs, 2 * LANES), jnp.float32)
    for s in range(subs):
        at = pl.ds(s * width, width)
        split = both(modes[:, at])
        pair[:, at] = split
        sums = sums + dot(both(mult[:, s, :]), split, NT)
    sums = quarters(sums)
    s_send[...] = sums
    pl.when(jnp.logical_not(late))(meet)

    def s_copy(j):
        return pltpu.make_async_remote_copy(
            src_ref=s_send, dst_ref=s_recv.at[me],
            send_sem=s_ssem, recv_sem=s_rsem,
            device_id=(home_of(j), head), device_id_type=MESH)

    turn = jnp.where(is_owner, mine + 1, lax.rem(g, 2) * crs_size)
    for i in range(slabs - 1):
        s_copy(lax.rem(turn + i, slabs)).start()

    @pl.when(is_plain)
    def _():
        s_copy(lax.rem(turn + slabs - 1, slabs)).start()

    @pl.when(jnp.logical_not(late))
    def _():
        for t in range(N2):
            f_start(t)

    @pl.when(jnp.logical_not(last))
    def _():
        for t in range(N2, N3):
            f_start(t)

    for t in range(N3, tiles):
        f_start(t)

    def a_copy(d):
        return pltpu.make_async_remote_copy(
            src_ref=a_send.at[d], dst_ref=a_recv.at[mine],
            send_sem=a_ssem, recv_sem=a_rsem,
            device_id=(lax.div(d, crs_size), lax.rem(d, crs_size)), device_id_type=MESH)

    def a_group(start, stop):
        inside = jnp.logical_and(me >= start, me < stop)
        for d in range(start, stop - 1):
            a_copy(d + jnp.where(jnp.logical_and(inside, d >= me), 1, 0)).start()

        @pl.when(jnp.logical_not(inside))
        def _():
            a_copy(jnp.int32(stop - 1)).start()

    @pl.when(is_owner)
    def _():
        s_recv[me] = sums

        lane = lax.broadcasted_iota(jnp.int32, (nrhs, LANES), 1)
        rhs = [jnp.zeros((nrhs, LANES), jnp.float32)] * (sub_size // 2)

        def rows_of(d):
            b, p = d // crs_size, d % crs_size
            x, n, q = around(b)

            def take(block, start, size):
                at = block // 2 * LANES + block % 2 * held + start
                return jnp.concatenate([high[at:at + size, :], low[at:at + size, :]], axis=1)

            others = [take(n, p * part, part), take(q, p * part, part)]
            halves_of = [take(b, 0, held), jnp.concatenate(others if p == 0 else others[::-1], axis=0)]
            spare = jnp.zeros((LANES - edge, 2 * LANES), jnp.float32)
            return jnp.concatenate(
                (halves_of if b % 2 == 0 else halves_of[::-1]) + [take(x, p * part, part), spare], axis=0)

        def only(value, at, size):
            return jnp.where((lane >= at) & (lane < at + size), value, 0.0)

        def turned(value, by):
            return pltpu.roll(value, by % LANES, 1)

        @pl.when(keeps)
        def _():
            landed(slab.at[pl.ds(0, (sub_size - 1) * held), :], f_rsem)

        @pl.when(jnp.logical_not(keeps))
        def _():
            landed(slab.at[pl.ds(0, sub_size * held), :], f_rsem)

        high[...], low[...] = parted(slab[...])
        landed(s_recv.at[pl.ds(0, devices - 1)], s_rsem)
        for b in range(sub_size):
            x, n, q = around(b)
            this, that = b % 2 * held, (b + 1) % 2 * held
            pair_sum = s_recv[b * crs_size] + s_recv[b * crs_size + 1]
            rhs[b // 2] = rhs[b // 2] + only(pair_sum, this, held)
            for p in range(crs_size):
                value = s_recv[b * crs_size + p]
                at, off = p * part, (1 - p) * part
                rhs[n // 2] = rhs[n // 2] + only(value, that + at, part)
                rhs[q // 2] = rhs[q // 2] + only(turned(value, at - off), that + at, part)
                rhs[x // 2] = rhs[x // 2] + only(turned(value, this + at - far), this + at, part)
        rhs_rows = jnp.concatenate(parted(jnp.concatenate(rhs, axis=1)), axis=0)
        split = jnp.concatenate([high[...], low[...]], axis=1)
        panel = quarters(dot(rhs_rows, split, NN))
        ph, pw = parted(panel)
        wide = jnp.concatenate(
            [jnp.concatenate([ph, ph], axis=1), jnp.concatenate([pw, pw], axis=1)], axis=0)
        first_rows = jnp.concatenate([rows_of(d) for d in range(crs_size)], axis=0)
        term = halves(dot(wide, first_rows, NT))
        for d in range(crs_size):
            a_send[d] = term[:, d * LANES:(d + 1) * LANES]
            a_copy(jnp.int32(d)).start()
        amps = halves(dot(wide, split, NT))
        tiled = [amps[:, i * LANES:(i + 1) * LANES] for i in range(sub_size // 2)]

        def form(d):
            b, p = d // crs_size, d % crs_size
            x, n, q = around(b)
            this, that = b % 2 * held, (b + 1) % 2 * held
            at, off = p * part, (1 - p) * part
            value = turned(tiled[x // 2], far - this - at)
            value = jnp.where((lane >= this) & (lane < this + held), tiled[b // 2], value)
            value = jnp.where((lane >= that + at) & (lane < that + at + part), tiled[n // 2], value)
            a_send[d] = jnp.where(
                (lane >= that + off) & (lane < that + off + part), turned(tiled[q // 2], off - at), value)

        quarter = devices // 4
        for start, stop in ((3 * quarter, devices), (2 * quarter, 3 * quarter), (2, quarter), (quarter, 2 * quarter)):
            for d in range(start, stop):
                form(d)
            a_group(start, stop)
        a_recv[mine] = a_send[me]
        landed(a_recv.at[pl.ds(0, slabs - 1)], a_rsem)

    @pl.when(is_plain)
    def _():
        landed(a_recv, a_rsem)

    amps = a_recv[0]
    for j in range(1, slabs):
        amps = amps + a_recv[j]
    for s in range(subs):
        out_h[:, s, :] = mult[:, s, :] - twice(amps, pair[:, s * width:(s + 1) * width])

    @pl.when(keeps)
    def _():
        landed(factor.at[:, 0:(tiles - 1) * LANES], f_ssem)

    @pl.when(jnp.logical_not(keeps))
    def _():
        landed(factor, f_ssem)

    @pl.when(is_owner)
    def _():
        landed(s_recv.at[pl.ds(0, slabs - 1)], s_ssem)
        landed(a_send.at[pl.ds(0, devices - 1)], a_ssem)

    @pl.when(is_plain)
    def _():
        landed(s_recv.at[pl.ds(0, slabs)], s_ssem)


def near_body(sub_size, crs_size, mult, own, nbr, face, nlist, factor):
    nk, subs, width = own.shape
    nrhs = mult.shape[0]
    cols = factor.shape[1]
    devices = sub_size * crs_size
    slabs = crs_size * cols // LANES
    order = sub_size * (LANES // 2)
    f32, bf16 = jnp.float32, jnp.bfloat16
    dma = pltpu.SemaphoreType.DMA
    hbm = pl.BlockSpec(memory_space=pl.ANY)
    names = nlist.T
    projected = pl.pallas_call(
        functools.partial(near_kernel, sub_size, crs_size),
        out_shape=pltpu.VMEM(mult.shape, mult.dtype),
        in_specs=[hbm] * 6,
        out_specs=pl.BlockSpec(memory_space=pltpu.VMEM),
        scratch_shapes=[
            pltpu.VMEM(mult.shape, f32), pltpu.VMEM(own.shape, f32), pltpu.VMEM(nbr.shape, f32),
            pltpu.VMEM(face.shape, face.dtype), pltpu.SMEM(names.shape, names.dtype),
            pltpu.VMEM(factor.shape, f32),
            pltpu.VMEM((LANES, subs * width), f32),
            pltpu.VMEM((2 * LANES, subs * width), bf16),
            pltpu.VMEM((nrhs, LANES), f32),
            pltpu.VMEM((devices, nrhs, LANES), f32),
            pltpu.VMEM((order, LANES), f32),
            pltpu.VMEM((order, LANES), f32),
            pltpu.VMEM((order, LANES), f32),
            pltpu.VMEM((devices, nrhs, LANES), f32),
            pltpu.VMEM((slabs, nrhs, LANES), f32),
            dma((4,)), dma, dma, dma, dma, dma, dma,
        ],
        compiler_params=pltpu.CompilerParams(collective_id=0, has_side_effects=True),
    )(mult, own, nbr, face, names, factor)
    return projected


def wide_kernel(
    sub_size, crs_size,
    mult_h, own_h, nbr_h, face_h, nlist_h, factor_h, out_h,
    mult, own, nbr, face, nlist, factor,
    modes, pair, c_send, c_recv, fcat, fown, fpair, rs_send, rs_recv, ag_send, panel,
    c_ssem, c_rsem, f_ssem, f_rsem, rs_ssem, rs_rsem, ag_ssem, ag_rsem, in_sem, met,
):
    nk, subs, width = own.shape
    nrhs = mult.shape[0]
    nface = nlist.shape[0]
    part = nk * subs
    parts = sub_size // nrhs
    row_len = sub_size // 2
    group = subs * crs_size
    devices = sub_size * crs_size
    g = lax.axis_index("sub")
    c = lax.axis_index("crs")
    me = g * crs_size + c
    up, down = part, part + EDGE
    off_x = part + 2 * EDGE
    off_n, off_p = off_x + part, off_x + 2 * part

    def rank(i):
        other = lax.rem(me + i, devices)
        return (other // crs_size, lax.rem(other, crs_size))

    loads = [
        pltpu.make_async_copy(a, b, in_sem.at[i]) for i, (a, b) in enumerate((
            (nlist_h, nlist), (face_h, face), (nbr_h, nbr), (own_h, own),
            (mult_h, mult), (factor_h, factor)))
    ]
    for load in loads:
        load.start()
    barrier = pltpu.get_barrier_semaphore()
    first, second = g // row_len, lax.rem(g, row_len)
    across = lax.rem(first + 1, 2) * row_len + second
    after = first * row_len + lax.rem(second + 1, row_len)
    before = first * row_len + lax.rem(second + row_len - 1, row_len)
    groups = (g, across, after, before)

    block = 1 << (devices.bit_length() // 2)
    base = me // block * block
    inner = [base + lax.rem(me - base + i, block) for i in range(1, block)]
    outer = [lax.rem(me + i, devices) for i in range(block, devices, block)]
    near = [groups[j] * crs_size + lax.rem(c + i, crs_size)
            for j in range(4) for i in range(crs_size) if j or i]

    def signal(semaphore, other):
        pl.semaphore_signal(
            semaphore, inc=1, device_id=(other // crs_size, lax.rem(other, crs_size)),
            device_id_type=MESH)

    for other in outer + near + inner:
        signal(barrier, other)

    modes[...] = jnp.zeros_like(modes)
    fcat[:, down + EDGE + 3 * part:, :] = jnp.zeros(
        (crs_size, LANES - (down + EDGE + 3 * part), fcat.shape[2]), jnp.float32)
    for load in loads[:4]:
        load.wait()
    fc = face[...]
    first_sub = me * subs
    line = lax.broadcasted_iota(jnp.int32, (subs, width), 0)
    target = jnp.zeros((subs, width), jnp.int32)
    for f in range(nface):
        name = jnp.zeros((subs, width), jnp.int32)
        for s in range(subs):
            name = jnp.where(line == s, nlist[f, first_sub + s], name)
        target = jnp.where(fc == f, name, target)
    third = c * subs + line
    nxt = jnp.where(third == group - 1, 0, third + 1)
    prv = jnp.where(third == 0, group - 1, third - 1)

    def chosen(block, line):
        return jnp.where(target == block * group + line, 1.0, 0.0)

    masks = (
        chosen(g, nxt), chosen(g, prv),
        chosen(across, third), chosen(after, third), chosen(before, third),
    )
    for s in range(subs):
        cols = pl.ds(s * width, width)
        own_s = own[:, s, :]
        nbr_s = nbr[:, s, :]
        rows = (
            nk * (s + 1) if s < subs - 1 else up,
            nk * (s - 1) if s > 0 else down + EDGE - nk,
            off_x + nk * s, off_n + nk * s, off_p + nk * s,
        )
        modes[pl.ds(nk * s, nk), cols] = own_s
        for d in range(5):
            value = nbr_s * masks[d][s:s + 1, :]
            spot = pl.ds(rows[d], nk)
            modes[spot, cols] = value
    loads[4].wait()
    sums = jnp.zeros((2 * nrhs, 2 * LANES), jnp.float32)
    for s in range(subs):
        cols = pl.ds(s * width, width)
        split = both(modes[:, cols])
        pair[:, cols] = split
        sums = sums + dot(both(mult[:, s, :]), split, NT)
    sums = quarters(sums)
    c_send[...] = sums
    c_recv[0, c] = sums

    pl.semaphore_wait(barrier, len(outer) + len(near) + len(inner))

    def c_copy(j, i):
        to = lax.rem(c + i, crs_size)
        return pltpu.make_async_remote_copy(
            src_ref=c_send, dst_ref=c_recv.at[j, c],
            send_sem=c_ssem.at[j, i], recv_sem=c_rsem.at[j, i],
            device_id=(groups[j], to), device_id_type=MESH)

    def c_wait(j, i):
        src = lax.rem(c + crs_size - i, crs_size)
        pltpu.make_async_remote_copy(
            src_ref=c_send, dst_ref=c_recv.at[j, src],
            send_sem=c_ssem.at[j, i], recv_sem=c_rsem.at[j, i],
            device_id=(groups[j], src), device_id_type=MESH).wait_recv()

    for j in (1, 2, 3, 0):
        for i in range(crs_size):
            if j or i:
                c_copy(j, i).start()

    def row(p, extra=0):
        return pl.multiple_of(p * part + extra, 8)

    def f_pieces(i):
        to = lax.rem(c + i, crs_size)
        nx = lax.rem(to + 1, crs_size)
        pv = lax.rem(to + crs_size - 1, crs_size)
        return to, (
            (row(to), 0, part, g),
            (row(nx), up, EDGE, g),
            (row(pv, part - EDGE), down, EDGE, g),
            (row(to), off_x, part, across),
            (row(to), off_p, part, after),
            (row(to), off_n, part, before),
        )

    def f_copy(i, n):
        to, pieces = f_pieces(i)
        start, place, size, where = pieces[n]
        return pltpu.make_async_remote_copy(
            src_ref=factor.at[pl.ds(start, size), :],
            dst_ref=fcat.at[c, pl.ds(place, size), :],
            send_sem=f_ssem.at[i, n], recv_sem=f_rsem.at[i, n],
            device_id=(where, to), device_id_type=MESH)

    def f_wait(i, n):
        to, pieces = f_pieces(i)
        start, place, size, where = pieces[n]
        src = lax.rem(c + crs_size - i, crs_size)
        pltpu.make_async_remote_copy(
            src_ref=factor.at[pl.ds(start, size), :],
            dst_ref=fcat.at[src, pl.ds(place, size), :],
            send_sem=f_ssem.at[i, n], recv_sem=f_rsem.at[i, n],
            device_id=(where, to), device_id_type=MESH).wait_recv()

    for other in outer:
        signal(met, other)

    loads[5].wait()
    span = LANES // part
    blocks = fown.shape[0]
    for b in range(blocks):
        held = factor[b * span * part:min((b + 1) * span, crs_size) * part, :]
        if held.shape[0] < LANES:
            held = jnp.concatenate(
                [held, jnp.zeros((LANES - held.shape[0], held.shape[1]), jnp.float32)], axis=0)
        fown[b] = both(held)

    for j in (0, 1, 2, 3):
        for i in range(crs_size):
            if j or i:
                c_wait(j, i)

    lane = lax.broadcasted_iota(jnp.int32, (nrhs, LANES), 1)

    def rolled(value, by):
        return pltpu.roll(value, (LANES - by) % LANES, 1) if by % LANES else value

    total = jnp.zeros((nrhs, factor.shape[1]), jnp.float32)
    for b in range(blocks):
        group_rhs = jnp.zeros((nrhs, LANES), jnp.float32)
        for p in range(b * span, min((b + 1) * span, crs_size)):
            at = (p - b * span) * part
            low = c_recv[0, (p - 1) % crs_size]
            high = c_recv[0, (p + 1) % crs_size]
            rhs = rolled(c_recv[0, p], -at)
            rhs = rhs + jnp.where(lane < at + EDGE, rolled(low, up - at), 0.0)
            rhs = rhs + jnp.where(
                lane >= at + part - EDGE, rolled(high, down - (at + part - EDGE)), 0.0)
            rhs = rhs + rolled(c_recv[1, p], off_x - at)
            rhs = rhs + rolled(c_recv[2, p], off_n - at)
            rhs = rhs + rolled(c_recv[3, p], off_p - at)
            group_rhs = jnp.where((lane >= at) & (lane < at + part), rhs, group_rhs)
        total = total + twice(group_rhs, fown[b])

    chunk = factor.shape[1] // parts
    for q in range(parts):
        for r in range(nrhs):
            rs_send[q * nrhs + r] = total[r:r + 1, q * chunk:(q + 1) * chunk]

    def rs_copy(i):
        to = lax.rem(g + i, sub_size)
        return pltpu.make_async_remote_copy(
            src_ref=rs_send.at[to], dst_ref=rs_recv.at[g],
            send_sem=rs_ssem.at[i], recv_sem=rs_rsem.at[i],
            device_id=(to, c), device_id_type=MESH)

    def rs_wait(i):
        src = lax.rem(g + sub_size - i, sub_size)
        pltpu.make_async_remote_copy(
            src_ref=rs_send.at[src], dst_ref=rs_recv.at[src],
            send_sem=rs_ssem.at[i], recv_sem=rs_rsem.at[i],
            device_id=(src, c), device_id_type=MESH).wait_recv()

    pl.semaphore_wait(met, len(outer))
    each(sub_size - 1, lambda i: rs_copy(i + 1).start())
    moves = [(i, n) for i in range(crs_size) for n in range(6) if i or n > 2]
    for i, n in moves:
        f_copy(i, n).start()
    _, pieces = f_pieces(0)
    for start, place, size, _ in pieces[:3]:
        fcat[c, pl.ds(place, size), :] = factor[pl.ds(start, size), :]

    rs_recv[g] = rs_send[g]
    each(sub_size - 1, lambda i: rs_wait(i + 1))
    mine = rs_recv[0]
    for q in range(1, sub_size):
        mine = mine + rs_recv[q]
    ag_send[...] = mine

    def ag_copy(i):
        return pltpu.make_async_remote_copy(
            src_ref=ag_send, dst_ref=panel.at[c, g],
            send_sem=ag_ssem.at[i], recv_sem=ag_rsem.at[i],
            device_id=rank(i), device_id_type=MESH)

    def ag_wait(i):
        fg, fcr = rank(devices - i)
        pltpu.make_async_remote_copy(
            src_ref=ag_send, dst_ref=panel.at[fcr, fg],
            send_sem=ag_ssem.at[i], recv_sem=ag_rsem.at[i],
            device_id=(fg, fcr), device_id_type=MESH).wait_recv()

    each(devices - 1, lambda i: ag_copy(i + 1).start())
    panel[c, g] = mine
    for i, n in moves:
        f_wait(i, n)
    for p in range(crs_size):
        fpair[p] = both(fcat[p])
    each(devices - 1, lambda i: ag_wait(i + 1))

    amps = jnp.zeros((2 * nrhs, 2 * LANES), jnp.float32)
    for p in range(crs_size):
        for q in range(parts):
            rows = panel[p, q * nrhs:(q + 1) * nrhs].reshape(nrhs, chunk)
            amps = amps + dot(both(rows), fpair[p, :, q * chunk:(q + 1) * chunk], NT)
    amps = quarters(amps)
    for s in range(subs):
        out_h[:, s, :] = twice(amps, pair[:, s * width:(s + 1) * width])

    for j in range(4):
        for i in range(crs_size):
            if j or i:
                c_copy(j, i).wait_send()
    for i, n in moves:
        f_copy(i, n).wait_send()
    each(sub_size - 1, lambda i: rs_copy(i + 1).wait_send())
    each(devices - 1, lambda i: ag_copy(i + 1).wait_send())


def wide_body(sub_size, crs_size, mult, own, nbr, face, nlist, factor):
    nk, subs, width = own.shape
    nrhs = mult.shape[0]
    part = nk * subs
    blocks = -(-crs_size // (LANES // part))
    cols = factor.shape[1]
    chunk = cols * nrhs // sub_size
    f32 = jnp.float32
    dma = pltpu.SemaphoreType.DMA
    bf16 = jnp.bfloat16
    hbm = pl.BlockSpec(memory_space=pl.ANY)
    names = nlist.T
    applied = pl.pallas_call(
        functools.partial(wide_kernel, sub_size, crs_size),
        out_shape=pltpu.VMEM(mult.shape, mult.dtype),
        in_specs=[hbm] * 6,
        out_specs=pl.BlockSpec(memory_space=pltpu.VMEM),
        scratch_shapes=[
            pltpu.VMEM(mult.shape, f32), pltpu.VMEM(own.shape, f32), pltpu.VMEM(nbr.shape, f32),
            pltpu.VMEM(face.shape, face.dtype), pltpu.SMEM(names.shape, names.dtype),
            pltpu.VMEM(factor.shape, f32),
            pltpu.VMEM((LANES, subs * width), f32),
            pltpu.VMEM((2 * LANES, subs * width), bf16),
            pltpu.VMEM((nrhs, LANES), f32),
            pltpu.VMEM((4, crs_size, nrhs, LANES), f32),
            pltpu.VMEM((crs_size, LANES, cols), f32),
            pltpu.VMEM((blocks, 2 * LANES, cols), bf16),
            pltpu.VMEM((crs_size, 2 * LANES, cols), bf16),
            pltpu.VMEM((sub_size, 1, chunk), f32),
            pltpu.VMEM((sub_size, 1, chunk), f32),
            pltpu.VMEM((1, chunk), f32),
            pltpu.VMEM((crs_size, sub_size, 1, chunk), f32),
            dma((4, crs_size)), dma((4, crs_size)),
            dma((crs_size, 6)), dma((crs_size, 6)),
            dma((sub_size,)), dma((sub_size,)),
            dma((sub_size * crs_size,)), dma((sub_size * crs_size,)), dma((6,)),
            pltpu.SemaphoreType.REGULAR,
        ],
        compiler_params=pltpu.CompilerParams(collective_id=0, has_side_effects=True),
    )(mult, own, nbr, face, names, factor)
    return mult - applied


def body(sub_size, crs_size, mult, own, nbr, face, nlist, factor):
    slabs = crs_size * factor.shape[1] // LANES
    held = own.shape[0] * own.shape[1] * crs_size
    fits = (slabs <= 6 and crs_size == 2 and factor.shape[1] % LANES == 0 and held * 5 <= LANES * 2
            and 12 <= sub_size <= LANES // 4 and mult.shape[0] > 2 * own.shape[0])
    form = near_body if fits else wide_body
    return form(sub_size, crs_size, mult, own, nbr, face, nlist, factor)


def solution(mesh):
    placed = (
        P(None, ("sub", "crs"), None),
        P(None, ("sub", "crs"), None),
        P(None, ("sub", "crs"), None),
        P(("sub", "crs"), None),
        P(),
        P("sub", "crs"),
    )
    return jax.shard_map(
        functools.partial(body, mesh.shape["sub"], mesh.shape["crs"]),
        mesh=mesh, in_specs=placed, out_specs=P(None, ("sub", "crs"), None), check_vma=False
    )
```

```python
import functools

import jax
import jax.numpy as jnp
from jax import lax
from jax.experimental import pallas as pl
from jax.experimental.pallas import tpu as pltpu
from jax.sharding import PartitionSpec as P

MESH = pl.DeviceIdType.MESH
NT = (((1,), (1,)), ((), ()))
NN = (((1,), (0,)), ((), ()))
LANES = 128
EDGE = 8


def each(count, step):
    if count <= 64:
        for i in sorted(range(count), key=lambda i: min(i, count - 1 - i)):
            step(i)
    else:
        lax.fori_loop(0, count, lambda i, t: (step(i), t)[1], 0)


def both(value, axis=0):
    high = value.astype(jnp.bfloat16)
    low = (value - high.astype(jnp.float32)).astype(jnp.bfloat16)
    return jnp.concatenate([high, low], axis=axis)


def halves(value):
    rows = value.shape[0] // 2
    return value[:rows] + value[rows:]


def quarters(value):
    value = halves(value)
    cols = value.shape[1] // 2
    return value[:, :cols] + value[:, cols:]


def dot(left, right, dims):
    return lax.dot_general(left, right, dims, preferred_element_type=jnp.float32)


def twice(left, right):
    high = left.astype(jnp.bfloat16)
    low = (left - high.astype(jnp.float32)).astype(jnp.bfloat16)
    wide = jnp.concatenate(
        [jnp.concatenate([high, high], axis=1), jnp.concatenate([low, low], axis=1)], axis=0)
    return halves(dot(wide, right, NN))


def homes_of(sub_size, slabs):
    q = sub_size // 4
    return (q, 2 * q + 2, q + 2, 2 * q + 1, q + 1, 2 * q)[:slabs]


N2, N3 = 2, 2


def parted(value):
    high = value.astype(jnp.bfloat16).astype(jnp.float32)
    return high, value - high


def near_kernel(
    sub_size, crs_size,
    mult_h, own_h, nbr_h, face_h, nlist_h, factor_h, out_h,
    mult, own, nbr, face, nlist, factor,
    modes, pair, s_send, s_recv, slab, wide_f, a_send, a_recv,
    in_sem, f_ssem, f_rsem, s_ssem, s_rsem, a_ssem, a_rsem,
):
    nk, subs, width = own.shape
    nrhs = mult.shape[0]
    nface = nlist.shape[0]
    part = nk * subs
    held = part * crs_size
    tiles = factor.shape[1] // LANES
    slabs = crs_size * tiles
    row_len = sub_size // 2
    group = subs * crs_size
    devices = sub_size * crs_size
    head = crs_size - 1
    homes = homes_of(sub_size, slabs)
    g = lax.axis_index("sub")
    c = lax.axis_index("crs")
    me = g * crs_size + c
    owns = jnp.full((), False)
    mine = jnp.zeros((), jnp.int32)
    for j, home in enumerate(homes):
        owns = jnp.logical_or(owns, g == home)
        mine = jnp.where(g == home, j, mine)
    is_owner = jnp.logical_and(c == head, owns)
    is_plain = jnp.logical_not(is_owner)
    keeps = jnp.logical_and(is_owner, mine >= head * tiles)
    far = 2 * held
    edge = far + part

    def around(g):
        first, second = g // row_len, g % row_len
        return (
            (first + 1) % 2 * row_len + second,
            first * row_len + (second + 1) % row_len,
            first * row_len + (second + row_len - 1) % row_len,
        )

    def landed(ref, semaphore):
        pltpu.make_async_copy(ref, ref, semaphore).wait()

    barrier = pltpu.get_barrier_semaphore()

    @pl.when(is_owner)
    def _():
        for i in range(devices - 1):
            to = i + jnp.where(i >= me, 1, 0)
            pl.semaphore_signal(
                barrier, inc=1, device_id=(to // crs_size, lax.rem(to, crs_size)), device_id_type=MESH)

    loads = [
        pltpu.make_async_copy(a, b, in_sem.at[i]) for i, a, b in (
            (0, factor_h, factor), (1, nlist_h, nlist), (2, face_h, face), (2, nbr_h, nbr),
            (2, own_h, own), (3, mult_h, mult))
    ]
    for load in loads:
        load.start()
    modes[edge:, :] = jnp.zeros((LANES - edge, modes.shape[1]), jnp.float32)

    @pl.when(is_owner)
    def _():
        for i in range(sub_size // 2):
            slab[i * LANES + far:(i + 1) * LANES, :] = jnp.zeros((LANES - far, LANES), jnp.float32)

    loads[0].wait()
    late = g >= sub_size // 2
    last = g >= sub_size - sub_size // 4

    def meet():
        @pl.when(is_owner)
        def _():
            pl.semaphore_wait(barrier, slabs - 1)

        @pl.when(is_plain)
        def _():
            pl.semaphore_wait(barrier, slabs)

    def home_of(j):
        home = jnp.zeros((), jnp.int32)
        for i in range(slabs):
            home = jnp.where(j == i, homes[i], home)
        return home

    def tile_in(t):
        return factor.at[:, pl.ds(pl.multiple_of(t * LANES, LANES), LANES)]

    def f_copy(t, home):
        return pltpu.make_async_remote_copy(
            src_ref=tile_in(t),
            dst_ref=slab.at[pl.ds(pl.multiple_of(g // 2 * LANES + lax.rem(g, 2) * held, 8), held), :],
            send_sem=f_ssem, recv_sem=f_rsem,
            device_id=(home, head), device_id_type=MESH)

    def f_start(t):
        t = lax.rem(t + g, tiles)
        home = home_of(c * tiles + t)
        self_kept = jnp.logical_and(c == head, g == home)

        @pl.when(jnp.logical_not(self_kept))
        def _():
            f_copy(t, home).start()

        @pl.when(self_kept)
        def _():
            slab[pl.ds(pl.multiple_of(g // 2 * LANES + lax.rem(g, 2) * held, 8), held), :] = tile_in(t)[...]

    @pl.when(late)
    def _():
        meet()
        for t in range(N2):
            f_start(t)

    @pl.when(last)
    def _():
        for t in range(N2, N3):
            f_start(t)

    loads[1].wait()
    landed(mult.at[pl.ds(0, 2 * nk + 1)], in_sem.at[2])
    across, after, before = around(g)
    fc = face[...]
    first_sub = me * subs
    line = lax.broadcasted_iota(jnp.int32, (subs, width), 0)
    target = jnp.zeros((subs, width), jnp.int32)
    for f in range(nface):
        name = jnp.zeros((subs, width), jnp.int32)
        for s in range(subs):
            name = jnp.where(line == s, nlist[f, first_sub + s], name)
        target = jnp.where(fc == f, name, target)
    third = c * subs + line
    nxt = jnp.where(third == group - 1, 0, third + 1)
    prv = jnp.where(third == 0, group - 1, third - 1)

    def chosen(block, line):
        return jnp.where(target == block * group + line, 1.0, 0.0)

    masks = (
        chosen(g, nxt), chosen(g, prv),
        chosen(across, third), chosen(after, third), chosen(before, third),
    )
    here, there = lax.rem(g, 2) * held, lax.rem(g + 1, 2) * held
    mine_at, other_at = c * part, (1 - c) * part

    def block(*pieces):
        rows, at = [], 0
        for start, value in pieces:
            if start > at:
                rows.append(jnp.zeros((start - at, width), jnp.float32))
            rows.append(value)
            at = start + nk
        if at < part:
            rows.append(jnp.zeros((part - at, width), jnp.float32))
        return jnp.concatenate(rows, axis=0)

    for s in range(subs):
        own_s = own[:, s, :]
        nbr_s = nbr[:, s, :]
        to = [nbr_s * masks[d][s:s + 1, :] for d in range(5)]
        first_at, last_at = s == 0, s == subs - 1
        inner = [(nk * s, own_s)]
        if not last_at:
            inner.append((nk * (s + 1), to[0]))
        if not first_at:
            inner.insert(0, (nk * (s - 1), to[1]))
        outer = []
        if last_at:
            outer.append((0, to[0]))
        if first_at:
            outer.append((part - nk, to[1]))
        for base, value in (
            (here + mine_at, block(*inner)),
            (here + other_at, block(*outer)),
            (there + mine_at, block((nk * s, to[3]))),
            (there + other_at, block((nk * s, to[4]))),
            (far, block((nk * s, to[2]))),
        ):
            start = base if isinstance(base, int) else pl.multiple_of(base, 8)
            modes[pl.ds(start, part), pl.ds(s * width, width)] = value
    loads[5].wait()
    sums = jnp.zeros((2 * nrhs, 2 * LANES), jnp.float32)
    for s in range(subs):
        at = pl.ds(s * width, width)
        split = both(modes[:, at])
        pair[:, at] = split
        sums = sums + dot(both(mult[:, s, :]), split, NT)
    sums = quarters(sums)
    s_send[...] = sums
    pl.when(jnp.logical_not(late))(meet)

    def s_copy(j):
        return pltpu.make_async_remote_copy(
            src_ref=s_send, dst_ref=s_recv.at[me],
            send_sem=s_ssem, recv_sem=s_rsem,
            device_id=(home_of(j), head), device_id_type=MESH)

    turn = jnp.where(is_owner, mine + 1, lax.rem(g, 2) * crs_size)
    for i in range(slabs - 1):
        s_copy(lax.rem(turn + i, slabs)).start()

    @pl.when(is_plain)
    def _():
        s_copy(lax.rem(turn + slabs - 1, slabs)).start()

    @pl.when(jnp.logical_not(late))
    def _():
        for t in range(N2):
            f_start(t)

    @pl.when(jnp.logical_not(last))
    def _():
        for t in range(N2, N3):
            f_start(t)

    for t in range(N3, tiles):
        f_start(t)

    def a_copy(d):
        return pltpu.make_async_remote_copy(
            src_ref=a_send.at[d], dst_ref=a_recv.at[mine],
            send_sem=a_ssem, recv_sem=a_rsem,
            device_id=(lax.div(d, crs_size), lax.rem(d, crs_size)), device_id_type=MESH)

    def a_group(start, stop):
        inside = jnp.logical_and(me >= start, me < stop)
        for d in range(start, stop - 1):
            a_copy(d + jnp.where(jnp.logical_and(inside, d >= me), 1, 0)).start()

        @pl.when(jnp.logical_not(inside))
        def _():
            a_copy(jnp.int32(stop - 1)).start()

    @pl.when(is_owner)
    def _():
        s_recv[me] = sums

        lane = lax.broadcasted_iota(jnp.int32, (nrhs, LANES), 1)
        rhs = [jnp.zeros((nrhs, LANES), jnp.float32)] * (sub_size // 2)

        def rows_of(d):
            b, p = d // crs_size, d % crs_size
            x, n, q = around(b)

            def take(block, start, size):
                at = block // 2 * LANES + block % 2 * held + start
                return jnp.concatenate(parted(slab[at:at + size, :]), axis=1)

            others = [take(n, p * part, part), take(q, p * part, part)]
            halves_of = [take(b, 0, held), jnp.concatenate(others if p == 0 else others[::-1], axis=0)]
            spare = jnp.zeros((LANES - edge, 2 * LANES), jnp.float32)
            return jnp.concatenate(
                (halves_of if b % 2 == 0 else halves_of[::-1]) + [take(x, p * part, part), spare], axis=0)

        def only(value, at, size):
            return jnp.where((lane >= at) & (lane < at + size), value, 0.0)

        def turned(value, by):
            return pltpu.roll(value, by % LANES, 1)

        @pl.when(keeps)
        def _():
            landed(slab.at[pl.ds(0, (sub_size - 1) * held), :], f_rsem)

        @pl.when(jnp.logical_not(keeps))
        def _():
            landed(slab.at[pl.ds(0, sub_size * held), :], f_rsem)

        wide_f[...] = both(slab[...], axis=1)
        landed(s_recv.at[pl.ds(0, devices - 1)], s_rsem)
        for b in range(sub_size):
            x, n, q = around(b)
            this, that = b % 2 * held, (b + 1) % 2 * held
            pair_sum = s_recv[b * crs_size] + s_recv[b * crs_size + 1]
            rhs[b // 2] = rhs[b // 2] + only(pair_sum, this, held)
            for p in range(crs_size):
                value = s_recv[b * crs_size + p]
                at, off = p * part, (1 - p) * part
                rhs[n // 2] = rhs[n // 2] + only(value, that + at, part)
                rhs[q // 2] = rhs[q // 2] + only(turned(value, at - off), that + at, part)
                rhs[x // 2] = rhs[x // 2] + only(turned(value, this + at - far), this + at, part)
        rhs_rows = jnp.concatenate(parted(jnp.concatenate(rhs, axis=1)), axis=0)
        panel = quarters(dot(rhs_rows.astype(jnp.bfloat16), wide_f[...], NN))
        ph, pw = parted(panel)
        wide = jnp.concatenate(
            [jnp.concatenate([ph, ph], axis=1), jnp.concatenate([pw, pw], axis=1)], axis=0)
        first_rows = jnp.concatenate([rows_of(d) for d in range(crs_size)], axis=0)
        term = halves(dot(wide, first_rows, NT))
        for d in range(crs_size):
            a_send[d] = term[:, d * LANES:(d + 1) * LANES]
            a_copy(jnp.int32(d)).start()
        amps = halves(dot(wide.astype(jnp.bfloat16), wide_f[...], NT))
        tiled = [amps[:, i * LANES:(i + 1) * LANES] for i in range(sub_size // 2)]

        def form(d):
            b, p = d // crs_size, d % crs_size
            x, n, q = around(b)
            this, that = b % 2 * held, (b + 1) % 2 * held
            at, off = p * part, (1 - p) * part
            value = turned(tiled[x // 2], far - this - at)
            value = jnp.where((lane >= this) & (lane < this + held), tiled[b // 2], value)
            value = jnp.where((lane >= that + at) & (lane < that + at + part), tiled[n // 2], value)
            a_send[d] = jnp.where(
                (lane >= that + off) & (lane < that + off + part), turned(tiled[q // 2], off - at), value)

        quarter = devices // 4
        for start, stop in ((3 * quarter, devices), (2 * quarter, 3 * quarter), (2, quarter), (quarter, 2 * quarter)):
            for d in range(start, stop):
                form(d)
            a_group(start, stop)
        a_recv[mine] = a_send[me]
        landed(a_recv.at[pl.ds(0, slabs - 1)], a_rsem)

    @pl.when(is_plain)
    def _():
        landed(a_recv, a_rsem)

    amps = a_recv[0]
    for j in range(1, slabs):
        amps = amps + a_recv[j]
    for s in range(subs):
        out_h[:, s, :] = mult[:, s, :] - twice(amps, pair[:, s * width:(s + 1) * width])

    @pl.when(keeps)
    def _():
        landed(factor.at[:, 0:(tiles - 1) * LANES], f_ssem)

    @pl.when(jnp.logical_not(keeps))
    def _():
        landed(factor, f_ssem)

    @pl.when(is_owner)
    def _():
        landed(s_recv.at[pl.ds(0, slabs - 1)], s_ssem)
        landed(a_send.at[pl.ds(0, devices - 1)], a_ssem)

    @pl.when(is_plain)
    def _():
        landed(s_recv.at[pl.ds(0, slabs)], s_ssem)


def near_body(sub_size, crs_size, mult, own, nbr, face, nlist, factor):
    nk, subs, width = own.shape
    nrhs = mult.shape[0]
    cols = factor.shape[1]
    devices = sub_size * crs_size
    slabs = crs_size * cols // LANES
    order = sub_size * (LANES // 2)
    f32, bf16 = jnp.float32, jnp.bfloat16
    dma = pltpu.SemaphoreType.DMA
    hbm = pl.BlockSpec(memory_space=pl.ANY)
    names = nlist.T
    projected = pl.pallas_call(
        functools.partial(near_kernel, sub_size, crs_size),
        out_shape=pltpu.VMEM(mult.shape, mult.dtype),
        in_specs=[hbm] * 6,
        out_specs=pl.BlockSpec(memory_space=pltpu.VMEM),
        scratch_shapes=[
            pltpu.VMEM(mult.shape, f32), pltpu.VMEM(own.shape, f32), pltpu.VMEM(nbr.shape, f32),
            pltpu.VMEM(face.shape, face.dtype), pltpu.SMEM(names.shape, names.dtype),
            pltpu.VMEM(factor.shape, f32),
            pltpu.VMEM((LANES, subs * width), f32),
            pltpu.VMEM((2 * LANES, subs * width), bf16),
            pltpu.VMEM((nrhs, LANES), f32),
            pltpu.VMEM((devices, nrhs, LANES), f32),
            pltpu.VMEM((order, LANES), f32),
            pltpu.VMEM((order, 2 * LANES), bf16),
            pltpu.VMEM((devices, nrhs, LANES), f32),
            pltpu.VMEM((slabs, nrhs, LANES), f32),
            dma((4,)), dma, dma, dma, dma, dma, dma,
        ],
        compiler_params=pltpu.CompilerParams(collective_id=0, has_side_effects=True),
    )(mult, own, nbr, face, names, factor)
    return projected


def wide_kernel(
    sub_size, crs_size,
    mult_h, own_h, nbr_h, face_h, nlist_h, factor_h, out_h,
    mult, own, nbr, face, nlist, factor,
    modes, pair, c_send, c_recv, fcat, fown, fpair, rs_send, rs_recv, ag_send, panel,
    c_ssem, c_rsem, f_ssem, f_rsem, rs_ssem, rs_rsem, ag_ssem, ag_rsem, in_sem, met,
):
    nk, subs, width = own.shape
    nrhs = mult.shape[0]
    nface = nlist.shape[0]
    part = nk * subs
    parts = sub_size // nrhs
    row_len = sub_size // 2
    group = subs * crs_size
    devices = sub_size * crs_size
    g = lax.axis_index("sub")
    c = lax.axis_index("crs")
    me = g * crs_size + c
    up, down = part, part + EDGE
    off_x = part + 2 * EDGE
    off_n, off_p = off_x + part, off_x + 2 * part

    def rank(i):
        other = lax.rem(me + i, devices)
        return (other // crs_size, lax.rem(other, crs_size))

    loads = [
        pltpu.make_async_copy(a, b, in_sem.at[i]) for i, (a, b) in enumerate((
            (nlist_h, nlist), (face_h, face), (nbr_h, nbr), (own_h, own),
            (mult_h, mult), (factor_h, factor)))
    ]
    for load in loads:
        load.start()
    barrier = pltpu.get_barrier_semaphore()
    first, second = g // row_len, lax.rem(g, row_len)
    across = lax.rem(first + 1, 2) * row_len + second
    after = first * row_len + lax.rem(second + 1, row_len)
    before = first * row_len + lax.rem(second + row_len - 1, row_len)
    groups = (g, across, after, before)

    block = 1 << (devices.bit_length() // 2)
    base = me // block * block
    inner = [base + lax.rem(me - base + i, block) for i in range(1, block)]
    outer = [lax.rem(me + i, devices) for i in range(block, devices, block)]
    near = [groups[j] * crs_size + lax.rem(c + i, crs_size)
            for j in range(4) for i in range(crs_size) if j or i]

    def signal(semaphore, other):
        pl.semaphore_signal(
            semaphore, inc=1, device_id=(other // crs_size, lax.rem(other, crs_size)),
            device_id_type=MESH)

    for other in outer + near + inner:
        signal(barrier, other)

    modes[...] = jnp.zeros_like(modes)
    fcat[:, down + EDGE + 3 * part:, :] = jnp.zeros(
        (crs_size, LANES - (down + EDGE + 3 * part), fcat.shape[2]), jnp.float32)
    for load in loads[:4]:
        load.wait()
    fc = face[...]
    first_sub = me * subs
    line = lax.broadcasted_iota(jnp.int32, (subs, width), 0)
    target = jnp.zeros((subs, width), jnp.int32)
    for f in range(nface):
        name = jnp.zeros((subs, width), jnp.int32)
        for s in range(subs):
            name = jnp.where(line == s, nlist[f, first_sub + s], name)
        target = jnp.where(fc == f, name, target)
    third = c * subs + line
    nxt = jnp.where(third == group - 1, 0, third + 1)
    prv = jnp.where(third == 0, group - 1, third - 1)

    def chosen(block, line):
        return jnp.where(target == block * group + line, 1.0, 0.0)

    masks = (
        chosen(g, nxt), chosen(g, prv),
        chosen(across, third), chosen(after, third), chosen(before, third),
    )
    for s in range(subs):
        cols = pl.ds(s * width, width)
        own_s = own[:, s, :]
        nbr_s = nbr[:, s, :]
        rows = (
            nk * (s + 1) if s < subs - 1 else up,
            nk * (s - 1) if s > 0 else down + EDGE - nk,
            off_x + nk * s, off_n + nk * s, off_p + nk * s,
        )
        modes[pl.ds(nk * s, nk), cols] = own_s
        for d in range(5):
            value = nbr_s * masks[d][s:s + 1, :]
            spot = pl.ds(rows[d], nk)
            modes[spot, cols] = value
    loads[4].wait()
    sums = jnp.zeros((2 * nrhs, 2 * LANES), jnp.float32)
    for s in range(subs):
        cols = pl.ds(s * width, width)
        split = both(modes[:, cols])
        pair[:, cols] = split
        sums = sums + dot(both(mult[:, s, :]), split, NT)
    sums = quarters(sums)
    c_send[...] = sums
    c_recv[0, c] = sums

    pl.semaphore_wait(barrier, len(outer) + len(near) + len(inner))

    def c_copy(j, i):
        to = lax.rem(c + i, crs_size)
        return pltpu.make_async_remote_copy(
            src_ref=c_send, dst_ref=c_recv.at[j, c],
            send_sem=c_ssem.at[j, i], recv_sem=c_rsem.at[j, i],
            device_id=(groups[j], to), device_id_type=MESH)

    def c_wait(j, i):
        src = lax.rem(c + crs_size - i, crs_size)
        pltpu.make_async_remote_copy(
            src_ref=c_send, dst_ref=c_recv.at[j, src],
            send_sem=c_ssem.at[j, i], recv_sem=c_rsem.at[j, i],
            device_id=(groups[j], src), device_id_type=MESH).wait_recv()

    for j in (1, 2, 3, 0):
        for i in range(crs_size):
            if j or i:
                c_copy(j, i).start()

    def row(p, extra=0):
        return pl.multiple_of(p * part + extra, 8)

    def f_pieces(i):
        to = lax.rem(c + i, crs_size)
        nx = lax.rem(to + 1, crs_size)
        pv = lax.rem(to + crs_size - 1, crs_size)
        return to, (
            (row(to), 0, part, g),
            (row(nx), up, EDGE, g),
            (row(pv, part - EDGE), down, EDGE, g),
            (row(to), off_x, part, across),
            (row(to), off_p, part, after),
            (row(to), off_n, part, before),
        )

    def f_copy(i, n):
        to, pieces = f_pieces(i)
        start, place, size, where = pieces[n]
        return pltpu.make_async_remote_copy(
            src_ref=factor.at[pl.ds(start, size), :],
            dst_ref=fcat.at[c, pl.ds(place, size), :],
            send_sem=f_ssem.at[i, n], recv_sem=f_rsem.at[i, n],
            device_id=(where, to), device_id_type=MESH)

    def f_wait(i, n):
        to, pieces = f_pieces(i)
        start, place, size, where = pieces[n]
        src = lax.rem(c + crs_size - i, crs_size)
        pltpu.make_async_remote_copy(
            src_ref=factor.at[pl.ds(start, size), :],
            dst_ref=fcat.at[src, pl.ds(place, size), :],
            send_sem=f_ssem.at[i, n], recv_sem=f_rsem.at[i, n],
            device_id=(where, to), device_id_type=MESH).wait_recv()

    for other in outer:
        signal(met, other)

    loads[5].wait()
    span = LANES // part
    blocks = fown.shape[0]
    for b in range(blocks):
        held = factor[b * span * part:min((b + 1) * span, crs_size) * part, :]
        if held.shape[0] < LANES:
            held = jnp.concatenate(
                [held, jnp.zeros((LANES - held.shape[0], held.shape[1]), jnp.float32)], axis=0)
        fown[b] = both(held)

    for j in (0, 1, 2, 3):
        for i in range(crs_size):
            if j or i:
                c_wait(j, i)

    lane = lax.broadcasted_iota(jnp.int32, (nrhs, LANES), 1)

    def rolled(value, by):
        return pltpu.roll(value, (LANES - by) % LANES, 1) if by % LANES else value

    total = jnp.zeros((nrhs, factor.shape[1]), jnp.float32)
    for b in range(blocks):
        group_rhs = jnp.zeros((nrhs, LANES), jnp.float32)
        for p in range(b * span, min((b + 1) * span, crs_size)):
            at = (p - b * span) * part
            low = c_recv[0, (p - 1) % crs_size]
            high = c_recv[0, (p + 1) % crs_size]
            rhs = rolled(c_recv[0, p], -at)
            rhs = rhs + jnp.where(lane < at + EDGE, rolled(low, up - at), 0.0)
            rhs = rhs + jnp.where(
                lane >= at + part - EDGE, rolled(high, down - (at + part - EDGE)), 0.0)
            rhs = rhs + rolled(c_recv[1, p], off_x - at)
            rhs = rhs + rolled(c_recv[2, p], off_n - at)
            rhs = rhs + rolled(c_recv[3, p], off_p - at)
            group_rhs = jnp.where((lane >= at) & (lane < at + part), rhs, group_rhs)
        total = total + twice(group_rhs, fown[b])

    chunk = factor.shape[1] // parts
    for q in range(parts):
        for r in range(nrhs):
            rs_send[q * nrhs + r] = total[r:r + 1, q * chunk:(q + 1) * chunk]

    def rs_copy(i):
        to = lax.rem(g + i, sub_size)
        return pltpu.make_async_remote_copy(
            src_ref=rs_send.at[to], dst_ref=rs_recv.at[g],
            send_sem=rs_ssem.at[i], recv_sem=rs_rsem.at[i],
            device_id=(to, c), device_id_type=MESH)

    def rs_wait(i):
        src = lax.rem(g + sub_size - i, sub_size)
        pltpu.make_async_remote_copy(
            src_ref=rs_send.at[src], dst_ref=rs_recv.at[src],
            send_sem=rs_ssem.at[i], recv_sem=rs_rsem.at[i],
            device_id=(src, c), device_id_type=MESH).wait_recv()

    pl.semaphore_wait(met, len(outer))
    each(sub_size - 1, lambda i: rs_copy(i + 1).start())
    moves = [(i, n) for i in range(crs_size) for n in range(6) if i or n > 2]
    for i, n in moves:
        f_copy(i, n).start()
    _, pieces = f_pieces(0)
    for start, place, size, _ in pieces[:3]:
        fcat[c, pl.ds(place, size), :] = factor[pl.ds(start, size), :]

    rs_recv[g] = rs_send[g]
    each(sub_size - 1, lambda i: rs_wait(i + 1))
    mine = rs_recv[0]
    for q in range(1, sub_size):
        mine = mine + rs_recv[q]
    ag_send[...] = mine

    def ag_copy(i):
        return pltpu.make_async_remote_copy(
            src_ref=ag_send, dst_ref=panel.at[c, g],
            send_sem=ag_ssem.at[i], recv_sem=ag_rsem.at[i],
            device_id=rank(i), device_id_type=MESH)

    def ag_wait(i):
        fg, fcr = rank(devices - i)
        pltpu.make_async_remote_copy(
            src_ref=ag_send, dst_ref=panel.at[fcr, fg],
            send_sem=ag_ssem.at[i], recv_sem=ag_rsem.at[i],
            device_id=(fg, fcr), device_id_type=MESH).wait_recv()

    each(devices - 1, lambda i: ag_copy(i + 1).start())
    panel[c, g] = mine
    for i, n in moves:
        f_wait(i, n)
    for p in range(crs_size):
        fpair[p] = both(fcat[p])
    each(devices - 1, lambda i: ag_wait(i + 1))

    amps = jnp.zeros((2 * nrhs, 2 * LANES), jnp.float32)
    for p in range(crs_size):
        for q in range(parts):
            rows = panel[p, q * nrhs:(q + 1) * nrhs].reshape(nrhs, chunk)
            amps = amps + dot(both(rows), fpair[p, :, q * chunk:(q + 1) * chunk], NT)
    amps = quarters(amps)
    for s in range(subs):
        out_h[:, s, :] = twice(amps, pair[:, s * width:(s + 1) * width])

    for j in range(4):
        for i in range(crs_size):
            if j or i:
                c_copy(j, i).wait_send()
    for i, n in moves:
        f_copy(i, n).wait_send()
    each(sub_size - 1, lambda i: rs_copy(i + 1).wait_send())
    each(devices - 1, lambda i: ag_copy(i + 1).wait_send())


def wide_body(sub_size, crs_size, mult, own, nbr, face, nlist, factor):
    nk, subs, width = own.shape
    nrhs = mult.shape[0]
    part = nk * subs
    blocks = -(-crs_size // (LANES // part))
    cols = factor.shape[1]
    chunk = cols * nrhs // sub_size
    f32 = jnp.float32
    dma = pltpu.SemaphoreType.DMA
    bf16 = jnp.bfloat16
    hbm = pl.BlockSpec(memory_space=pl.ANY)
    names = nlist.T
    applied = pl.pallas_call(
        functools.partial(wide_kernel, sub_size, crs_size),
        out_shape=pltpu.VMEM(mult.shape, mult.dtype),
        in_specs=[hbm] * 6,
        out_specs=pl.BlockSpec(memory_space=pltpu.VMEM),
        scratch_shapes=[
            pltpu.VMEM(mult.shape, f32), pltpu.VMEM(own.shape, f32), pltpu.VMEM(nbr.shape, f32),
            pltpu.VMEM(face.shape, face.dtype), pltpu.SMEM(names.shape, names.dtype),
            pltpu.VMEM(factor.shape, f32),
            pltpu.VMEM((LANES, subs * width), f32),
            pltpu.VMEM((2 * LANES, subs * width), bf16),
            pltpu.VMEM((nrhs, LANES), f32),
            pltpu.VMEM((4, crs_size, nrhs, LANES), f32),
            pltpu.VMEM((crs_size, LANES, cols), f32),
            pltpu.VMEM((blocks, 2 * LANES, cols), bf16),
            pltpu.VMEM((crs_size, 2 * LANES, cols), bf16),
            pltpu.VMEM((sub_size, 1, chunk), f32),
            pltpu.VMEM((sub_size, 1, chunk), f32),
            pltpu.VMEM((1, chunk), f32),
            pltpu.VMEM((crs_size, sub_size, 1, chunk), f32),
            dma((4, crs_size)), dma((4, crs_size)),
            dma((crs_size, 6)), dma((crs_size, 6)),
            dma((sub_size,)), dma((sub_size,)),
            dma((sub_size * crs_size,)), dma((sub_size * crs_size,)), dma((6,)),
            pltpu.SemaphoreType.REGULAR,
        ],
        compiler_params=pltpu.CompilerParams(collective_id=0, has_side_effects=True),
    )(mult, own, nbr, face, names, factor)
    return mult - applied


def body(sub_size, crs_size, mult, own, nbr, face, nlist, factor):
    slabs = crs_size * factor.shape[1] // LANES
    held = own.shape[0] * own.shape[1] * crs_size
    fits = (slabs <= 6 and crs_size == 2 and factor.shape[1] % LANES == 0 and held * 5 <= LANES * 2
            and 12 <= sub_size <= LANES // 4 and mult.shape[0] > 2 * own.shape[0])
    form = near_body if fits else wide_body
    return form(sub_size, crs_size, mult, own, nbr, face, nlist, factor)


def solution(mesh):
    placed = (
        P(None, ("sub", "crs"), None),
        P(None, ("sub", "crs"), None),
        P(None, ("sub", "crs"), None),
        P(("sub", "crs"), None),
        P(),
        P("sub", "crs"),
    )
    return jax.shard_map(
        functools.partial(body, mesh.shape["sub"], mesh.shape["crs"]),
        mesh=mesh, in_specs=placed, out_specs=P(None, ("sub", "crs"), None), check_vma=False
    )
```
